128 devices in a mesh: dom: 32 (over x, y, core), shift: 4 (over z).
Axes of the slice: x: 4, y: 4, z: 4, core: 2. Of those that a mesh axis runs over, the one named last changes fastest.
Arguments:
- sources: float32 [32, 128, 16, 128], P('shift', 'dom'), may hold values from -6 to 6
- kappa: float32 [128, 16, 128], P('dom'), may hold values from 0 to 2
- mass: float32 [128, 16, 128], P('dom'), may hold values from 0.25 to 4
- shift_table: float32 [64], replicated, may hold values from 0.5 to 4
- shift_ids: int32 [16], P('shift'), may hold values from 0 to 63
- sketch: bfloat16 [1024, 128, 16, 128], P(None, 'dom'), may hold values from -0.1875 to 0.1875
Outputs:
- solution: float32 [16, 32, 128, 16, 128], P('shift', None, 'dom')
- residual: float32 [16, 32, 128, 16, 128], P('shift', None, 'dom')
The draws below stay inside these ranges and needn't reach their ends.
Inputs may be any that keep to these rules, and one draw needn't show every extreme that they name: `shift_ids`: index into shift_table.
All inputs are finite; a program needn't handle non-finite values.
Results may differ from the reference program's by a relative error of at most 0.0026.
Values sent between devices are 32-bit elements; how exact they have to be, the bound alone decides.
A program may use at most 128 MiB of HBM per device.

```python
import math
import jax
import jax.numpy as jnp
from jax import lax

SK = 1024
SHIFTS = 16
TABLE = 64
NY = 16
NZ = 128
B = 32
NX = 128


def plant(array, stream_key, least, top_value):
    dims = array.shape
    place = [jax.random.randint(jax.random.fold_in(stream_key, axis), (), 0, dims[axis]) for axis in range(len(dims))]
    array = array.at[tuple(place)].set(least)
    longest = dims.index(max(dims))
    place[longest] = (place[longest] + 1) % dims[longest]
    return array.at[tuple(place)].set(top_value)


def block_scale(own_key, shape, cuts, least, largest):
    gain, own = 1.0, jax.random.fold_in(own_key, 6)
    for dim, blocks in cuts:
        steps = jnp.exp(jax.random.uniform(jax.random.fold_in(own, dim), (blocks,), jnp.float32, least / len(cuts), largest / len(cuts)))
        gain = gain * jnp.repeat(steps, shape[dim] // blocks).reshape([-1 if axis == dim else 1 for axis in range(len(shape))])
    return gain


def gaussian(key, shape, deviation, reach, pieces=(), held_as=jnp.bfloat16):
    drawn = jax.random.normal(key, shape, jnp.float32) * deviation
    if len(pieces) > 0:
        drawn = block_scale(key, shape, pieces, -0.22, 0.18) * drawn
    return jnp.clip(drawn, min=-reach, max=reach).astype(held_as)


def setup_inputs(seed: int = 0) -> dict:
    splits = jax.random.split(jax.random.key(seed), 7)
    return {
        "sources": gaussian(splits[0], (B, NX, NY, NZ), 1.0, 6.0, ((0, 4), (1, 32)), jnp.float32),
        "kappa": jnp.clip(2.0 * jax.random.uniform(splits[1], (NX, NY, NZ), jnp.float32) ** block_scale(splits[1], (NX, NY, NZ), ((0, 32),), -0.2, 0.2), 0.0, 2.0),
        "mass": jnp.clip(jnp.exp(math.log(4.0) - 2.7725887 * jax.random.uniform(splits[2], (NX, NY, NZ), jnp.float32) ** block_scale(splits[2], (NX, NY, NZ), ((0, 32),), -0.2, 0.2)), 0.25, 4.0),
        "shift_table": jnp.clip(jax.random.uniform(splits[3], (TABLE,), jnp.float32, 0.5, 4.0), 0.5, 4.0),
        "shift_ids": plant(jax.random.randint(splits[4], (SHIFTS,), 0, TABLE), jax.random.fold_in(splits[4], 1), 0, TABLE - 1).astype(jnp.int32),
        "sketch": gaussian(splits[5], (SK, NX, NY, NZ), SK ** -0.5, 0.1875, ((1, 32),)),
    }


def shift_values(shift_table, shift_ids):
    entries = jnp.arange(shift_table.shape[0], dtype=jnp.int32)
    picked = jnp.where(shift_ids[:, None] == entries[None, :], shift_table[None, :], 0.0)
    return lax.optimization_barrier(jnp.sum(picked, axis=1))

def apply_operator(field, diag):
    padded = jnp.pad(field, ((0, 0), (1, 1), (1, 1), (1, 1)))
    beside = padded[:, 2:, 1:-1, 1:-1] + padded[:, :-2, 1:-1, 1:-1]
    beside = beside + padded[:, 1:-1, 2:, 1:-1] + padded[:, 1:-1, :-2, 1:-1]
    beside = beside + padded[:, 1:-1, 1:-1, 2:] + padded[:, 1:-1, 1:-1, :-2]
    return diag * field - beside

def solve_small(gram):
    h_vals = [gram[:, 1 + i, 0] for i in range(3)]
    ridge = 0.001 * (gram[:, 1, 1] + gram[:, 2, 2] + gram[:, 3, 3]) / 3.0 + 1.0
    entry = [[gram[:, 1 + i, 1 + k] + (ridge if i == k else 0.0) for k in range(3)] for i in range(3)]
    l00 = jnp.sqrt(entry[0][0])
    l10 = entry[1][0] / l00
    l20 = entry[2][0] / l00
    l11 = jnp.sqrt(entry[1][1] - l10 * l10)
    l21 = (entry[2][1] - l20 * l10) / l11
    l22 = jnp.sqrt(entry[2][2] - l20 * l20 - l21 * l21)
    f0 = h_vals[0] / l00
    f1 = (h_vals[1] - l10 * f0) / l11
    f2 = (h_vals[2] - l20 * f0 - l21 * f1) / l22
    c2 = f2 / l22
    c1 = (f1 - l21 * c2) / l11
    c0 = (f0 - l10 * c1 - l20 * c2) / l00
    return (c0, c1, c2)

def gram_of(sketched):
    return jnp.einsum('rib,rkb->bik', sketched, sketched, precision=lax.Precision.HIGHEST)

def reference(sources, kappa, mass, shift_table, shift_ids, sketch):
    sigma = shift_values(shift_table, shift_ids)
    matrix = sketch.reshape(sketch.shape[0], -1)
    count = sources.shape[0]

    def one_shift(value):
        diag = (6.0 - kappa + value * mass)[None]
        center = 6.0 + value
        w0 = sources
        z0 = apply_operator(w0, diag)
        w1 = (z0 - center * w0) / 6.0
        z1 = apply_operator(w1, diag)
        w2 = (z1 - center * w1) / 6.0
        z2 = apply_operator(w2, diag)
        stacked = jnp.stack([w0, z0, z1, z2], axis=0).astype(jnp.bfloat16).reshape(4 * count, -1)
        sketched = lax.dot_general(matrix, stacked, (((1,), (1,)), ((), ())), preferred_element_type=jnp.float32)
        gram = gram_of(sketched.reshape(matrix.shape[0], 4, count))
        c0, c1, c2 = solve_small(gram)
        c0 = c0[:, None, None, None]
        c1 = c1[:, None, None, None]
        c2 = c2[:, None, None, None]
        solution = c0 * w0 + c1 * w1 + c2 * w2
        residual = w0 - c0 * z0 - c1 * z1 - c2 * z2
        return (solution, residual)
    solution, residual = lax.map(one_shift, sigma)
    return (solution, residual)
```

```python
import functools

import jax
import jax.numpy as jnp
from jax import lax
from jax.experimental import pallas as pl
from jax.experimental.pallas import tpu as pltpu
from jax.sharding import PartitionSpec as P

HALO = 3
LANES = 128
MID = 2.25
F32 = jnp.float32
BF16 = jnp.bfloat16
BASIS = 10
SPLIT = 6
IMAGES = ((0,), (1, 6), (2, 3, 7), (4, 5, 8, 9))
VMEM_SPEC = pl.BlockSpec(memory_space=pltpu.VMEM)
HBM_SPEC = pl.BlockSpec(memory_space=pltpu.HBM)
SMEM_SPEC = pl.BlockSpec(memory_space=pltpu.SMEM)
DMA = pltpu.SemaphoreType.DMA


def in_hbm(array):
    return pltpu.with_memory_space_constraint(array, pltpu.HBM)


def in_vmem(array):
    return pltpu.with_memory_space_constraint(array, pltpu.VMEM)


def remote(src, dst, send, recv, **where):
    return pltpu.make_async_remote_copy(
        src_ref=src, dst_ref=dst, send_sem=send, recv_sem=recv,
        device_id=where, device_id_type=pl.DeviceIdType.MESH,
    )


def signal(sem, **where):
    pl.semaphore_signal(sem, inc=1, device_id=where, device_id_type=pl.DeviceIdType.MESH)


def plane_of(ref, p, ny):
    return ref[pl.ds(p * ny, ny)]


def neighbour_sum(ref, p, ny):
    inner = plane_of(ref, p, ny)
    total = plane_of(ref, p - 1, ny) + plane_of(ref, p + 1, ny)
    none = jnp.zeros((1,) + inner.shape[1:], F32)
    total = total + jnp.concatenate([none, inner[:-1]], axis=0)
    total = total + jnp.concatenate([inner[1:], none], axis=0)
    lane = lax.broadcasted_iota(jnp.int32, inner.shape, 2)
    total = total + jnp.where(lane > 0, pltpu.roll(inner, 1, 2), 0.0)
    return total + jnp.where(lane < LANES - 1, pltpu.roll(inner, LANES - 1, 2), 0.0)


def edge_flag(p, planes, width, low, high):
    if p < width:
        return low
    return high if p >= planes - width else None


def masked(value, flag):
    return value if flag is None else value * flag


def edge_flags(me, n):
    return (me > 0).astype(F32), (me < n - 1).astype(F32)


def prepare_kernel(
    n, ny, src_hbm, kappa_hbm, mass_hbm, sketch_hbm,
    sketch_out, weights_out, wide_out, kappa_out, mass1,
    wide, kappa, mass, diag, g0, g1, h0, h1, h2,
    load_sem, in_sem, halo_send, halo_recv,
):
    me = lax.axis_index("dom")
    nb, rows = src_hbm.shape[0], src_hbm.shape[1]
    slab = rows // ny
    right, left = lax.rem(me + 1, n), lax.rem(me + n - 1, n)
    has_right, has_left = me < n - 1, me > 0
    depth = HALO * ny
    thin = (HALO - 1) * ny

    barrier = pltpu.get_barrier_semaphore()

    @pl.when(has_right)
    def _():
        signal(barrier, dom=right)

    @pl.when(has_left)
    def _():
        signal(barrier, dom=left)

    inputs = [
        pltpu.make_async_copy(src_hbm.at[b], wide.at[pl.ds(depth, rows), b], in_sem.at[b])
        for b in range(nb)
    ]
    inputs.append(pltpu.make_async_copy(kappa_hbm, kappa.at[pl.ds(thin, rows)], in_sem.at[nb]))
    inputs.append(pltpu.make_async_copy(mass_hbm, mass.at[pl.ds(thin, rows)], in_sem.at[nb + 1]))
    for copy in inputs:
        copy.start()

    def load(k):
        return pltpu.make_async_copy(sketch_hbm.at[:, k], sketch_out.at[k], load_sem.at[k])

    loads = sketch_hbm.shape[1]
    early = 4
    for k in range(early):
        load(k).start()
    for copy in inputs:
        copy.wait()

    def halo(which, side):
        ref, width = ((wide, depth), (kappa, thin), (mass, thin))[which]
        first, target, there = ((rows, 0, right), (width, width + rows, left))[side]
        return remote(
            ref.at[pl.ds(first, width)], ref.at[pl.ds(target, width)],
            halo_send.at[which, side], halo_recv.at[which, side], dom=there,
        )

    pl.semaphore_wait(barrier, has_right.astype(jnp.int32) + has_left.astype(jnp.int32))

    @pl.when(has_right)
    def _():
        for which in range(3):
            halo(which, 0).start()

    @pl.when(has_left)
    def _():
        for which in range(3):
            halo(which, 1).start()

    for k in range(early, loads):
        load(k).start()

    @pl.when(jnp.logical_not(has_left))
    def _():
        wide.reshape(wide.shape[0], nb, LANES)[pl.ds(0, depth)] = jnp.zeros((depth, nb, LANES), F32)
        kappa[pl.ds(0, thin)] = jnp.zeros((thin, 1, LANES), F32)
        mass[pl.ds(0, thin)] = jnp.zeros((thin, 1, LANES), F32)

    @pl.when(jnp.logical_not(has_right))
    def _():
        wide.reshape(wide.shape[0], nb, LANES)[pl.ds(depth + rows, depth)] = jnp.zeros(
            (depth, nb, LANES), F32
        )
        kappa[pl.ds(thin + rows, thin)] = jnp.zeros((thin, 1, LANES), F32)
        mass[pl.ds(thin + rows, thin)] = jnp.zeros((thin, 1, LANES), F32)

    @pl.when(has_left)
    def _():
        for which in range(3):
            halo(which, 0).wait_recv()

    @pl.when(has_right)
    def _():
        for which in range(3):
            halo(which, 1).wait_recv()

    full = (ny, nb, LANES)
    field = wide.reshape(wide.shape[0], nb, LANES)
    low, high = edge_flags(me, n)
    planes = slab + 2 * HALO
    for p in range(planes - 2):
        k = jnp.broadcast_to(kappa[pl.ds(p * ny, ny)], full)
        m = jnp.broadcast_to(mass[pl.ds(p * ny, ny)] - 1.0, full)
        diag[pl.ds(p * ny, ny)] = MID * m - k
        mass1[pl.ds(p * ny, ny)] = m
        kappa_out[pl.ds(p * ny, ny)] = k
    for p in range(planes):
        wide_out[pl.ds(p * ny, ny)] = plane_of(field, p, ny)

    for p in range(planes - 2):
        flag = edge_flag(p, planes - 2, 2, low, high)
        w = plane_of(field, p + 1, ny)
        out = pl.ds(p * ny, ny)
        g0[out] = masked(diag[out] * w - neighbour_sum(field, p + 1, ny), flag)
        g1[out] = mass1[out] * w
    for p in range(planes - 4):
        flag = edge_flag(p, planes - 4, 1, low, high)
        at, out = pl.ds((p + 1) * ny, ny), pl.ds(p * ny, ny)
        d, m = diag[at], mass1[at]
        u0, u1 = g0[at], g1[at]
        h0[out] = masked(d * u0 - neighbour_sum(g0, p + 1, ny), flag)
        h1[out] = masked(d * u1 - neighbour_sum(g1, p + 1, ny) + m * u0, flag)
        h2[out] = m * u1
    for p in range(slab):
        at, inner = pl.ds((p + 2) * ny, ny), pl.ds((p + 1) * ny, ny)
        d, m = diag[at], mass1[at]
        v0, v1, v2 = h0[inner], h1[inner], h2[inner]
        e0 = d * v0 - neighbour_sum(h0, p + 1, ny)
        e1 = d * v1 - neighbour_sum(h1, p + 1, ny) + m * v0
        e2 = d * v2 - neighbour_sum(h2, p + 1, ny) + m * v1
        e3 = m * v2
        first = jnp.concatenate(
            [plane_of(field, p + HALO, ny), g0[at], v0, v1, e0, e1], axis=1
        )
        second = jnp.concatenate([g1[at], v2, e2, e3], axis=1)
        high_part = first.astype(BF16)
        low_part = (first - high_part.astype(F32)).astype(BF16)
        columns = jnp.concatenate([high_part, second.astype(BF16), low_part], axis=1)
        pairs = ny // 2
        weights_out[pl.ds(p * pairs, pairs)] = columns.reshape(pairs, 2 * columns.shape[1], LANES)

    for k in range(loads):
        load(k).wait()

    @pl.when(has_right)
    def _():
        for which in range(3):
            halo(which, 0).wait_send()

    @pl.when(has_left)
    def _():
        for which in range(3):
            halo(which, 1).wait_send()


def solve_small(h_vals, entry):
    l00 = jnp.sqrt(entry[0][0])
    l10 = entry[1][0] / l00
    l20 = entry[2][0] / l00
    l11 = jnp.sqrt(entry[1][1] - l10 * l10)
    l21 = (entry[2][1] - l20 * l10) / l11
    l22 = jnp.sqrt(entry[2][2] - l20 * l20 - l21 * l21)
    f0 = h_vals[0] / l00
    f1 = (h_vals[1] - l10 * f0) / l11
    f2 = (h_vals[2] - l20 * f0 - l21 * f1) / l22
    c2 = f2 / l22
    c1 = (f1 - l21 * c2) / l11
    c0 = (f0 - l10 * c1 - l20 * c2) / l00
    return (c0, c1, c2)


def pair_lane(i, k):
    distance = (k - i) % BASIS
    if distance <= BASIS // 2:
        return BASIS * distance + i
    return BASIS * (BASIS - distance) + k


def coefficients(gram, sigma):
    tau, center = sigma - MID, sigma + 6.0

    def product(left, right):
        by_degree = {}
        for p, i in enumerate(IMAGES[left]):
            for q, k in enumerate(IMAGES[right]):
                at = pair_lane(i, k)
                column = gram[:, at : at + 1]
                by_degree[p + q] = by_degree[p + q] + column if p + q in by_degree else column
        top = max(by_degree)
        total = jnp.broadcast_to(by_degree[top], gram.shape)
        for degree in range(top - 1, -1, -1):
            total = total * tau + by_degree[degree]
        return total

    ww = [[product(i, k) if i <= k else None for k in range(4)] for i in range(4)]

    def between(i, k):
        total = ww[i][k]
        if i > 0:
            total = total + center * ww[i - 1][k]
        if k > 0:
            low = ww[min(i, k - 1)][max(i, k - 1)]
            if i > 0:
                low = low + center * ww[i - 1][k - 1]
            total = total + center * low
        return total

    scale = (1.0, 1.0, 1.0 / 6.0, 1.0 / 36.0)
    h_vals = [between(0, i) * scale[i] for i in (1, 2, 3)]
    entry = [[None] * 3 for _ in range(3)]
    for i in range(3):
        for k in range(i + 1):
            entry[i][k] = between(k + 1, i + 1) * (scale[i + 1] * scale[k + 1])
    ridge = 0.001 * (entry[0][0] + entry[1][1] + entry[2][2]) / 3.0 + 1.0
    for i in range(3):
        entry[i][i] = entry[i][i] + ridge
    c0, c1, c2 = solve_small(h_vals, entry)
    c1, c2 = c1 * (1.0 / 6.0), c2 * (1.0 / 36.0)
    return (c0, c1, c2, 1.0 - c0 * center, c0 + c1 * center, c1 + c2 * center)


def project_kernel(
    n, groups, ny, sketch_ref, weights_ref, own_ref, kappa_ref, mass1_ref, table_ref, ids_ref,
    fields_out, own_out, coeff_out,
    wide, step_ref, product, picked, near, first, second, out_buf, in_buf, rows_buf,
    z_send, z_recv, halo_send, halo_recv, rs_send, rs_recv, g_send, g_recv, s_send, s_recv,
):
    me = lax.axis_index("dom")
    group = lax.axis_index("shift")
    planes = own_ref.shape[0] // ny
    nb = own_ref.shape[1]
    slab = planes - 2 * HALO
    rows, depth = slab * ny, HALO * ny
    right, left = lax.rem(me + 1, n), lax.rem(me + n - 1, n)
    has_right, has_left = me < n - 1, me > 0
    shifts = ids_ref.shape[0]
    low, high = edge_flags(me, n)

    barrier = pltpu.get_barrier_semaphore()
    for t in range(1, n):
        signal(barrier, dom=lax.rem(me + t, n))
    for t in range(1, groups):
        signal(barrier, shift=lax.rem(group + t, groups))

    hops = []
    for k in range(1, groups // 2 + 1):
        for way in range(2):
            part = (0, slab)
            if 2 * k == groups:
                part = ((0, slab // 2), (slab // 2, slab - slab // 2))[way]
            hops.append((way, k, part))

    def shifted(way, k):
        return lax.rem(group + (k if way == 0 else groups - k), groups)

    def across(hop):
        way, k, (start, count) = hop
        at = pl.ds(depth + start * ny, count * ny)
        slot = group if k == 1 else shifted(1 - way, k - 1)
        src = own_ref.at[at] if k == 1 else wide.at[slot, at]
        return remote(
            src, wide.at[slot, at], z_send.at[way, k - 1], z_recv.at[way, k - 1],
            shift=shifted(way, 1),
        )

    def arrived(hop):
        way, k, _ = hop
        return shifted(1 - way, k)

    def halo(index, slot, side):
        start, target, there = ((rows, 0, right), (depth, depth + rows, left))[side]
        return remote(
            wide.at[slot, pl.ds(start, depth)], wide.at[slot, pl.ds(target, depth)],
            halo_send.at[index, side], halo_recv.at[index, side], dom=there,
        )

    def slot_of(index):
        if index == 2:
            return shifted(0, 2)
        return shifted(1 - index, 1)

    def send_halo(index):
        slot = slot_of(index)

        @pl.when(has_right)
        def _():
            halo(index, slot, 0).start()

        @pl.when(has_left)
        def _():
            halo(index, slot, 1).start()

    def take_halo(index):
        slot = slot_of(index)

        @pl.when(has_left)
        def _():
            halo(index, slot, 0).wait_recv()

        @pl.when(has_right)
        def _():
            halo(index, slot, 1).wait_recv()

        @pl.when(jnp.logical_not(has_left))
        def _():
            wide[slot, pl.ds(0, depth)] = jnp.zeros((depth, nb, LANES), F32)

        @pl.when(jnp.logical_not(has_right))
        def _():
            wide[slot, pl.ds(depth + rows, depth)] = jnp.zeros((depth, nb, LANES), F32)

    per = 2
    steps = sketch_ref.shape[0] // per

    def multiply(u):
        at = [u * per + i for i in range(per)]
        return lax.dot_general(
            jnp.concatenate([sketch_ref[k] for k in at], axis=1),
            jnp.concatenate([weights_ref[k] for k in at], axis=1),
            (((1,), (1,)), ((), ())), preferred_element_type=F32,
        )

    def accumulate(u, carry):
        product[...] += multiply(u)
        return carry

    product[...] = multiply(0)
    lax.fori_loop(1, steps // 2, accumulate, 0)
    pl.semaphore_wait(barrier, n - 1 + groups - 1)
    for hop in hops:
        if hop[1] == 1:
            across(hop).start()
    lax.fori_loop(steps // 2, steps, accumulate, 0)

    half = product.shape[1] // 2
    odd = lax.rem(lax.broadcasted_iota(jnp.int32, picked.shape, 0), 2) == 1
    picked[...] = jnp.where(odd, product[:, half:], product[:, :half])
    count = picked.shape[0] // 2
    turned = (picked[pl.ds(0, count, stride=2)] + picked[pl.ds(1, count, stride=2)]).T
    split, columns = SPLIT * nb, BASIS * nb
    sketched = jnp.concatenate([turned[:split] + turned[columns:], turned[split:columns]], axis=0)
    chunks = count // LANES
    flat_out = out_buf.reshape(chunks * columns, LANES)
    for r in range(chunks):
        flat_out[pl.ds(r * columns, columns)] = sketched[:, r * LANES : (r + 1) * LANES]
    parts = n // nb
    span = chunks // parts

    def piece(dest):
        return out_buf.at[pl.ds(dest // nb * span, span), :, lax.rem(dest, nb)]

    def scatter(t):
        dest = lax.rem(me + t, n)
        return remote(
            piece(dest), in_buf.at[me, :, pl.ds(0, BASIS)], rs_send.at[t - 1], rs_recv.at[t - 1],
            dom=dest,
        )

    for t in range(1, n):
        scatter(t).start()
    in_buf[me, :, pl.ds(0, BASIS)] = piece(me)[...]

    for hop in hops:
        if hop[1] == 1:
            across(hop).wait_recv()
    for hop in hops:
        if hop[1] == 2:
            across(hop).start()
    for index in range(2):
        send_halo(index)

    def images(field, slot):
        for p in range(planes - 2):
            near[pl.ds(p * ny, ny)] = neighbour_sum(field, p + 1, ny)

        def one_shift(j, carry):
            for p in range(planes - 2):
                at = pl.ds(p * ny, ny)
                flag = edge_flag(p, planes - 2, 2, low, high)
                first[at] = masked(step_ref[j, at] * plane_of(field, p + 1, ny) - near[at], flag)
            for p in range(planes - 4):
                at = pl.ds((p + 1) * ny, ny)
                flag = edge_flag(p, planes - 4, 1, low, high)
                second[pl.ds(p * ny, ny)] = masked(
                    step_ref[j, at] * first[at] - neighbour_sum(first, p + 1, ny), flag
                )
            for p in range(slab):
                at, inner, out = pl.ds((p + 2) * ny, ny), pl.ds((p + 1) * ny, ny), pl.ds(p * ny, ny)
                fields_out[slot, j, 0, out] = first[at]
                fields_out[slot, j, 1, out] = second[inner]
                fields_out[slot, j, 2, out] = (
                    step_ref[j, at] * second[inner] - neighbour_sum(second, p + 1, ny)
                )
            return carry

        lax.fori_loop(0, shifts, one_shift, 0)
        for p in range(slab):
            own_out[slot, pl.ds(p * ny, ny)] = plane_of(field, p + HALO, ny)

    for j in range(shifts):
        step_ref[j] = table_ref[ids_ref[j]] * mass1_ref[...] - kappa_ref[...]
    images(own_ref, group)

    flat_in = in_buf.reshape(n * span * in_buf.shape[2], LANES)
    tall = span * in_buf.shape[2]
    for t in range(1, n):
        scatter(t).wait_recv()
    total = flat_in[pl.ds(0, tall)]
    for t in range(1, n):
        total = total + flat_in[pl.ds(t * tall, tall)]
    lane = lax.broadcasted_iota(jnp.int32, (BASIS, LANES), 1)
    place = lax.broadcasted_iota(jnp.int32, (BASIS, LANES), 0)
    views = [total[r * in_buf.shape[2] :][:BASIS] for r in range(span)]
    twice = [jnp.concatenate([view, view], axis=0) for view in views]
    packed = jnp.zeros((BASIS, LANES), F32)
    for d in range(BASIS // 2 + 1):
        terms = sum(view * wrap[d : d + BASIS] for view, wrap in zip(views, twice))
        packed = jnp.where(lane == place + BASIS * d, jnp.sum(terms, axis=1, keepdims=True), packed)
    rows_buf[group, me] = jnp.sum(packed, axis=0, keepdims=True)

    def share(t):
        return remote(
            rows_buf.at[group, me], rows_buf.at[group, me], g_send.at[t - 1], g_recv.at[t - 1],
            dom=lax.rem(me + t, n),
        )

    for t in range(1, n):
        share(t).start()
    for hop in hops:
        if hop[1] == 2:
            across(hop).wait_recv()
    send_halo(2)
    take_halo(0)
    images(wide.at[slot_of(0)], slot_of(0))
    take_halo(1)
    images(wide.at[slot_of(1)], slot_of(1))
    for t in range(1, n):
        share(t).wait_recv()

    def spread(t):
        return remote(
            rows_buf.at[group], rows_buf.at[group], s_send.at[t - 1], s_recv.at[t - 1],
            shift=lax.rem(group + t, groups),
        )

    for t in range(1, groups):
        spread(t).start()
    take_halo(2)
    images(wide.at[slot_of(2)], slot_of(2))
    for t in range(1, groups):
        spread(t).wait_recv()

    lane_row = lax.broadcasted_iota(jnp.int32, (1, LANES), 1)
    sigma = jnp.full((1, LANES), MID, F32)
    for j in range(shifts):
        sigma = jnp.where(lane_row == j, table_ref[ids_ref[j]], sigma)
    flat_rows = rows_buf.reshape(groups * n, LANES)
    gram = []
    for g in range(groups):
        block = flat_rows[pl.ds(g * n, n)]
        gram.append(sum(block[q * nb : (q + 1) * nb] for q in range(parts)))
    solved = coefficients(jnp.concatenate(gram, axis=0), sigma)
    for i, value in enumerate(solved):
        for j in range(shifts):
            spreaded = jnp.broadcast_to(value[:, j : j + 1], value.shape)
            coeff_out[j, i] = spreaded.reshape(groups, nb, LANES)

    for index in range(3):
        slot = slot_of(index)

        @pl.when(has_right)
        def _():
            halo(index, slot, 0).wait_send()

        @pl.when(has_left)
        def _():
            halo(index, slot, 1).wait_send()

    for hop in hops:
        across(hop).wait_send()
    for t in range(1, n):
        scatter(t).wait_send()
        share(t).wait_send()
    for t in range(1, groups):
        spread(t).wait_send()


def combine_kernel(fields_ref, own_ref, coeff_ref, sol_hbm, res_hbm, sol_buf, res_buf, sem):
    groups, shifts = fields_ref.shape[0], fields_ref.shape[1]
    rows, nb = fields_ref.shape[3], fields_ref.shape[4]

    def copies(g, j):
        out = []
        for which, (buf, hbm) in enumerate(((sol_buf, sol_hbm), (res_buf, res_hbm))):
            for b in range(nb):
                out.append(
                    pltpu.make_async_copy(
                        buf.at[g, j, :, b], hbm.at[j, g * nb + b], sem.at[which, g, j, b]
                    )
                )
        return out

    def one(u, carry):
        g, j = u // shifts, lax.rem(u, shifts)
        c = [coeff_ref[j, i, g][None] for i in range(6)]
        w0 = own_ref[g]
        w1, w2, w3 = (fields_ref[g, j, i] for i in range(3))
        sol_buf.at[g, j].reshape(rows, nb, LANES)[...] = c[0] * w0 + c[1] * w1 + c[2] * w2
        res_buf.at[g, j].reshape(rows, nb, LANES)[...] = (
            c[3] * w0 - c[4] * w1 - c[5] * w2 - c[2] * w3
        )
        for copy in copies(g, j):
            copy.start()
        return carry

    lax.fori_loop(0, groups * shifts, one, 0)

    def finish(u, carry):
        for copy in copies(u // shifts, lax.rem(u, shifts)):
            copy.wait()
        return carry

    lax.fori_loop(0, groups * shifts, finish, 0)


def on_device(sources, kappa, mass, shift_table, shift_ids, sketch):
    n, groups = lax.axis_size("dom"), lax.axis_size("shift")
    nb, slab, ny = sources.shape[0], sources.shape[1], sources.shape[2]
    shifts = shift_ids.shape[0]
    sk = sketch.shape[0]
    rows = slab * ny
    planes = slab + 2 * HALO
    wide_rows, inner = planes * ny, (planes - 2) * ny
    pairs = rows // 2
    weights = 2 * (BASIS + SPLIT) * nb
    vec = (nb, LANES)
    sketch, weight, wide, kappa, mass = pl.pallas_call(
        functools.partial(prepare_kernel, n, ny),
        out_shape=(
            pltpu.VMEM((pairs, sk, 2, LANES), BF16),
            pltpu.VMEM((pairs, weights, LANES), BF16),
            pltpu.VMEM((wide_rows,) + vec, F32),
            pltpu.VMEM((inner,) + vec, F32),
            pltpu.VMEM((inner,) + vec, F32),
        ),
        in_specs=[HBM_SPEC] * 4,
        out_specs=(VMEM_SPEC,) * 5,
        scratch_shapes=[
            pltpu.VMEM((wide_rows, nb, 1, LANES), F32),
            pltpu.VMEM((inner, 1, LANES), F32),
            pltpu.VMEM((inner, 1, LANES), F32),
            pltpu.VMEM((inner,) + vec, F32),
            pltpu.VMEM((inner,) + vec, F32),
            pltpu.VMEM((inner,) + vec, F32),
            pltpu.VMEM((inner - 2 * ny,) + vec, F32),
            pltpu.VMEM((inner - 2 * ny,) + vec, F32),
            pltpu.VMEM((inner - 2 * ny,) + vec, F32),
            DMA((pairs,)), DMA((nb + 2,)), DMA((3, 2)), DMA((3, 2)),
        ],
        compiler_params=pltpu.CompilerParams(
            collective_id=0, has_side_effects=True, vmem_limit_bytes=16 << 20
        ),
        name="prepare",
    )(
        in_hbm(sources.reshape(nb, rows, 1, LANES)), in_hbm(kappa.reshape(rows, 1, LANES)),
        in_hbm(mass.reshape(rows, 1, LANES)), in_hbm(sketch.reshape(sk, pairs, 2, LANES)),
    )
    parts = n // nb
    span = sk // LANES // parts
    fields, own, coeff = pl.pallas_call(
        functools.partial(project_kernel, n, groups, ny),
        out_shape=(
            pltpu.VMEM((groups, shifts, 3, rows) + vec, F32),
            pltpu.VMEM((groups, rows) + vec, F32),
            pltpu.VMEM((shifts, 6, groups) + vec, F32),
        ),
        in_specs=[VMEM_SPEC] * 5 + [SMEM_SPEC] * 2,
        out_specs=(VMEM_SPEC,) * 3,
        scratch_shapes=[
            pltpu.VMEM((groups, wide_rows) + vec, F32),
            pltpu.VMEM((shifts, inner) + vec, F32),
            pltpu.VMEM((2 * sk, weights), F32),
            pltpu.VMEM((2 * sk, weights // 2), F32),
            pltpu.VMEM((inner,) + vec, F32),
            pltpu.VMEM((inner,) + vec, F32),
            pltpu.VMEM((inner - 2 * ny,) + vec, F32),
            pltpu.VMEM((sk // LANES, BASIS, nb, 1, LANES), F32),
            pltpu.VMEM((n, span, 16, 1, LANES), F32),
            pltpu.VMEM((groups, n, 1, LANES), F32),
            DMA((2, groups // 2)), DMA((2, groups // 2)),
            DMA((3, 2)), DMA((3, 2)),
            DMA((n - 1,)), DMA((n - 1,)),
            DMA((n - 1,)), DMA((n - 1,)),
            DMA((groups - 1,)), DMA((groups - 1,)),
        ],
        compiler_params=pltpu.CompilerParams(
            collective_id=1, has_side_effects=True, vmem_limit_bytes=16 << 20
        ),
        name="project",
    )(
        in_vmem(sketch.reshape(pairs, 2 * sk, LANES)), in_vmem(weight), in_vmem(wide), in_vmem(kappa),
        in_vmem(mass), shift_table, shift_ids,
    )

    out = pltpu.HBM((shifts, groups * nb, rows, 1, LANES), F32)
    buf = pltpu.VMEM((groups, shifts, rows, nb, 1, LANES), F32)
    solution, residual = pl.pallas_call(
        combine_kernel,
        out_shape=(out, out),
        in_specs=[VMEM_SPEC] * 3,
        out_specs=(HBM_SPEC,) * 2,
        scratch_shapes=[buf, buf, DMA((2, groups, shifts, nb))],
        compiler_params=pltpu.CompilerParams(vmem_limit_bytes=16 << 20),
        name="combine",
    )(in_vmem(fields), in_vmem(own), in_vmem(coeff))
    shape = (shifts, groups * nb, slab, ny, LANES)
    return solution.reshape(shape), residual.reshape(shape)


def solution(mesh):
    placed = (
        P("shift", "dom", None, None),
        P("dom", None, None),
        P("dom", None, None),
        P(),
        P("shift"),
        P(None, "dom", None, None),
    )
    return jax.shard_map(
        on_device,
        mesh=mesh,
        in_specs=placed,
        out_specs=(P("shift", None, "dom", None, None), P("shift", None, "dom", None, None)),
        check_vma=False,
    )
```

```python
import functools

import jax
import jax.numpy as jnp
from jax import lax
from jax.experimental import pallas as pl
from jax.experimental.pallas import tpu as pltpu
from jax.sharding import PartitionSpec as P

HALO = 3
LANES = 128
MID = 2.25
F32 = jnp.float32
BF16 = jnp.bfloat16
BASIS = 10
SPLIT = 6
IMAGES = ((0,), (1, 6), (2, 3, 7), (4, 5, 8, 9))
VMEM_SPEC = pl.BlockSpec(memory_space=pltpu.VMEM)
HBM_SPEC = pl.BlockSpec(memory_space=pltpu.HBM)
SMEM_SPEC = pl.BlockSpec(memory_space=pltpu.SMEM)
DMA = pltpu.SemaphoreType.DMA


def in_hbm(array):
    return pltpu.with_memory_space_constraint(array, pltpu.HBM)


def in_vmem(array):
    return pltpu.with_memory_space_constraint(array, pltpu.VMEM)


def remote(src, dst, send, recv, **where):
    return pltpu.make_async_remote_copy(
        src_ref=src, dst_ref=dst, send_sem=send, recv_sem=recv,
        device_id=where, device_id_type=pl.DeviceIdType.MESH,
    )


def signal(sem, **where):
    pl.semaphore_signal(sem, inc=1, device_id=where, device_id_type=pl.DeviceIdType.MESH)


def wrapped(index, size):
    return jnp.where(index >= size, index - size, index)


def drain(ref, sem):
    pltpu.make_async_copy(ref, ref, sem).wait()


def plane_of(ref, p, ny):
    return ref[pl.ds(p * ny, ny)]


def neighbour_sum(ref, p, ny):
    inner = plane_of(ref, p, ny)
    total = plane_of(ref, p - 1, ny) + plane_of(ref, p + 1, ny)
    none = jnp.zeros((1,) + inner.shape[1:], F32)
    total = total + jnp.concatenate([none, inner[:-1]], axis=0)
    total = total + jnp.concatenate([inner[1:], none], axis=0)
    lane = lax.broadcasted_iota(jnp.int32, inner.shape, 2)
    total = total + jnp.where(lane > 0, pltpu.roll(inner, 1, 2), 0.0)
    return total + jnp.where(lane < LANES - 1, pltpu.roll(inner, LANES - 1, 2), 0.0)


def edge_flag(p, planes, width, low, high):
    if p < width:
        return low
    return high if p >= planes - width else None


def masked(value, flag):
    return value if flag is None else value * flag


def edge_flags(me, n):
    return (me > 0).astype(F32), (me < n - 1).astype(F32)


def prepare_kernel(
    n, groups, ny, src_hbm, kappa_hbm, mass_hbm, sketch_hbm,
    sketch_out, weights_out, wide, passed_out, kappa_out, mass1,
    coef, diag, g0, g1, h0, h1, h2,
    load_sem, in_sem, wide_send, wide_recv, coef_send, coef_recv, z_send, z_recv,
):
    me = lax.axis_index("dom")
    group = lax.axis_index("shift")
    nb, rows = src_hbm.shape[0], src_hbm.shape[1]
    slab = rows // ny
    right, left = wrapped(me + 1, n), wrapped(me + n - 1, n)
    up, down = wrapped(group + 1, groups), wrapped(group + groups - 1, groups)
    has_right, has_left = me < n - 1, me > 0
    depth = HALO * ny
    thin = (HALO - 1) * ny
    planes = slab + 2 * HALO

    barrier = pltpu.get_barrier_semaphore()
    inputs = [
        pltpu.make_async_copy(src_hbm.at[b], wide.at[pl.ds(depth, rows), b], in_sem.at[0])
        for b in range(nb)
    ]
    inputs.append(pltpu.make_async_copy(kappa_hbm, coef.at[0, pl.ds(thin, rows)], in_sem.at[1]))
    inputs.append(pltpu.make_async_copy(mass_hbm, coef.at[1, pl.ds(thin, rows)], in_sem.at[1]))
    for copy in inputs:
        copy.start()

    @pl.when(has_right)
    def _():
        signal(barrier, dom=right)

    @pl.when(has_left)
    def _():
        signal(barrier, dom=left)

    signal(barrier, shift=up)
    signal(barrier, shift=down)

    def load(k):
        return pltpu.make_async_copy(sketch_hbm.at[:, k], sketch_out.at[k], load_sem.at[0])

    loads = sketch_hbm.shape[1]
    early = 6
    for k in range(early):
        load(k).start()
    drain(wide.at[pl.ds(depth, rows)], in_sem.at[0])
    drain(coef.at[:, pl.ds(thin, rows)], in_sem.at[1])

    def wide_halo(k, side):
        first, target, there = (
            (depth + rows - (k + 1) * ny, depth - (k + 1) * ny, right),
            (depth + k * ny, depth + rows + k * ny, left),
        )[side]
        return remote(
            wide.at[pl.ds(first, ny)], wide.at[pl.ds(target, ny)],
            wide_send.at[side], wide_recv.at[k, side], dom=there,
        )

    def coef_halo(side):
        first, target, there = ((rows, 0, right), (thin, thin + rows, left))[side]
        return remote(
            coef.at[:, pl.ds(first, thin)], coef.at[:, pl.ds(target, thin)],
            coef_send.at[side], coef_recv.at[side], dom=there,
        )

    def pass_on(way):
        count = passed_out.shape[1]
        there = (up, down)[way]
        return remote(
            wide.at[pl.ds(depth + way * count, count)], passed_out.at[way],
            z_send.at[0], z_recv.at[way], shift=there,
        )

    pl.semaphore_wait(barrier, has_right.astype(jnp.int32) + has_left.astype(jnp.int32) + 2)

    def send_halo(side):
        wide_halo(0, side).start()
        coef_halo(side).start()
        for k in range(1, HALO):
            wide_halo(k, side).start()

    pl.when(has_right)(lambda: send_halo(0))
    pl.when(has_left)(lambda: send_halo(1))
    for way in range(2):
        pass_on(way).start()
    for k in range(early, loads):
        load(k).start()

    field = wide.reshape(wide.shape[0], nb, LANES)

    @pl.when(jnp.logical_not(has_left))
    def _():
        field[pl.ds(0, depth)] = jnp.zeros((depth, nb, LANES), F32)
        coef[:, pl.ds(0, thin)] = jnp.zeros((2, thin, 1, LANES), F32)

    @pl.when(jnp.logical_not(has_right))
    def _():
        field[pl.ds(depth + rows, depth)] = jnp.zeros((depth, nb, LANES), F32)
        coef[:, pl.ds(thin + rows, thin)] = jnp.zeros((2, thin, 1, LANES), F32)

    full = (ny, nb, LANES)
    low, high = edge_flags(me, n)

    def factors(p):
        at = pl.ds(p * ny, ny)
        k = jnp.broadcast_to(coef[0, at], full)
        m = jnp.broadcast_to(coef[1, at] - 1.0, full)
        diag[at] = MID * m - k
        mass1[at] = m
        kappa_out[at] = k

    def level1(p):
        flag = edge_flag(p, planes - 2, 2, low, high)
        w = plane_of(field, p + 1, ny)
        out = pl.ds(p * ny, ny)
        g0[out] = masked(diag[out] * w - neighbour_sum(field, p + 1, ny), flag)
        g1[out] = mass1[out] * w

    def level2(p):
        flag = edge_flag(p, planes - 4, 1, low, high)
        at, out = pl.ds((p + 1) * ny, ny), pl.ds(p * ny, ny)
        d, m = diag[at], mass1[at]
        u0, u1 = g0[at], g1[at]
        h0[out] = masked(d * u0 - neighbour_sum(g0, p + 1, ny), flag)
        h1[out] = masked(d * u1 - neighbour_sum(g1, p + 1, ny) + m * u0, flag)
        h2[out] = m * u1

    def level3(p):
        at, inner = pl.ds((p + 2) * ny, ny), pl.ds((p + 1) * ny, ny)
        d, m = diag[at], mass1[at]
        v0, v1, v2 = h0[inner], h1[inner], h2[inner]
        e0 = d * v0 - neighbour_sum(h0, p + 1, ny)
        e1 = d * v1 - neighbour_sum(h1, p + 1, ny) + m * v0
        e2 = d * v2 - neighbour_sum(h2, p + 1, ny) + m * v1
        e3 = m * v2
        first = jnp.concatenate(
            [plane_of(field, p + HALO, ny), g0[at], v0, v1, e0, e1], axis=1
        )
        second = jnp.concatenate([g1[at], v2, e2, e3], axis=1)
        high_part = first.astype(BF16)
        low_part = (first - high_part.astype(F32)).astype(BF16)
        columns = jnp.concatenate([high_part, second.astype(BF16), low_part], axis=1)
        pairs = ny // 2
        weights_out[pl.ds(p * pairs, pairs)] = columns.reshape(pairs, 2 * columns.shape[1], LANES)

    done = [set(), set(), set(), set()]

    def advance(reach):
        ready = set(range(HALO - reach, planes - HALO + reach))
        if reach != 1:
            coefs = range(2, planes - 4) if reach == 0 else (0, 1, planes - 4, planes - 3)
            for p in (coefs if reach in (0, 2) else ()):
                factors(p)
        usable = range(2, planes - 4) if reach < 2 else range(planes - 2)
        for p in range(planes - 2):
            if p not in done[1] and {p, p + 1, p + 2} <= ready and p in usable:
                level1(p)
                done[1].add(p)
        for p in range(planes - 4):
            if p not in done[2] and {p, p + 1, p + 2} <= done[1]:
                level2(p)
                done[2].add(p)
        for p in range(slab):
            if p not in done[3] and {p, p + 1, p + 2} <= done[2]:
                level3(p)
                done[3].add(p)

    advance(0)
    pl.when(has_left)(lambda: wide_halo(0, 0).wait_recv())
    pl.when(has_right)(lambda: wide_halo(0, 1).wait_recv())
    advance(1)

    def take(side):
        coef_halo(side).wait_recv()
        wide_halo(1, side).wait_recv()

    pl.when(has_left)(lambda: take(0))
    pl.when(has_right)(lambda: take(1))
    advance(2)
    pl.when(has_left)(lambda: wide_halo(2, 0).wait_recv())
    pl.when(has_right)(lambda: wide_halo(2, 1).wait_recv())
    advance(3)
    for way in range(2):
        pass_on(way).wait_recv()
    drain(sketch_out, load_sem.at[0])

    def sent(side):
        drain(wide.at[pl.ds(0, depth)], wide_send.at[side])
        drain(coef.at[:, pl.ds(0, thin)], coef_send.at[side])

    pl.when(has_right)(lambda: sent(0))
    pl.when(has_left)(lambda: sent(1))
    drain(wide.at[pl.ds(depth, rows)], z_send.at[0])


def solve_small(h_vals, entry):
    l00 = jnp.sqrt(entry[0][0])
    l10 = entry[1][0] / l00
    l20 = entry[2][0] / l00
    l11 = jnp.sqrt(entry[1][1] - l10 * l10)
    l21 = (entry[2][1] - l20 * l10) / l11
    l22 = jnp.sqrt(entry[2][2] - l20 * l20 - l21 * l21)
    f0 = h_vals[0] / l00
    f1 = (h_vals[1] - l10 * f0) / l11
    f2 = (h_vals[2] - l20 * f0 - l21 * f1) / l22
    c2 = f2 / l22
    c1 = (f1 - l21 * c2) / l11
    c0 = (f0 - l10 * c1 - l20 * c2) / l00
    return (c0, c1, c2)


def pair_lane(i, k):
    distance = (k - i) % BASIS
    if distance <= BASIS // 2:
        return BASIS * distance + i
    return BASIS * (BASIS - distance) + k


def coefficients(gram, sigma):
    tau, center = sigma - MID, sigma + 6.0

    def product(left, right):
        by_degree = {}
        for p, i in enumerate(IMAGES[left]):
            for q, k in enumerate(IMAGES[right]):
                at = pair_lane(i, k)
                column = gram[:, at : at + 1]
                by_degree[p + q] = by_degree[p + q] + column if p + q in by_degree else column
        top = max(by_degree)
        total = jnp.broadcast_to(by_degree[top], gram.shape)
        for degree in range(top - 1, -1, -1):
            total = total * tau + by_degree[degree]
        return total

    ww = [[product(i, k) if i <= k else None for k in range(4)] for i in range(4)]

    def between(i, k):
        total = ww[i][k]
        if i > 0:
            total = total + center * ww[i - 1][k]
        if k > 0:
            low = ww[min(i, k - 1)][max(i, k - 1)]
            if i > 0:
                low = low + center * ww[i - 1][k - 1]
            total = total + center * low
        return total

    scale = (1.0, 1.0, 1.0 / 6.0, 1.0 / 36.0)
    h_vals = [between(0, i) * scale[i] for i in (1, 2, 3)]
    entry = [[None] * 3 for _ in range(3)]
    for i in range(3):
        for k in range(i + 1):
            entry[i][k] = between(k + 1, i + 1) * (scale[i + 1] * scale[k + 1])
    ridge = 0.001 * (entry[0][0] + entry[1][1] + entry[2][2]) / 3.0 + 1.0
    for i in range(3):
        entry[i][i] = entry[i][i] + ridge
    c0, c1, c2 = solve_small(h_vals, entry)
    c1, c2 = c1 * (1.0 / 6.0), c2 * (1.0 / 36.0)
    return (c0, c1, c2, 1.0 - c0 * center, c0 + c1 * center, c1 + c2 * center)


def project_kernel(
    n, groups, ny, sketch_ref, weights_ref, own_ref, passed_ref, kappa_ref, mass1_ref, table_ref, ids_ref,
    fields_out, own_out, coeff_out,
    wide, step_ref, picked, near, first, second, out_buf, in_buf, rows_buf,
    z_send, z_recv, halo_send, halo_recv, rs_send, rs_recv, g_send, g_recv, s_send, s_recv,
):
    me = lax.axis_index("dom")
    group = lax.axis_index("shift")
    planes = own_ref.shape[0] // ny
    nb = own_ref.shape[1]
    slab = planes - 2 * HALO
    rows, depth = slab * ny, HALO * ny
    right, left = wrapped(me + 1, n), wrapped(me + n - 1, n)
    around = [group] + [wrapped(group + t, groups) for t in range(1, groups)]
    up, down = around[1], around[groups - 1]
    has_right, has_left = me < n - 1, me > 0
    shifts = ids_ref.shape[0]
    low, high = edge_flags(me, n)

    barrier = pltpu.get_barrier_semaphore()
    for t in range(1, n):
        signal(barrier, dom=wrapped(me + t, n))
    for t in range(1, groups):
        signal(barrier, shift=around[t])

    slots = (down, up, around[groups // 2])
    half = passed_ref.shape[1]

    def across(way):
        at = pl.ds(depth + (1 - way) * half, half)
        return remote(
            own_ref.at[at], wide.at[way, at], z_send.at[0], z_recv.at[way], shift=(up, down)[way]
        )

    def beyond(way):
        return remote(
            passed_ref.at[way], wide.at[2, pl.ds(depth + way * half, half)],
            z_send.at[0], z_recv.at[2], shift=(up, down)[way],
        )

    def halo(index, side, src, first_plane, count):
        target = ((first_plane - (slab - HALO)) * ny, depth + rows + first_plane * ny)[side]
        return remote(
            src, wide.at[index, pl.ds(target, count * ny)],
            halo_send.at[side], halo_recv.at[index, side], dom=(right, left)[side],
        )

    def planes_for(side):
        return range(slab - HALO, slab) if side == 0 else range(HALO)

    def early_halo(index, side):
        held = range(index * slab // 2, (index + 1) * slab // 2)
        mine = [p for p in planes_for(side) if p in held]
        at = pl.ds((mine[0] - held[0]) * ny, len(mine) * ny)
        return halo(index, side, passed_ref.at[index, at], mine[0], len(mine))

    def late_halo(index, side):
        held = range((1 - index) * slab // 2, (2 - index) * slab // 2)
        if index == 2:
            held = range(slab)
        mine = [p for p in planes_for(side) if p in held]
        at = pl.ds(depth + mine[0] * ny, len(mine) * ny)
        return halo(index, side, wide.at[index, at], mine[0], len(mine))

    def to_both(start):
        pl.when(has_right)(lambda: start(0))
        pl.when(has_left)(lambda: start(1))

    def take_halo(index):
        def take(side):
            drain(wide.at[index, pl.ds(0, depth)], halo_recv.at[index, side])

        pl.when(has_left)(lambda: take(0))
        pl.when(has_right)(lambda: take(1))

    steps = sketch_ref.shape[0] // 2
    tall = sketch_ref.shape[1] // 2

    def stage(u):
        tile = jnp.concatenate([weights_ref[2 * u], weights_ref[2 * u + 1]], axis=1)
        for unit in range(2):
            pltpu.matmul_push_rhs(tile, 0, unit, transpose=True)

    def multiply(accs):
        def accumulate(u):
            for unit in range(2):
                at = pl.ds(unit * tall, tall)
                part = jnp.concatenate([sketch_ref[2 * u, at], sketch_ref[2 * u + 1, at]], axis=1)
                pltpu.matmul_acc_lhs(accs[unit], part, load_staged_rhs=0)

        def step(u, carry):
            accumulate(u)
            stage(u + 1)
            return carry

        for acc in accs:
            pltpu.matmul_pop(acc)
        stage(0)
        lax.fori_loop(0, steps // 2, step, 0)
        pl.semaphore_wait(barrier, n - 1 + groups - 1)
        for way in range(2):
            across(way).start()
        for index in range(2):
            to_both(lambda side: early_halo(index, side).start())
        for way in range(2):
            beyond(way).start()
        lax.fori_loop(steps // 2, steps - 1, step, 0)
        accumulate(steps - 1)
        odd = lax.rem(lax.broadcasted_iota(jnp.int32, (tall, LANES), 0), 2) == 1
        for unit in range(2):
            value = pltpu.matmul_pop(accs[unit])
            picked[pl.ds(unit * tall, tall)] = jnp.where(odd, value[:, LANES:], value[:, :LANES])

    pl.run_scoped(
        lambda *accs: multiply(accs),
        pltpu.ACC(0)((tall, 2 * LANES), F32), pltpu.ACC(1)((tall, 2 * LANES), F32),
    )
    count = picked.shape[0] // 2
    turned = (picked[pl.ds(0, count, stride=2)] + picked[pl.ds(1, count, stride=2)]).T
    split, columns = SPLIT * nb, BASIS * nb
    sketched = jnp.concatenate([turned[:split] + turned[columns:], turned[split:columns]], axis=0)
    chunks = count // LANES
    flat_out = out_buf.reshape(chunks * columns, LANES)
    for r in range(chunks):
        flat_out[pl.ds(r * columns, columns)] = sketched[:, r * LANES : (r + 1) * LANES]
    parts = n // nb
    span = chunks // parts

    def piece(dest):
        return out_buf.at[pl.ds(dest // nb * span, span), :, lax.rem(dest, nb)]

    def scatter(t):
        dest = wrapped(me + t, n)
        return remote(
            piece(dest), in_buf.at[me, :, pl.ds(0, BASIS)], rs_send.at[0], rs_recv.at[0], dom=dest
        )

    for t in range(1, n):
        scatter(t).start()
    in_buf[me, :, pl.ds(0, BASIS)] = piece(me)[...]

    def clear(at):
        for index in range(groups - 1):
            wide[index, at] = jnp.zeros((depth, nb, LANES), F32)

    pl.when(jnp.logical_not(has_left))(lambda: clear(pl.ds(0, depth)))
    pl.when(jnp.logical_not(has_right))(lambda: clear(pl.ds(depth + rows, depth)))
    for index in range(2):
        wide[index, pl.ds(depth + index * half, half)] = passed_ref[index]
    for j in range(shifts):
        step_ref[j] = table_ref[ids_ref[j]] * mass1_ref[...] - kappa_ref[...]

    def images(field, slot):
        for p in range(planes - 2):
            near[pl.ds(p * ny, ny)] = neighbour_sum(field, p + 1, ny)

        def one_shift(j, carry):
            for p in range(planes - 2):
                at = pl.ds(p * ny, ny)
                flag = edge_flag(p, planes - 2, 2, low, high)
                first[at] = masked(step_ref[j, at] * plane_of(field, p + 1, ny) - near[at], flag)
            for p in range(planes - 4):
                at = pl.ds((p + 1) * ny, ny)
                flag = edge_flag(p, planes - 4, 1, low, high)
                second[pl.ds(p * ny, ny)] = masked(
                    step_ref[j, at] * first[at] - neighbour_sum(first, p + 1, ny), flag
                )
            for p in range(slab):
                at, inner, out = pl.ds((p + 2) * ny, ny), pl.ds((p + 1) * ny, ny), pl.ds(p * ny, ny)
                fields_out[slot, j, 0, out] = first[at]
                fields_out[slot, j, 1, out] = second[inner]
                fields_out[slot, j, 2, out] = (
                    step_ref[j, at] * second[inner] - neighbour_sum(second, p + 1, ny)
                )
            return carry

        lax.fori_loop(0, shifts, one_shift, 0)
        for p in range(slab):
            own_out[slot, pl.ds(p * ny, ny)] = plane_of(field, p + HALO, ny)

    images(own_ref, group)
    for way in range(2):
        across(way).wait_recv()
        to_both(lambda side: late_halo(way, side).start())

    peers = pl.ds(0, n - 1)
    drain(in_buf.at[peers, :, pl.ds(0, BASIS)], rs_recv.at[0])
    flat_in = in_buf.reshape(n * span * in_buf.shape[2], LANES)
    tile = span * in_buf.shape[2]
    total = flat_in[pl.ds(0, tile)]
    for t in range(1, n):
        total = total + flat_in[pl.ds(t * tile, tile)]
    lane = lax.broadcasted_iota(jnp.int32, (BASIS, LANES), 1)
    place = lax.broadcasted_iota(jnp.int32, (BASIS, LANES), 0)
    views = [total[r * in_buf.shape[2] :][:BASIS] for r in range(span)]
    twice = [jnp.concatenate([view, view], axis=0) for view in views]
    packed = jnp.zeros((BASIS, LANES), F32)
    for d in range(BASIS // 2 + 1):
        terms = sum(view * wrap[d : d + BASIS] for view, wrap in zip(views, twice))
        packed = jnp.where(lane == place + BASIS * d, jnp.sum(terms, axis=1, keepdims=True), packed)
    rows_buf[group, me] = jnp.sum(packed, axis=0, keepdims=True)

    def share(t):
        return remote(
            rows_buf.at[group, me], rows_buf.at[group, me], g_send.at[0], g_recv.at[0],
            dom=wrapped(me + t, n),
        )

    for t in range(1, n):
        share(t).start()
    drain(wide.at[2, pl.ds(depth, rows)], z_recv.at[2])
    to_both(lambda side: late_halo(2, side).start())
    take_halo(0)
    images(wide.at[0], slots[0])
    take_halo(1)
    images(wide.at[1], slots[1])
    drain(rows_buf.at[0, peers], g_recv.at[0])

    def spread(t):
        return remote(
            rows_buf.at[group], rows_buf.at[group], s_send.at[0], s_recv.at[0], shift=around[t]
        )

    for t in range(1, groups):
        spread(t).start()
    take_halo(2)
    images(wide.at[2], slots[2])
    others = pl.ds(0, groups - 1)
    drain(rows_buf.at[others], s_recv.at[0])

    lane_row = lax.broadcasted_iota(jnp.int32, (1, LANES), 1)
    sigma = jnp.full((1, LANES), MID, F32)
    for j in range(shifts):
        sigma = jnp.where(lane_row == j, table_ref[ids_ref[j]], sigma)
    flat_rows = rows_buf.reshape(groups * n, LANES)
    gram = []
    for g in range(groups):
        block = flat_rows[pl.ds(g * n, n)]
        gram.append(sum(block[q * nb : (q + 1) * nb] for q in range(parts)))
    solved = coefficients(jnp.concatenate(gram, axis=0), sigma)
    for i, value in enumerate(solved):
        for j in range(shifts):
            spreaded = jnp.broadcast_to(value[:, j : j + 1], value.shape)
            coeff_out[j, i] = spreaded.reshape(groups, nb, LANES)

    to_both(lambda side: drain(wide.at[:, pl.ds(0, depth)], halo_send.at[side]))
    drain(wide.at[pl.ds(0, 2), pl.ds(0, rows)], z_send.at[0])
    drain(in_buf.at[peers, :, pl.ds(0, BASIS)], rs_send.at[0])
    drain(rows_buf.at[0, peers], g_send.at[0])
    drain(rows_buf.at[others], s_send.at[0])


def combine_kernel(fields_ref, own_ref, coeff_ref, sol_hbm, res_hbm, sol_buf, res_buf, sem):
    groups, shifts = fields_ref.shape[0], fields_ref.shape[1]
    rows, nb = fields_ref.shape[3], fields_ref.shape[4]

    def copies(g, j):
        out = []
        for which, (buf, hbm) in enumerate(((sol_buf, sol_hbm), (res_buf, res_hbm))):
            for b in range(nb):
                out.append(
                    pltpu.make_async_copy(
                        buf.at[g, j, :, b], hbm.at[j, g * nb + b], sem.at[which]
                    )
                )
        return out

    def one(u, carry):
        g, j = u // shifts, lax.rem(u, shifts)
        c = [coeff_ref[j, i, g][None] for i in range(6)]
        w0 = own_ref[g]
        w1, w2, w3 = (fields_ref[g, j, i] for i in range(3))
        sol_buf.at[g, j].reshape(rows, nb, LANES)[...] = c[0] * w0 + c[1] * w1 + c[2] * w2
        res_buf.at[g, j].reshape(rows, nb, LANES)[...] = (
            c[3] * w0 - c[4] * w1 - c[5] * w2 - c[2] * w3
        )
        for copy in copies(g, j):
            copy.start()
        return carry

    lax.fori_loop(0, groups * shifts, one, 0)

    drain(sol_hbm, sem.at[0])
    drain(res_hbm, sem.at[1])


def on_device(sources, kappa, mass, shift_table, shift_ids, sketch):
    n, groups = lax.axis_size("dom"), lax.axis_size("shift")
    nb, slab, ny = sources.shape[0], sources.shape[1], sources.shape[2]
    shifts = shift_ids.shape[0]
    sk = sketch.shape[0]
    rows = slab * ny
    planes = slab + 2 * HALO
    wide_rows, inner = planes * ny, (planes - 2) * ny
    pairs = rows // 2
    weights = 2 * (BASIS + SPLIT) * nb
    vec = (nb, LANES)
    half = rows // 2
    sketch, weight, wide, passed, kappa, mass = pl.pallas_call(
        functools.partial(prepare_kernel, n, groups, ny),
        out_shape=(
            pltpu.VMEM((pairs, sk, 2, LANES), BF16),
            pltpu.VMEM((pairs, weights, LANES), BF16),
            pltpu.VMEM((wide_rows, nb, 1, LANES), F32),
            pltpu.VMEM((2, half, nb, 1, LANES), F32),
            pltpu.VMEM((inner,) + vec, F32),
            pltpu.VMEM((inner,) + vec, F32),
        ),
        in_specs=[HBM_SPEC] * 4,
        out_specs=(VMEM_SPEC,) * 6,
        scratch_shapes=[
            pltpu.VMEM((2, inner, 1, LANES), F32),
            pltpu.VMEM((inner,) + vec, F32),
            pltpu.VMEM((inner,) + vec, F32),
            pltpu.VMEM((inner,) + vec, F32),
            pltpu.VMEM((inner - 2 * ny,) + vec, F32),
            pltpu.VMEM((inner - 2 * ny,) + vec, F32),
            pltpu.VMEM((inner - 2 * ny,) + vec, F32),
            DMA((1,)), DMA((2,)),
            DMA((2,)), DMA((HALO, 2)), DMA((2,)), DMA((2,)), DMA((1,)), DMA((2,)),
        ],
        compiler_params=pltpu.CompilerParams(
            collective_id=0, has_side_effects=True, vmem_limit_bytes=16 << 20
        ),
        name="prepare",
    )(
        in_hbm(sources.reshape(nb, rows, 1, LANES)), in_hbm(kappa.reshape(rows, 1, LANES)),
        in_hbm(mass.reshape(rows, 1, LANES)), in_hbm(sketch.reshape(sk, pairs, 2, LANES)),
    )
    parts = n // nb
    span = sk // LANES // parts
    fields, own, coeff = pl.pallas_call(
        functools.partial(project_kernel, n, groups, ny),
        out_shape=(
            pltpu.VMEM((groups, shifts, 3, rows) + vec, F32),
            pltpu.VMEM((groups, rows) + vec, F32),
            pltpu.VMEM((shifts, 6, groups) + vec, F32),
        ),
        in_specs=[VMEM_SPEC] * 6 + [SMEM_SPEC] * 2,
        out_specs=(VMEM_SPEC,) * 3,
        scratch_shapes=[
            pltpu.VMEM((groups - 1, wide_rows) + vec, F32),
            pltpu.VMEM((shifts, inner) + vec, F32),
            pltpu.VMEM((2 * sk, weights // 2), F32),
            pltpu.VMEM((inner,) + vec, F32),
            pltpu.VMEM((inner,) + vec, F32),
            pltpu.VMEM((inner - 2 * ny,) + vec, F32),
            pltpu.VMEM((sk // LANES, BASIS, nb, 1, LANES), F32),
            pltpu.VMEM((n, span, 16, 1, LANES), F32),
            pltpu.VMEM((groups, n, 1, LANES), F32),
            DMA((1,)), DMA((3,)), DMA((2,)), DMA((3, 2)),
            DMA((1,)), DMA((1,)), DMA((1,)), DMA((1,)), DMA((1,)), DMA((1,)),
        ],
        compiler_params=pltpu.CompilerParams(
            collective_id=1, has_side_effects=True, vmem_limit_bytes=16 << 20
        ),
        name="project",
    )(
        in_vmem(sketch.reshape(pairs, 2 * sk, LANES)), in_vmem(weight),
        in_vmem(wide.reshape((wide_rows,) + vec)), in_vmem(passed.reshape((2, half) + vec)),
        in_vmem(kappa), in_vmem(mass), shift_table, shift_ids,
    )

    out = pltpu.HBM((shifts, groups * nb, rows, 1, LANES), F32)
    buf = pltpu.VMEM((groups, shifts, rows, nb, 1, LANES), F32)
    solution, residual = pl.pallas_call(
        combine_kernel,
        out_shape=(out, out),
        in_specs=[VMEM_SPEC] * 3,
        out_specs=(HBM_SPEC,) * 2,
        scratch_shapes=[buf, buf, DMA((2,))],
        compiler_params=pltpu.CompilerParams(vmem_limit_bytes=16 << 20),
        name="combine",
    )(in_vmem(fields), in_vmem(own), in_vmem(coeff))
    shape = (shifts, groups * nb, slab, ny, LANES)
    return solution.reshape(shape), residual.reshape(shape)


def solution(mesh):
    placed = (
        P("shift", "dom", None, None),
        P("dom", None, None),
        P("dom", None, None),
        P(),
        P("shift"),
        P(None, "dom", None, None),
    )
    return jax.shard_map(
        on_device,
        mesh=mesh,
        in_specs=placed,
        out_specs=(P("shift", None, "dom", None, None), P("shift", None, "dom", None, None)),
        check_vma=False,
    )
```

```python
import functools

import jax
import jax.numpy as jnp
from jax import lax
from jax.experimental import pallas as pl
from jax.experimental.pallas import tpu as pltpu
from jax.sharding import PartitionSpec as P

HALO = 3
LANES = 128
MID = 2.25
F32 = jnp.float32
BF16 = jnp.bfloat16
BASIS = 10
LINES = 4
SPLIT = 6
IMAGES = ((0,), (1, 6), (2, 3, 7), (4, 5, 8, 9))
VMEM_SPEC = pl.BlockSpec(memory_space=pltpu.VMEM)
HBM_SPEC = pl.BlockSpec(memory_space=pltpu.HBM)
SMEM_SPEC = pl.BlockSpec(memory_space=pltpu.SMEM)
DMA = pltpu.SemaphoreType.DMA


def in_hbm(array):
    return pltpu.with_memory_space_constraint(array, pltpu.HBM)


def in_vmem(array):
    return pltpu.with_memory_space_constraint(array, pltpu.VMEM)


def remote(src, dst, send, recv, **where):
    return pltpu.make_async_remote_copy(
        src_ref=src, dst_ref=dst, send_sem=send, recv_sem=recv,
        device_id=where, device_id_type=pl.DeviceIdType.MESH,
    )


def signal(sem, **where):
    pl.semaphore_signal(sem, inc=1, device_id=where, device_id_type=pl.DeviceIdType.MESH)


def wrapped(index, size):
    return jnp.where(index >= size, index - size, index)


def drain(ref, sem):
    pltpu.make_async_copy(ref, ref, sem).wait()


def plane_of(ref, p, ny):
    return ref[pl.ds(p * ny, ny)]


def neighbour_sum(ref, p, ny):
    inner = plane_of(ref, p, ny)
    total = plane_of(ref, p - 1, ny) + plane_of(ref, p + 1, ny)
    none = jnp.zeros((1,) + inner.shape[1:], F32)
    total = total + jnp.concatenate([none, inner[:-1]], axis=0)
    total = total + jnp.concatenate([inner[1:], none], axis=0)
    lane = lax.broadcasted_iota(jnp.int32, inner.shape, 2)
    total = total + jnp.where(lane > 0, pltpu.roll(inner, 1, 2), 0.0)
    return total + jnp.where(lane < LANES - 1, pltpu.roll(inner, LANES - 1, 2), 0.0)


def edge_flag(p, planes, width, low, high):
    if p < width:
        return low
    return high if p >= planes - width else None


def masked(value, flag):
    return value if flag is None else value * flag


def edge_flags(me, n):
    return (me > 0).astype(F32), (me < n - 1).astype(F32)


def prepare_kernel(
    n, groups, ny, src_hbm, kappa_hbm, mass_hbm, sketch_hbm,
    sketch_out, weights_out, wide, passed_out, kappa_out, mass1,
    coef, diag, g0, g1, h0, h1, h2,
    load_sem, in_sem, wide_send, wide_recv, coef_send, coef_recv, z_send, z_recv,
):
    me = lax.axis_index("dom")
    group = lax.axis_index("shift")
    nb, rows = src_hbm.shape[0], src_hbm.shape[1]
    slab = rows // ny
    right, left = wrapped(me + 1, n), wrapped(me + n - 1, n)
    up, down = wrapped(group + 1, groups), wrapped(group + groups - 1, groups)
    has_right, has_left = me < n - 1, me > 0
    depth = HALO * ny
    thin = (HALO - 1) * ny
    planes = slab + 2 * HALO

    barrier = pltpu.get_barrier_semaphore()
    inputs = [
        pltpu.make_async_copy(src_hbm.at[b], wide.at[pl.ds(depth, rows), b], in_sem.at[0])
        for b in range(nb)
    ]
    inputs.append(pltpu.make_async_copy(kappa_hbm, coef.at[0, pl.ds(thin, rows)], in_sem.at[1]))
    inputs.append(pltpu.make_async_copy(mass_hbm, coef.at[1, pl.ds(thin, rows)], in_sem.at[1]))
    for copy in inputs:
        copy.start()

    @pl.when(has_right)
    def _():
        signal(barrier, dom=right)

    @pl.when(has_left)
    def _():
        signal(barrier, dom=left)

    signal(barrier, shift=up)
    signal(barrier, shift=down)

    def load(k):
        return pltpu.make_async_copy(sketch_hbm.at[:, k], sketch_out.at[k], load_sem.at[0])

    loads = sketch_hbm.shape[1]
    early = 6
    for k in range(early):
        load(k).start()
    drain(wide.at[pl.ds(depth, rows)], in_sem.at[0])
    drain(coef.at[:, pl.ds(thin, rows)], in_sem.at[1])

    def wide_halo(k, side):
        first, target, there = (
            (depth + rows - (k + 1) * ny, depth - (k + 1) * ny, right),
            (depth + k * ny, depth + rows + k * ny, left),
        )[side]
        return remote(
            wide.at[pl.ds(first, ny)], wide.at[pl.ds(target, ny)],
            wide_send.at[side], wide_recv.at[k, side], dom=there,
        )

    def coef_halo(side):
        first, target, there = ((rows, 0, right), (thin, thin + rows, left))[side]
        return remote(
            coef.at[:, pl.ds(first, thin)], coef.at[:, pl.ds(target, thin)],
            coef_send.at[side], coef_recv.at[side], dom=there,
        )

    def pass_on(way):
        count = passed_out.shape[1]
        there = (up, down)[way]
        return remote(
            wide.at[pl.ds(depth + way * count, count)], passed_out.at[way],
            z_send.at[0], z_recv.at[way], shift=there,
        )

    pl.semaphore_wait(barrier, has_right.astype(jnp.int32) + has_left.astype(jnp.int32) + 2)

    def send_halo(side):
        wide_halo(0, side).start()
        coef_halo(side).start()
        for k in range(1, HALO):
            wide_halo(k, side).start()

    pl.when(has_right)(lambda: send_halo(0))
    pl.when(has_left)(lambda: send_halo(1))
    for way in range(2):
        pass_on(way).start()
    for k in range(early, loads):
        load(k).start()

    field = wide.reshape(wide.shape[0], nb, LANES)

    @pl.when(jnp.logical_not(has_left))
    def _():
        field[pl.ds(0, depth)] = jnp.zeros((depth, nb, LANES), F32)
        coef[:, pl.ds(0, thin)] = jnp.zeros((2, thin, 1, LANES), F32)

    @pl.when(jnp.logical_not(has_right))
    def _():
        field[pl.ds(depth + rows, depth)] = jnp.zeros((depth, nb, LANES), F32)
        coef[:, pl.ds(thin + rows, thin)] = jnp.zeros((2, thin, 1, LANES), F32)

    full = (ny, nb, LANES)
    low, high = edge_flags(me, n)

    def factors(p):
        at = pl.ds(p * ny, ny)
        k = jnp.broadcast_to(coef[0, at], full)
        m = jnp.broadcast_to(coef[1, at] - 1.0, full)
        diag[at] = MID * m - k
        mass1[at] = m
        kappa_out[at] = k

    def level1(p):
        flag = edge_flag(p, planes - 2, 2, low, high)
        w = plane_of(field, p + 1, ny)
        out = pl.ds(p * ny, ny)
        g0[out] = masked(diag[out] * w - neighbour_sum(field, p + 1, ny), flag)
        g1[out] = mass1[out] * w

    def level2(p):
        flag = edge_flag(p, planes - 4, 1, low, high)
        at, out = pl.ds((p + 1) * ny, ny), pl.ds(p * ny, ny)
        d, m = diag[at], mass1[at]
        u0, u1 = g0[at], g1[at]
        h0[out] = masked(d * u0 - neighbour_sum(g0, p + 1, ny), flag)
        h1[out] = masked(d * u1 - neighbour_sum(g1, p + 1, ny) + m * u0, flag)
        h2[out] = m * u1

    def level3(p):
        at, inner = pl.ds((p + 2) * ny, ny), pl.ds((p + 1) * ny, ny)
        d, m = diag[at], mass1[at]
        v0, v1, v2 = h0[inner], h1[inner], h2[inner]
        e0 = d * v0 - neighbour_sum(h0, p + 1, ny)
        e1 = d * v1 - neighbour_sum(h1, p + 1, ny) + m * v0
        e2 = d * v2 - neighbour_sum(h2, p + 1, ny) + m * v1
        e3 = m * v2
        first = jnp.concatenate(
            [plane_of(field, p + HALO, ny), g0[at], v0, v1, e0, e1], axis=1
        )
        second = jnp.concatenate([g1[at], v2, e2, e3], axis=1)
        high_part = first.astype(BF16)
        low_part = (first - high_part.astype(F32)).astype(BF16)
        columns = jnp.concatenate([high_part, second.astype(BF16), low_part], axis=1)
        pairs = ny // 2
        weights_out[pl.ds(p * pairs, pairs)] = columns.reshape(pairs, 2 * columns.shape[1], LANES)

    done = [set(), set(), set(), set()]

    def advance(reach):
        ready = set(range(HALO - reach, planes - HALO + reach))
        if reach != 1:
            coefs = range(2, planes - 4) if reach == 0 else (0, 1, planes - 4, planes - 3)
            for p in (coefs if reach in (0, 2) else ()):
                factors(p)
        usable = range(2, planes - 4) if reach < 2 else range(planes - 2)
        for p in range(planes - 2):
            if p not in done[1] and {p, p + 1, p + 2} <= ready and p in usable:
                level1(p)
                done[1].add(p)
        for p in range(planes - 4):
            if p not in done[2] and {p, p + 1, p + 2} <= done[1]:
                level2(p)
                done[2].add(p)
        for p in range(slab):
            if p not in done[3] and {p, p + 1, p + 2} <= done[2]:
                level3(p)
                done[3].add(p)

    def clear_units(*accs):
        for acc in accs:
            pltpu.matmul_pop(acc)

    advance(0)
    pl.run_scoped(
        clear_units,
        pltpu.ACC(0)((sketch_hbm.shape[0], 2 * LANES), F32),
        pltpu.ACC(1)((sketch_hbm.shape[0], 2 * LANES), F32),
    )
    pl.when(has_left)(lambda: wide_halo(0, 0).wait_recv())
    pl.when(has_right)(lambda: wide_halo(0, 1).wait_recv())
    advance(1)

    def take(side):
        coef_halo(side).wait_recv()
        wide_halo(1, side).wait_recv()

    pl.when(has_left)(lambda: take(0))
    pl.when(has_right)(lambda: take(1))
    advance(2)
    pl.when(has_left)(lambda: wide_halo(2, 0).wait_recv())
    pl.when(has_right)(lambda: wide_halo(2, 1).wait_recv())
    advance(3)
    for way in range(2):
        pass_on(way).wait_recv()
    drain(sketch_out, load_sem.at[0])

    def sent(side):
        drain(wide.at[pl.ds(0, depth)], wide_send.at[side])
        drain(coef.at[:, pl.ds(0, thin)], coef_send.at[side])

    pl.when(has_right)(lambda: sent(0))
    pl.when(has_left)(lambda: sent(1))
    drain(wide.at[pl.ds(depth, rows)], z_send.at[0])


def solve_small(h_vals, entry):
    l00 = jnp.sqrt(entry[0][0])
    l10 = entry[1][0] / l00
    l20 = entry[2][0] / l00
    l11 = jnp.sqrt(entry[1][1] - l10 * l10)
    l21 = (entry[2][1] - l20 * l10) / l11
    l22 = jnp.sqrt(entry[2][2] - l20 * l20 - l21 * l21)
    f0 = h_vals[0] / l00
    f1 = (h_vals[1] - l10 * f0) / l11
    f2 = (h_vals[2] - l20 * f0 - l21 * f1) / l22
    c2 = f2 / l22
    c1 = (f1 - l21 * c2) / l11
    c0 = (f0 - l10 * c1 - l20 * c2) / l00
    return (c0, c1, c2)


def pair_lane(i, k):
    distance = (k - i) % BASIS
    if distance <= BASIS // 2:
        return BASIS * distance + i
    return BASIS * (BASIS - distance) + k


def coefficients(gram, sigma):
    tau, center = sigma - MID, sigma + 6.0

    def product(left, right):
        by_degree = {}
        for p, i in enumerate(IMAGES[left]):
            for q, k in enumerate(IMAGES[right]):
                at = pair_lane(i, k)
                column = gram[:, at : at + 1]
                by_degree[p + q] = by_degree[p + q] + column if p + q in by_degree else column
        top = max(by_degree)
        total = jnp.broadcast_to(by_degree[top], gram.shape)
        for degree in range(top - 1, -1, -1):
            total = total * tau + by_degree[degree]
        return total

    ww = [[product(i, k) if i <= k else None for k in range(4)] for i in range(4)]

    def between(i, k):
        total = ww[i][k]
        if i > 0:
            total = total + center * ww[i - 1][k]
        if k > 0:
            low = ww[min(i, k - 1)][max(i, k - 1)]
            if i > 0:
                low = low + center * ww[i - 1][k - 1]
            total = total + center * low
        return total

    scale = (1.0, 1.0, 1.0 / 6.0, 1.0 / 36.0)
    h_vals = [between(0, i) * scale[i] for i in (1, 2, 3)]
    entry = [[None] * 3 for _ in range(3)]
    for i in range(3):
        for k in range(i + 1):
            entry[i][k] = between(k + 1, i + 1) * (scale[i + 1] * scale[k + 1])
    ridge = 0.001 * (entry[0][0] + entry[1][1] + entry[2][2]) / 3.0 + 1.0
    for i in range(3):
        entry[i][i] = entry[i][i] + ridge
    c0, c1, c2 = solve_small(h_vals, entry)
    c1, c2 = c1 * (1.0 / 6.0), c2 * (1.0 / 36.0)
    return (c0, c1, c2, 1.0 - c0 * center, c0 + c1 * center, c1 + c2 * center)


def project_kernel(
    n, groups, lines, ny, sketch_ref, weights_ref, own_ref, passed_ref, kappa_ref, mass1_ref, table_ref, ids_ref,
    fields_out, own_out, coeff_out,
    wide, step_ref, picked, near, first, second, out_buf, in_buf, rows_buf,
    z_send, z_recv, halo_send, halo_recv, rs_send, rs_recv, g_send, g_recv, row_sem,
):
    me = lax.axis_index("dom")
    group = lax.axis_index("shift")
    planes = own_ref.shape[0] // ny
    nb = own_ref.shape[1]
    slab = planes - 2 * HALO
    rows, depth = slab * ny, HALO * ny
    right, left = wrapped(me + 1, n), wrapped(me + n - 1, n)
    around = [group] + [wrapped(group + t, groups) for t in range(1, groups)]
    up, down = around[1], around[groups - 1]
    has_right, has_left = me < n - 1, me > 0
    shifts = ids_ref.shape[0]
    low, high = edge_flags(me, n)

    barrier = pltpu.get_barrier_semaphore()
    row = n // lines
    base = me // row * row
    for t in range(1, row):
        signal(barrier, dom=base + wrapped(me - base + t, row))
    for t in range(1, lines):
        signal(barrier, dom=wrapped(me + t * row, n))
    for t in range(1, groups):
        signal(barrier, shift=around[t])

    slots = (down, up, around[groups // 2])
    half = passed_ref.shape[1]

    def across(way):
        at = pl.ds(depth + (1 - way) * half, half)
        return remote(
            own_ref.at[at], wide.at[way, at], z_send.at[0], z_recv.at[way], shift=(up, down)[way]
        )

    def beyond(way):
        return remote(
            passed_ref.at[way], wide.at[2, pl.ds(depth + way * half, half)],
            z_send.at[0], z_recv.at[2], shift=(up, down)[way],
        )

    def halo(index, side, src, first_plane, count):
        target = ((first_plane - (slab - HALO)) * ny, depth + rows + first_plane * ny)[side]
        return remote(
            src, wide.at[index, pl.ds(target, count * ny)],
            halo_send.at[side], halo_recv.at[index, side], dom=(right, left)[side],
        )

    def planes_for(side):
        return range(slab - HALO, slab) if side == 0 else range(HALO)

    def early_halo(index, side):
        held = range(index * slab // 2, (index + 1) * slab // 2)
        mine = [p for p in planes_for(side) if p in held]
        at = pl.ds((mine[0] - held[0]) * ny, len(mine) * ny)
        return halo(index, side, passed_ref.at[index, at], mine[0], len(mine))

    def late_halo(index, side):
        held = range((1 - index) * slab // 2, (2 - index) * slab // 2)
        if index == 2:
            held = range(slab)
        mine = [p for p in planes_for(side) if p in held]
        at = pl.ds(depth + mine[0] * ny, len(mine) * ny)
        return halo(index, side, wide.at[index, at], mine[0], len(mine))

    def to_both(start):
        pl.when(has_right)(lambda: start(0))
        pl.when(has_left)(lambda: start(1))

    def take_halo(index):
        def take(side):
            drain(wide.at[index, pl.ds(0, depth)], halo_recv.at[index, side])

        pl.when(has_left)(lambda: take(0))
        pl.when(has_right)(lambda: take(1))

    steps = sketch_ref.shape[0] // 2
    pieces = 2
    tall = sketch_ref.shape[1] // (2 * pieces)
    split, columns = SPLIT * nb, BASIS * nb
    chunks = 2 * pieces * tall // (2 * LANES)
    parts = n // nb
    span = chunks // parts
    flat_out = out_buf.reshape(chunks * columns, LANES)

    def piece(dest):
        return out_buf.at[pl.ds(dest // nb * span, span), :, lax.rem(dest, nb)]

    def scatter(dest):
        return remote(
            piece(dest), in_buf.at[me, :, pl.ds(0, BASIS)], rs_send.at[0], rs_recv.at[0], dom=dest
        )

    def stage(u):
        tile = jnp.concatenate([weights_ref[2 * u], weights_ref[2 * u + 1]], axis=1)
        for unit in range(2):
            pltpu.matmul_push_rhs(tile, 0, unit, transpose=True)

    def multiply(accs):
        def accumulate(u, part):
            for unit in range(2):
                at = pl.ds((2 * part + unit) * tall, tall)
                tile = jnp.concatenate([sketch_ref[2 * u, at], sketch_ref[2 * u + 1, at]], axis=1)
                pltpu.matmul_acc_lhs(accs[unit], tile, load_staged_rhs=0)

        def run(part, start, stop):
            def step(u, carry):
                accumulate(u, part)
                stage(u + 1)
                return carry

            lax.fori_loop(start, stop, step, 0)

        def finish(part):
            accumulate(steps - 1, part)
            if part + 1 < pieces:
                stage(0)
            odd = lax.rem(lax.broadcasted_iota(jnp.int32, (tall, LANES), 0), 2) == 1
            for unit in range(2):
                value = pltpu.matmul_pop(accs[unit])
                picked[pl.ds((2 * part + unit) * tall, tall)] = jnp.where(
                    odd, value[:, LANES:], value[:, :LANES]
                )
            first = part * 2 * tall
            turned = (
                picked[pl.ds(first, tall, stride=2)] + picked[pl.ds(first + 1, tall, stride=2)]
            ).T
            sketched = jnp.concatenate(
                [turned[:split] + turned[columns:], turned[split:columns]], axis=0
            )
            share = chunks // pieces
            for r in range(share):
                flat_out[pl.ds((part * share + r) * columns, columns)] = sketched[
                    :, r * LANES : (r + 1) * LANES
                ]
            mine = n // pieces
            for t in range(mine):
                dest = part * mine + lax.rem(me + t, mine)
                pl.when(dest != me)(lambda: scatter(dest).start())

        stage(0)
        run(0, 0, steps // 2)
        pl.semaphore_wait(barrier, row - 1 + lines - 1 + groups - 1)
        for t in range(1, lines):
            signal(row_sem, dom=wrapped(me + t * row, n))
        for way in range(2):
            across(way).start()
        run(0, steps // 2, steps - 1)
        pl.semaphore_wait(row_sem, lines - 1)
        finish(0)
        for index in range(2):
            to_both(lambda side: early_halo(index, side).start())
        for way in range(2):
            beyond(way).start()
        run(1, 0, steps - 1)
        finish(1)

    pl.run_scoped(
        lambda *accs: multiply(accs),
        pltpu.ACC(0)((tall, 2 * LANES), F32), pltpu.ACC(1)((tall, 2 * LANES), F32),
    )
    in_buf[me, :, pl.ds(0, BASIS)] = piece(me)[...]

    def clear(at):
        for index in range(groups - 1):
            wide[index, at] = jnp.zeros((depth, nb, LANES), F32)

    pl.when(jnp.logical_not(has_left))(lambda: clear(pl.ds(0, depth)))
    pl.when(jnp.logical_not(has_right))(lambda: clear(pl.ds(depth + rows, depth)))
    for index in range(2):
        wide[index, pl.ds(depth + index * half, half)] = passed_ref[index]
    for j in range(shifts):
        step_ref[j] = table_ref[ids_ref[j]] * mass1_ref[...] - kappa_ref[...]

    def images(field, slot):
        for p in range(planes - 2):
            near[pl.ds(p * ny, ny)] = neighbour_sum(field, p + 1, ny)

        def one_shift(j, carry):
            for p in range(planes - 2):
                at = pl.ds(p * ny, ny)
                flag = edge_flag(p, planes - 2, 2, low, high)
                first[at] = masked(step_ref[j, at] * plane_of(field, p + 1, ny) - near[at], flag)
            for p in range(planes - 4):
                at = pl.ds((p + 1) * ny, ny)
                flag = edge_flag(p, planes - 4, 1, low, high)
                second[pl.ds(p * ny, ny)] = masked(
                    step_ref[j, at] * first[at] - neighbour_sum(first, p + 1, ny), flag
                )
            for p in range(slab):
                at, inner, out = pl.ds((p + 2) * ny, ny), pl.ds((p + 1) * ny, ny), pl.ds(p * ny, ny)
                fields_out[slot, j, 0, out] = first[at]
                fields_out[slot, j, 1, out] = second[inner]
                fields_out[slot, j, 2, out] = (
                    step_ref[j, at] * second[inner] - neighbour_sum(second, p + 1, ny)
                )
            return carry

        lax.fori_loop(0, shifts, one_shift, 0)
        for p in range(slab):
            own_out[slot, pl.ds(p * ny, ny)] = plane_of(field, p + HALO, ny)

    images(own_ref, group)
    for way in range(2):
        across(way).wait_recv()
        to_both(lambda side: late_halo(way, side).start())

    peers = pl.ds(0, n - 1)
    drain(in_buf.at[peers, :, pl.ds(0, BASIS)], rs_recv.at[0])
    flat_in = in_buf.reshape(n * span * in_buf.shape[2], LANES)
    tile = span * in_buf.shape[2]
    total = flat_in[pl.ds(0, tile)]
    for t in range(1, n):
        total = total + flat_in[pl.ds(t * tile, tile)]
    lane = lax.broadcasted_iota(jnp.int32, (BASIS, LANES), 1)
    place = lax.broadcasted_iota(jnp.int32, (BASIS, LANES), 0)
    views = [total[r * in_buf.shape[2] :][:BASIS] for r in range(span)]
    twice = [jnp.concatenate([view, view], axis=0) for view in views]
    packed = jnp.zeros((BASIS, LANES), F32)
    for d in range(BASIS // 2 + 1):
        terms = sum(view * wrap[d : d + BASIS] for view, wrap in zip(views, twice))
        packed = jnp.where(lane == place + BASIS * d, jnp.sum(terms, axis=1, keepdims=True), packed)
    slot = group * n + me
    rows_buf[slot] = jnp.sum(packed, axis=0, keepdims=True)

    def share(t, z):
        return remote(
            rows_buf.at[slot], rows_buf.at[slot], g_send.at[0], g_recv.at[0],
            dom=wrapped(me + t, n), shift=around[z],
        )

    for z in (2, 1, 3, 0):
        for t in range(n):
            if z or t:
                share(t, z).start()
    drain(wide.at[2, pl.ds(depth, rows)], z_recv.at[2])
    to_both(lambda side: late_halo(2, side).start())
    take_halo(0)
    images(wide.at[0], slots[0])
    take_halo(1)
    images(wide.at[1], slots[1])
    take_halo(2)
    images(wide.at[2], slots[2])
    everyone = pl.ds(0, groups * n - 1)
    drain(rows_buf.at[everyone], g_recv.at[0])

    lane_row = lax.broadcasted_iota(jnp.int32, (1, LANES), 1)
    sigma = jnp.full((1, LANES), MID, F32)
    for j in range(shifts):
        sigma = jnp.where(lane_row == j, table_ref[ids_ref[j]], sigma)
    flat_rows = rows_buf.reshape(groups * n, LANES)
    gram = []
    for g in range(groups):
        block = flat_rows[pl.ds(g * n, n)]
        gram.append(sum(block[q * nb : (q + 1) * nb] for q in range(parts)))
    solved = coefficients(jnp.concatenate(gram, axis=0), sigma)
    for i, value in enumerate(solved):
        for j in range(shifts):
            spreaded = jnp.broadcast_to(value[:, j : j + 1], value.shape)
            coeff_out[j, i] = spreaded.reshape(groups, nb, LANES)

    to_both(lambda side: drain(wide.at[:, pl.ds(0, depth)], halo_send.at[side]))
    drain(wide.at[pl.ds(0, 2), pl.ds(0, rows)], z_send.at[0])
    drain(in_buf.at[peers, :, pl.ds(0, BASIS)], rs_send.at[0])
    drain(rows_buf.at[everyone], g_send.at[0])


def combine_kernel(fields_ref, own_ref, coeff_ref, sol_hbm, res_hbm, sol_buf, res_buf, sem):
    groups, shifts = fields_ref.shape[0], fields_ref.shape[1]
    rows, nb = fields_ref.shape[3], fields_ref.shape[4]

    def copies(g, j):
        out = []
        for which, (buf, hbm) in enumerate(((sol_buf, sol_hbm), (res_buf, res_hbm))):
            for b in range(nb):
                out.append(
                    pltpu.make_async_copy(
                        buf.at[g, j, :, b], hbm.at[j, g * nb + b], sem.at[which]
                    )
                )
        return out

    def one(u, carry):
        g, j = u // shifts, lax.rem(u, shifts)
        c = [coeff_ref[j, i, g][None] for i in range(6)]
        w0 = own_ref[g]
        w1, w2, w3 = (fields_ref[g, j, i] for i in range(3))
        sol_buf.at[g, j].reshape(rows, nb, LANES)[...] = c[0] * w0 + c[1] * w1 + c[2] * w2
        res_buf.at[g, j].reshape(rows, nb, LANES)[...] = (
            c[3] * w0 - c[4] * w1 - c[5] * w2 - c[2] * w3
        )
        for copy in copies(g, j):
            copy.start()
        return carry

    lax.fori_loop(0, groups * shifts, one, 0)

    drain(sol_hbm, sem.at[0])
    drain(res_hbm, sem.at[1])


def on_device(sources, kappa, mass, shift_table, shift_ids, sketch):
    n, groups = lax.axis_size("dom"), lax.axis_size("shift")
    nb, slab, ny = sources.shape[0], sources.shape[1], sources.shape[2]
    shifts = shift_ids.shape[0]
    sk = sketch.shape[0]
    rows = slab * ny
    planes = slab + 2 * HALO
    wide_rows, inner = planes * ny, (planes - 2) * ny
    pairs = rows // 2
    weights = 2 * (BASIS + SPLIT) * nb
    vec = (nb, LANES)
    half = rows // 2
    sketch, weight, wide, passed, kappa, mass = pl.pallas_call(
        functools.partial(prepare_kernel, n, groups, ny),
        out_shape=(
            pltpu.VMEM((pairs, sk, 2, LANES), BF16),
            pltpu.VMEM((pairs, weights, LANES), BF16),
            pltpu.VMEM((wide_rows, nb, 1, LANES), F32),
            pltpu.VMEM((2, half, nb, 1, LANES), F32),
            pltpu.VMEM((inner,) + vec, F32),
            pltpu.VMEM((inner,) + vec, F32),
        ),
        in_specs=[HBM_SPEC] * 4,
        out_specs=(VMEM_SPEC,) * 6,
        scratch_shapes=[
            pltpu.VMEM((2, inner, 1, LANES), F32),
            pltpu.VMEM((inner,) + vec, F32),
            pltpu.VMEM((inner,) + vec, F32),
            pltpu.VMEM((inner,) + vec, F32),
            pltpu.VMEM((inner - 2 * ny,) + vec, F32),
            pltpu.VMEM((inner - 2 * ny,) + vec, F32),
            pltpu.VMEM((inner - 2 * ny,) + vec, F32),
            DMA((1,)), DMA((2,)),
            DMA((2,)), DMA((HALO, 2)), DMA((2,)), DMA((2,)), DMA((1,)), DMA((2,)),
        ],
        compiler_params=pltpu.CompilerParams(
            collective_id=0, has_side_effects=True, vmem_limit_bytes=16 << 20
        ),
        name="prepare",
    )(
        in_hbm(sources.reshape(nb, rows, 1, LANES)), in_hbm(kappa.reshape(rows, 1, LANES)),
        in_hbm(mass.reshape(rows, 1, LANES)), in_hbm(sketch.reshape(sk, pairs, 2, LANES)),
    )
    parts = n // nb
    span = sk // LANES // parts
    fields, own, coeff = pl.pallas_call(
        functools.partial(project_kernel, n, groups, LINES, ny),
        out_shape=(
            pltpu.VMEM((groups, shifts, 3, rows) + vec, F32),
            pltpu.VMEM((groups, rows) + vec, F32),
            pltpu.VMEM((shifts, 6, groups) + vec, F32),
        ),
        in_specs=[VMEM_SPEC] * 6 + [SMEM_SPEC] * 2,
        out_specs=(VMEM_SPEC,) * 3,
        scratch_shapes=[
            pltpu.VMEM((groups - 1, wide_rows) + vec, F32),
            pltpu.VMEM((shifts, inner) + vec, F32),
            pltpu.VMEM((2 * sk, weights // 2), F32),
            pltpu.VMEM((inner,) + vec, F32),
            pltpu.VMEM((inner,) + vec, F32),
            pltpu.VMEM((inner - 2 * ny,) + vec, F32),
            pltpu.VMEM((sk // LANES, BASIS, nb, 1, LANES), F32),
            pltpu.VMEM((n, span, 16, 1, LANES), F32),
            pltpu.VMEM((groups * n, 1, LANES), F32),
            DMA((1,)), DMA((3,)), DMA((2,)), DMA((3, 2)),
            DMA((1,)), DMA((1,)), DMA((1,)), DMA((1,)), pltpu.SemaphoreType.REGULAR,
        ],
        compiler_params=pltpu.CompilerParams(
            collective_id=1, has_side_effects=True, vmem_limit_bytes=16 << 20
        ),
        name="project",
    )(
        in_vmem(sketch.reshape(pairs, 2 * sk, LANES)), in_vmem(weight),
        in_vmem(wide.reshape((wide_rows,) + vec)), in_vmem(passed.reshape((2, half) + vec)),
        in_vmem(kappa), in_vmem(mass), shift_table, shift_ids,
    )

    out = pltpu.HBM((shifts, groups * nb, rows, 1, LANES), F32)
    buf = pltpu.VMEM((groups, shifts, rows, nb, 1, LANES), F32)
    solution, residual = pl.pallas_call(
        combine_kernel,
        out_shape=(out, out),
        in_specs=[VMEM_SPEC] * 3,
        out_specs=(HBM_SPEC,) * 2,
        scratch_shapes=[buf, buf, DMA((2,))],
        compiler_params=pltpu.CompilerParams(vmem_limit_bytes=16 << 20),
        name="combine",
    )(in_vmem(fields), in_vmem(own), in_vmem(coeff))
    shape = (shifts, groups * nb, slab, ny, LANES)
    return solution.reshape(shape), residual.reshape(shape)


def solution(mesh):
    placed = (
        P("shift", "dom", None, None),
        P("dom", None, None),
        P("dom", None, None),
        P(),
        P("shift"),
        P(None, "dom", None, None),
    )
    return jax.shard_map(
        on_device,
        mesh=mesh,
        in_specs=placed,
        out_specs=(P("shift", None, "dom", None, None), P("shift", None, "dom", None, None)),
        check_vma=False,
    )
```

```python
import functools

import jax
import jax.numpy as jnp
from jax import lax
from jax.experimental import pallas as pl
from jax.experimental.pallas import tpu as pltpu
from jax.sharding import PartitionSpec as P

HALO = 3
LANES = 128
MID = 2.25
F32 = jnp.float32
BF16 = jnp.bfloat16
BASIS = 10
PASSED = 3
LINES = 4
SPLIT = 6
IMAGES = ((0,), (1, 6), (2, 3, 7), (4, 5, 8, 9))
VMEM_SPEC = pl.BlockSpec(memory_space=pltpu.VMEM)
HBM_SPEC = pl.BlockSpec(memory_space=pltpu.HBM)
SMEM_SPEC = pl.BlockSpec(memory_space=pltpu.SMEM)
DMA = pltpu.SemaphoreType.DMA


def in_hbm(array):
    return pltpu.with_memory_space_constraint(array, pltpu.HBM)


def in_vmem(array):
    return pltpu.with_memory_space_constraint(array, pltpu.VMEM)


def remote(src, dst, send, recv, **where):
    return pltpu.make_async_remote_copy(
        src_ref=src, dst_ref=dst, send_sem=send, recv_sem=recv,
        device_id=where, device_id_type=pl.DeviceIdType.MESH,
    )


def signal(sem, **where):
    pl.semaphore_signal(sem, inc=1, device_id=where, device_id_type=pl.DeviceIdType.MESH)


def wrapped(index, size):
    return jnp.where(index >= size, index - size, index)


def drain(ref, sem):
    pltpu.make_async_copy(ref, ref, sem).wait()


def plane_of(ref, p, ny):
    return ref[pl.ds(p * ny, ny)]


def neighbour_sum(ref, p, ny):
    inner = plane_of(ref, p, ny)
    total = plane_of(ref, p - 1, ny) + plane_of(ref, p + 1, ny)
    none = jnp.zeros((1,) + inner.shape[1:], F32)
    total = total + jnp.concatenate([none, inner[:-1]], axis=0)
    total = total + jnp.concatenate([inner[1:], none], axis=0)
    lane = lax.broadcasted_iota(jnp.int32, inner.shape, 2)
    total = total + jnp.where(lane > 0, pltpu.roll(inner, 1, 2), 0.0)
    return total + jnp.where(lane < LANES - 1, pltpu.roll(inner, LANES - 1, 2), 0.0)


def edge_flag(p, planes, width, low, high):
    if p < width:
        return low
    return high if p >= planes - width else None


def masked(value, flag):
    return value if flag is None else value * flag


def edge_flags(me, n):
    return (me > 0).astype(F32), (me < n - 1).astype(F32)


def prepare_kernel(
    n, groups, ny, src_hbm, kappa_hbm, mass_hbm, sketch_hbm,
    sketch_out, weights_out, wide, passed_out, kappa_out, mass1,
    coef, diag, g0, g1, h0, h1, h2,
    load_sem, in_sem, wide_send, wide_recv, coef_send, coef_recv, z_send, z_recv,
):
    me = lax.axis_index("dom")
    group = lax.axis_index("shift")
    nb, rows = src_hbm.shape[0], src_hbm.shape[1]
    slab = rows // ny
    right, left = wrapped(me + 1, n), wrapped(me + n - 1, n)
    up, down = wrapped(group + 1, groups), wrapped(group + groups - 1, groups)
    has_right, has_left = me < n - 1, me > 0
    depth = HALO * ny
    thin = (HALO - 1) * ny
    planes = slab + 2 * HALO

    barrier = pltpu.get_barrier_semaphore()
    inputs = [
        pltpu.make_async_copy(src_hbm.at[b], wide.at[pl.ds(depth, rows), b], in_sem.at[0])
        for b in range(nb)
    ]
    inputs.append(pltpu.make_async_copy(kappa_hbm, coef.at[0, pl.ds(thin, rows)], in_sem.at[1]))
    inputs.append(pltpu.make_async_copy(mass_hbm, coef.at[1, pl.ds(thin, rows)], in_sem.at[1]))
    for copy in inputs:
        copy.start()

    @pl.when(has_right)
    def _():
        signal(barrier, dom=right)

    @pl.when(has_left)
    def _():
        signal(barrier, dom=left)

    signal(barrier, shift=up)
    signal(barrier, shift=down)

    def load(k):
        return pltpu.make_async_copy(sketch_hbm.at[:, k], sketch_out.at[k], load_sem.at[0])

    loads = sketch_hbm.shape[1]
    for k in range(loads):
        load(k).start()
    drain(wide.at[pl.ds(depth, rows)], in_sem.at[0])
    drain(coef.at[:, pl.ds(thin, rows)], in_sem.at[1])

    def wide_halo(k, side):
        first, target, there = (
            (depth + rows - (k + 1) * ny, depth - (k + 1) * ny, right),
            (depth + k * ny, depth + rows + k * ny, left),
        )[side]
        return remote(
            wide.at[pl.ds(first, ny)], wide.at[pl.ds(target, ny)],
            wide_send.at[side], wide_recv.at[k, side], dom=there,
        )

    def coef_halo(side):
        first, target, there = ((rows, 0, right), (thin, thin + rows, left))[side]
        return remote(
            coef.at[:, pl.ds(first, thin)], coef.at[:, pl.ds(target, thin)],
            coef_send.at[side], coef_recv.at[side], dom=there,
        )

    def pass_on(way):
        count = passed_out.shape[1]
        there = (up, down)[way]
        return remote(
            wide.at[pl.ds(depth + way * (rows - count), count)], passed_out.at[way],
            z_send.at[0], z_recv.at[way], shift=there,
        )

    pl.semaphore_wait(barrier, has_right.astype(jnp.int32) + has_left.astype(jnp.int32) + 2)

    def send_halo(side):
        wide_halo(0, side).start()
        coef_halo(side).start()
        for k in range(1, HALO):
            wide_halo(k, side).start()

    pl.when(has_right)(lambda: send_halo(0))
    pl.when(has_left)(lambda: send_halo(1))
    for way in range(2):
        pass_on(way).start()

    field = wide.reshape(wide.shape[0], nb, LANES)

    @pl.when(jnp.logical_not(has_left))
    def _():
        field[pl.ds(0, depth)] = jnp.zeros((depth, nb, LANES), F32)
        coef[:, pl.ds(0, thin)] = jnp.zeros((2, thin, 1, LANES), F32)

    @pl.when(jnp.logical_not(has_right))
    def _():
        field[pl.ds(depth + rows, depth)] = jnp.zeros((depth, nb, LANES), F32)
        coef[:, pl.ds(thin + rows, thin)] = jnp.zeros((2, thin, 1, LANES), F32)

    full = (ny, nb, LANES)
    low, high = edge_flags(me, n)

    def factors(p):
        at = pl.ds(p * ny, ny)
        k = jnp.broadcast_to(coef[0, at], full)
        m = jnp.broadcast_to(coef[1, at] - 1.0, full)
        diag[at] = MID * m - k
        mass1[at] = m
        kappa_out[at] = k

    def level1(p):
        flag = edge_flag(p, planes - 2, 2, low, high)
        w = plane_of(field, p + 1, ny)
        out = pl.ds(p * ny, ny)
        g0[out] = masked(diag[out] * w - neighbour_sum(field, p + 1, ny), flag)
        g1[out] = mass1[out] * w

    def level2(p):
        flag = edge_flag(p, planes - 4, 1, low, high)
        at, out = pl.ds((p + 1) * ny, ny), pl.ds(p * ny, ny)
        d, m = diag[at], mass1[at]
        u0, u1 = g0[at], g1[at]
        h0[out] = masked(d * u0 - neighbour_sum(g0, p + 1, ny), flag)
        h1[out] = masked(d * u1 - neighbour_sum(g1, p + 1, ny) + m * u0, flag)
        h2[out] = m * u1

    def level3(p):
        at, inner = pl.ds((p + 2) * ny, ny), pl.ds((p + 1) * ny, ny)
        d, m = diag[at], mass1[at]
        v0, v1, v2 = h0[inner], h1[inner], h2[inner]
        e0 = d * v0 - neighbour_sum(h0, p + 1, ny)
        e1 = d * v1 - neighbour_sum(h1, p + 1, ny) + m * v0
        e2 = d * v2 - neighbour_sum(h2, p + 1, ny) + m * v1
        e3 = m * v2
        first = jnp.concatenate(
            [plane_of(field, p + HALO, ny), g0[at], v0, v1, e0, e1], axis=1
        )
        second = jnp.concatenate([g1[at], v2, e2, e3], axis=1)
        high_part = first.astype(BF16)
        low_part = (first - high_part.astype(F32)).astype(BF16)
        columns = jnp.concatenate([high_part, second.astype(BF16), low_part], axis=1)
        pairs = ny // 2
        weights_out[pl.ds(p * pairs, pairs)] = columns.reshape(pairs, 2 * columns.shape[1], LANES)

    done = [set(), set(), set(), set()]

    def advance(reach):
        ready = set(range(HALO - reach, planes - HALO + reach))
        if reach != 1:
            coefs = range(2, planes - 4) if reach == 0 else (0, 1, planes - 4, planes - 3)
            for p in (coefs if reach in (0, 2) else ()):
                factors(p)
        usable = range(2, planes - 4) if reach < 2 else range(planes - 2)
        for p in range(planes - 2):
            if p not in done[1] and {p, p + 1, p + 2} <= ready and p in usable:
                level1(p)
                done[1].add(p)
        for p in range(planes - 4):
            if p not in done[2] and {p, p + 1, p + 2} <= done[1]:
                level2(p)
                done[2].add(p)
        for p in range(slab):
            if p not in done[3] and {p, p + 1, p + 2} <= done[2]:
                level3(p)
                done[3].add(p)

    def clear_units(*accs):
        for acc in accs:
            pltpu.matmul_pop(acc)

    advance(0)
    pl.run_scoped(
        clear_units,
        pltpu.ACC(0)((sketch_hbm.shape[0], 2 * LANES), F32),
        pltpu.ACC(1)((sketch_hbm.shape[0], 2 * LANES), F32),
    )
    pl.when(has_left)(lambda: wide_halo(0, 0).wait_recv())
    pl.when(has_right)(lambda: wide_halo(0, 1).wait_recv())
    advance(1)

    def take(side):
        coef_halo(side).wait_recv()
        wide_halo(1, side).wait_recv()

    pl.when(has_left)(lambda: take(0))
    pl.when(has_right)(lambda: take(1))
    advance(2)
    pl.when(has_left)(lambda: wide_halo(2, 0).wait_recv())
    pl.when(has_right)(lambda: wide_halo(2, 1).wait_recv())
    advance(3)
    for way in range(2):
        pass_on(way).wait_recv()
    drain(sketch_out, load_sem.at[0])

    def sent(side):
        drain(wide.at[pl.ds(0, depth)], wide_send.at[side])
        drain(coef.at[:, pl.ds(0, thin)], coef_send.at[side])

    pl.when(has_right)(lambda: sent(0))
    pl.when(has_left)(lambda: sent(1))
    drain(wide.at[pl.ds(0, 2 * passed_out.shape[1])], z_send.at[0])


def solve_small(h_vals, entry):
    l00 = jnp.sqrt(entry[0][0])
    l10 = entry[1][0] / l00
    l20 = entry[2][0] / l00
    l11 = jnp.sqrt(entry[1][1] - l10 * l10)
    l21 = (entry[2][1] - l20 * l10) / l11
    l22 = jnp.sqrt(entry[2][2] - l20 * l20 - l21 * l21)
    f0 = h_vals[0] / l00
    f1 = (h_vals[1] - l10 * f0) / l11
    f2 = (h_vals[2] - l20 * f0 - l21 * f1) / l22
    c2 = f2 / l22
    c1 = (f1 - l21 * c2) / l11
    c0 = (f0 - l10 * c1 - l20 * c2) / l00
    return (c0, c1, c2)


def pair_lane(i, k):
    distance = (k - i) % BASIS
    if distance <= BASIS // 2:
        return BASIS * distance + i
    return BASIS * (BASIS - distance) + k


def coefficients(gram, sigma):
    tau, center = sigma - MID, sigma + 6.0

    def product(left, right):
        by_degree = {}
        for p, i in enumerate(IMAGES[left]):
            for q, k in enumerate(IMAGES[right]):
                at = pair_lane(i, k)
                column = gram[:, at : at + 1]
                by_degree[p + q] = by_degree[p + q] + column if p + q in by_degree else column
        top = max(by_degree)
        total = jnp.broadcast_to(by_degree[top], gram.shape)
        for degree in range(top - 1, -1, -1):
            total = total * tau + by_degree[degree]
        return total

    ww = [[product(i, k) if i <= k else None for k in range(4)] for i in range(4)]

    def between(i, k):
        total = ww[i][k]
        if i > 0:
            total = total + center * ww[i - 1][k]
        if k > 0:
            low = ww[min(i, k - 1)][max(i, k - 1)]
            if i > 0:
                low = low + center * ww[i - 1][k - 1]
            total = total + center * low
        return total

    scale = (1.0, 1.0, 1.0 / 6.0, 1.0 / 36.0)
    h_vals = [between(0, i) * scale[i] for i in (1, 2, 3)]
    entry = [[None] * 3 for _ in range(3)]
    for i in range(3):
        for k in range(i + 1):
            entry[i][k] = between(k + 1, i + 1) * (scale[i + 1] * scale[k + 1])
    ridge = 0.001 * (entry[0][0] + entry[1][1] + entry[2][2]) / 3.0 + 1.0
    for i in range(3):
        entry[i][i] = entry[i][i] + ridge
    c0, c1, c2 = solve_small(h_vals, entry)
    c1, c2 = c1 * (1.0 / 6.0), c2 * (1.0 / 36.0)
    return (c0, c1, c2, 1.0 - c0 * center, c0 + c1 * center, c1 + c2 * center)


def project_kernel(
    n, groups, lines, ny, sketch_ref, weights_ref, own_ref, passed_ref, kappa_ref, mass1_ref, table_ref, ids_ref,
    fields_out, own_out, coeff_out,
    wide, step_ref, picked, near, first, second, out_buf, in_buf, rows_buf,
    z_send, z_recv, halo_send, halo_recv, rs_send, rs_recv, g_send, g_recv, row_sem,
):
    me = lax.axis_index("dom")
    group = lax.axis_index("shift")
    planes = own_ref.shape[0] // ny
    nb = own_ref.shape[1]
    slab = planes - 2 * HALO
    rows, depth = slab * ny, HALO * ny
    right, left = wrapped(me + 1, n), wrapped(me + n - 1, n)
    around = [group] + [wrapped(group + t, groups) for t in range(1, groups)]
    up, down = around[1], around[groups - 1]
    has_right, has_left = me < n - 1, me > 0
    shifts = ids_ref.shape[0]
    low, high = edge_flags(me, n)

    barrier = pltpu.get_barrier_semaphore()
    row = n // lines
    base = me // row * row
    for t in range(1, row):
        signal(barrier, dom=base + wrapped(me - base + t, row))
    for t in range(1, lines):
        signal(barrier, dom=wrapped(me + t * row, n))
    for t in range(1, groups):
        signal(barrier, shift=around[t])

    slots = (down, up, around[groups // 2])
    came = passed_ref.shape[1]
    before = (range(came // ny), range(slab - came // ny, slab))
    half = slab // 2

    def planes_at(start, count):
        return pl.ds(depth + start * ny, count * ny)

    def across(way):
        at = planes_at((slab - 1, 0)[way] - (1 - way) * (slab - 1 - came // ny), slab - came // ny)
        return remote(
            own_ref.at[at], wide.at[way, at], z_send.at[0], z_recv.at[way], shift=(up, down)[way]
        )

    def beyond(way):
        at = pl.ds((way * half - before[way][0]) * ny, half * ny)
        return remote(
            passed_ref.at[way, at], wide.at[2, planes_at(way * half, half)],
            z_send.at[0], z_recv.at[2], shift=(up, down)[way],
        )

    def beside(way):
        at = pl.ds((depth + rows, 0)[way], depth)
        return remote(
            own_ref.at[at], wide.at[way, at], z_send.at[0], z_recv.at[3 + way],
            shift=(up, down)[way],
        )

    def halo(index, side, src, first_plane, count):
        target = ((first_plane - (slab - HALO)) * ny, depth + rows + first_plane * ny)[side]
        return remote(
            src, wide.at[index, pl.ds(target, count * ny)],
            halo_send.at[side], halo_recv.at[index, side], dom=(right, left)[side],
        )

    def planes_for(side):
        return range(slab - HALO, slab) if side == 0 else range(HALO)

    def early_halo(index, side):
        mine = [p for p in planes_for(side) if p in before[index]]
        if index != side:
            return
        at = pl.ds((mine[0] - before[index][0]) * ny, len(mine) * ny)
        halo(index, side, passed_ref.at[index, at], mine[0], len(mine)).start()

    def late_halo(index, side):
        mine = [p for p in planes_for(side) if index == 2 or p not in before[index]]
        if mine and index in (side, 2):
            at = planes_at(mine[0], len(mine))
            halo(index, side, wide.at[index, at], mine[0], len(mine)).start()

    def to_both(start):
        pl.when(has_right)(lambda: start(0))
        pl.when(has_left)(lambda: start(1))

    def take_halo(index):
        def take(side):
            drain(wide.at[index, pl.ds(0, depth)], halo_recv.at[index, side])

        if index < 2:
            drain(wide.at[index, pl.ds(0, depth)], z_recv.at[3 + index])
        if index != 1:
            pl.when(has_left)(lambda: take(0))
        if index != 0:
            pl.when(has_right)(lambda: take(1))

    steps = sketch_ref.shape[0] // 2
    pieces = 2
    tall = sketch_ref.shape[1] // (2 * pieces)
    split, columns = SPLIT * nb, BASIS * nb
    chunks = 2 * pieces * tall // (2 * LANES)
    parts = n // nb
    span = chunks // parts
    flat_out = out_buf.reshape(chunks * columns, LANES)

    def part_of(dest):
        return lax.rem(dest, 2) * (parts // 2) + lax.rem(dest // 2, parts // 2)

    def piece(dest):
        return out_buf.at[pl.ds(part_of(dest) * span, span), :, dest // parts]

    def scatter(dest):
        return remote(
            piece(dest), in_buf.at[me, :, pl.ds(0, BASIS)], rs_send.at[0], rs_recv.at[0], dom=dest
        )

    def stage(u):
        tile = jnp.concatenate([weights_ref[2 * u], weights_ref[2 * u + 1]], axis=1)
        for unit in range(2):
            pltpu.matmul_push_rhs(tile, 0, unit, transpose=True)

    def multiply(accs):
        def accumulate(u, part):
            for unit in range(2):
                at = pl.ds((2 * part + unit) * tall, tall)
                tile = jnp.concatenate([sketch_ref[2 * u, at], sketch_ref[2 * u + 1, at]], axis=1)
                pltpu.matmul_acc_lhs(accs[unit], tile, load_staged_rhs=0)

        def run(part, start, stop):
            def step(u, carry):
                accumulate(u, part)
                stage(u + 1)
                return carry

            lax.fori_loop(start, stop, step, 0)

        def finish(part):
            accumulate(steps - 1, part)
            if part + 1 < pieces:
                stage(0)
            odd = lax.rem(lax.broadcasted_iota(jnp.int32, (tall, LANES), 0), 2) == 1
            for unit in range(2):
                value = pltpu.matmul_pop(accs[unit])
                picked[pl.ds((2 * part + unit) * tall, tall)] = jnp.where(
                    odd, value[:, LANES:], value[:, :LANES]
                )
            first = part * 2 * tall
            turned = (
                picked[pl.ds(first, tall, stride=2)] + picked[pl.ds(first + 1, tall, stride=2)]
            ).T
            sketched = jnp.concatenate(
                [turned[:split] + turned[columns:], turned[split:columns]], axis=0
            )
            share = chunks // pieces
            for r in range(share):
                flat_out[pl.ds((part * share + r) * columns, columns)] = sketched[
                    :, r * LANES : (r + 1) * LANES
                ]
            mine = n // pieces
            for t in range(mine):
                dest = pieces * lax.rem(me // pieces + t, mine) + part
                pl.when(dest != me)(lambda: scatter(dest).start())

        stage(0)
        run(0, 0, steps // 2)
        pl.semaphore_wait(barrier, row - 1 + lines - 1 + groups - 1)
        for t in range(1, lines):
            signal(row_sem, dom=wrapped(me + t * row, n))
        for way in range(2):
            across(way).start()
        for way in range(2):
            beyond(way).start()
        for way in range(2):
            beside(way).start()
        run(0, steps // 2, steps - 1)
        pl.semaphore_wait(row_sem, lines - 1)
        for index in range(2):
            to_both(lambda side: early_halo(index, side))
        finish(0)
        run(1, 0, steps - 1)
        finish(1)

    pl.run_scoped(
        lambda *accs: multiply(accs),
        pltpu.ACC(0)((tall, 2 * LANES), F32), pltpu.ACC(1)((tall, 2 * LANES), F32),
    )
    in_buf[me, :, pl.ds(0, BASIS)] = piece(me)[...]

    def clear(at, indices):
        for index in indices:
            wide[index, at] = jnp.zeros((depth, nb, LANES), F32)

    pl.when(jnp.logical_not(has_left))(lambda: clear(pl.ds(0, depth), (0, 2)))
    pl.when(jnp.logical_not(has_right))(lambda: clear(pl.ds(depth + rows, depth), (1, 2)))
    for index in range(2):
        wide[index, planes_at(before[index][0], came // ny)] = passed_ref[index]
    for j in range(shifts):
        step_ref[j] = table_ref[ids_ref[j]] * mass1_ref[...] - kappa_ref[...]

    def split_sums(field, at, acc):
        parts_of = [field[pl.ds(p * ny, ny)].reshape(ny * nb, LANES) for p in at]
        high_parts = [part.astype(BF16) for part in parts_of]
        low_parts = [
            (part - high_part.astype(F32)).astype(BF16)
            for part, high_part in zip(parts_of, high_parts)
        ]
        pltpu.matmul_acc_lhs(acc, jnp.concatenate(high_parts, axis=1))
        pltpu.matmul_acc_lhs(acc, jnp.concatenate(low_parts, axis=1))

    def plane_sum(field, p):
        inner = plane_of(field, p, ny)
        total = plane_of(field, p - 1, ny) + plane_of(field, p + 1, ny)
        none = jnp.zeros((1,) + inner.shape[1:], F32)
        total = total + jnp.concatenate([none, inner[:-1]], axis=0)
        return total + jnp.concatenate([inner[1:], none], axis=0)

    def neighbour_sums(field, start, stop, accs):
        pairs = [(p, p + 1) for p in range(start, stop, 2)]
        for pair, acc in zip(pairs, accs):
            split_sums(field, pair, acc)
        across_planes = [plane_sum(field, p) for p in range(start, stop)]
        for pair, acc in zip(pairs, accs):
            value = pltpu.matmul_pop(acc)
            for i, p in enumerate(pair):
                along = value[:, i * LANES : (i + 1) * LANES].reshape(ny, nb, LANES)
                yield p, across_planes[p - start] + along

    def images(field, slot, accs):
        for p, total in neighbour_sums(field, 1, planes - 1, accs[0]):
            near[pl.ds((p - 1) * ny, ny)] = total

        def shift_pair(u, carry):
            for i in range(2):
                j = 2 * u + i
                for p in range(planes - 2):
                    at = pl.ds(p * ny, ny)
                    flag = edge_flag(p, planes - 2, 2, low, high)
                    first[i, at] = masked(
                        step_ref[j, at] * plane_of(field, p + 1, ny) - near[at], flag
                    )
            for i in range(2):
                j = 2 * u + i
                for p, total in neighbour_sums(first.at[i], 1, planes - 3, accs[i]):
                    at = pl.ds(p * ny, ny)
                    flag = edge_flag(p - 1, planes - 4, 1, low, high)
                    second[i, pl.ds((p - 1) * ny, ny)] = masked(
                        step_ref[j, at] * first[i, at] - total, flag
                    )
            for i in range(2):
                j = 2 * u + i
                for p, total in neighbour_sums(second.at[i], 1, planes - 5, accs[i]):
                    at, inner, out = (pl.ds((p + k) * ny, ny) for k in (1, 0, -1))
                    fields_out[slot, j, 0, out] = first[i, at]
                    fields_out[slot, j, 1, out] = second[i, inner]
                    fields_out[slot, j, 2, out] = step_ref[j, at] * second[i, inner] - total
            return carry

        lax.fori_loop(0, shifts // 2, shift_pair, 0)
        for p in range(slab):
            own_out[slot, pl.ds(p * ny, ny)] = plane_of(field, p + HALO, ny)

    def after(*accs):
        accs = (accs[:4], accs[4:])
        here = lax.broadcasted_iota(jnp.int32, (2 * LANES, 2 * LANES), 0)
        there = lax.broadcasted_iota(jnp.int32, (2 * LANES, 2 * LANES), 1)
        beside = (jnp.abs(here - there) == 1) & (here // LANES == there // LANES)
        neighbours = jnp.where(beside, 1.0, 0.0).astype(BF16)
        for unit in range(2):
            pltpu.matmul_push_rhs(neighbours, 0, unit)
            pltpu.matmul_acc_lhs(
                accs[0][unit], jnp.zeros((ny * nb, 2 * LANES), BF16), load_staged_rhs=0
            )
        for way in range(2):
            across(way).wait_recv()
            to_both(lambda side: late_halo(way, side))
        images(own_ref, group, accs)
        drain(wide.at[2, pl.ds(depth, rows)], z_recv.at[2])
        to_both(lambda side: late_halo(2, side))
        peers = pl.ds(0, n - 1)
        drain(in_buf.at[peers, :, pl.ds(0, BASIS)], rs_recv.at[0])
        flat_in = in_buf.reshape(n * span * in_buf.shape[2], LANES)
        tile = span * in_buf.shape[2]
        total = flat_in[pl.ds(0, tile)]
        for t in range(1, n):
            total = total + flat_in[pl.ds(t * tile, tile)]
        lane = lax.broadcasted_iota(jnp.int32, (BASIS, LANES), 1)
        place = lax.broadcasted_iota(jnp.int32, (BASIS, LANES), 0)
        views = [total[r * in_buf.shape[2] :][:BASIS] for r in range(span)]
        twice = [jnp.concatenate([view, view], axis=0) for view in views]
        packed = jnp.zeros((BASIS, LANES), F32)
        for d in range(BASIS // 2 + 1):
            terms = sum(view * wrap[d : d + BASIS] for view, wrap in zip(views, twice))
            packed = jnp.where(lane == place + BASIS * d, jnp.sum(terms, axis=1, keepdims=True), packed)
        slot = group * n + part_of(me) * nb + me // parts
        rows_buf[slot] = jnp.sum(packed, axis=0, keepdims=True)

        def share(t, z):
            return remote(
                rows_buf.at[slot], rows_buf.at[slot], g_send.at[0], g_recv.at[0],
                dom=wrapped(me + t, n), shift=around[z],
            )

        for z in (2, 1, 3, 0):
            for t in range(n):
                if z or t:
                    share(t, z).start()
        take_halo(0)
        images(wide.at[0], slots[0], accs)
        take_halo(1)
        images(wide.at[1], slots[1], accs)
        take_halo(2)
        images(wide.at[2], slots[2], accs)
        everyone = pl.ds(0, groups * n - 1)
        drain(rows_buf.at[everyone], g_recv.at[0])

        lane_row = lax.broadcasted_iota(jnp.int32, (1, LANES), 1)
        sigma = jnp.full((1, LANES), MID, F32)
        for j in range(shifts):
            sigma = jnp.where(lane_row == j, table_ref[ids_ref[j]], sigma)
        flat_rows = rows_buf.reshape(groups * n, LANES)
        gram = []
        for g in range(groups):
            block = flat_rows[pl.ds(g * n, n)]
            gram.append(sum(block[q * nb : (q + 1) * nb] for q in range(parts)))
        solved = coefficients(jnp.concatenate(gram, axis=0), sigma)
        for i, value in enumerate(solved):
            for j in range(shifts):
                spreaded = jnp.broadcast_to(value[:, j : j + 1], value.shape)
                coeff_out[j, i] = spreaded.reshape(groups, nb, LANES)

        to_both(lambda side: drain(wide.at[pl.ds(0, 2), pl.ds(0, depth)], halo_send.at[side]))
        drain(wide.at[pl.ds(0, 2), pl.ds(0, rows - came + half * ny + depth)], z_send.at[0])
        drain(in_buf.at[peers, :, pl.ds(0, BASIS)], rs_send.at[0])
        drain(rows_buf.at[everyone], g_send.at[0])

    unit_sums = [pltpu.ACC(i % 2)((ny * nb, 2 * LANES), F32) for i in range(8)]
    pl.run_scoped(after, *unit_sums)


def combine_kernel(fields_ref, own_ref, coeff_ref, sol_hbm, res_hbm, sol_buf, res_buf, sem):
    groups, shifts = fields_ref.shape[0], fields_ref.shape[1]
    rows, nb = fields_ref.shape[3], fields_ref.shape[4]

    def copies(g, j):
        out = []
        for which, (buf, hbm) in enumerate(((sol_buf, sol_hbm), (res_buf, res_hbm))):
            for b in range(nb):
                out.append(
                    pltpu.make_async_copy(
                        buf.at[g, j, :, b], hbm.at[j, g * nb + b], sem.at[which]
                    )
                )
        return out

    def one(u, carry):
        g, j = u // shifts, lax.rem(u, shifts)
        c = [coeff_ref[j, i, g][None] for i in range(6)]
        w0 = own_ref[g]
        w1, w2, w3 = (fields_ref[g, j, i] for i in range(3))
        sol_buf.at[g, j].reshape(rows, nb, LANES)[...] = c[0] * w0 + c[1] * w1 + c[2] * w2
        res_buf.at[g, j].reshape(rows, nb, LANES)[...] = (
            c[3] * w0 - c[4] * w1 - c[5] * w2 - c[2] * w3
        )
        for copy in copies(g, j):
            copy.start()
        return carry

    lax.fori_loop(0, groups * shifts, one, 0)

    drain(sol_hbm, sem.at[0])
    drain(res_hbm, sem.at[1])


def on_device(sources, kappa, mass, shift_table, shift_ids, sketch):
    n, groups = lax.axis_size("dom"), lax.axis_size("shift")
    nb, slab, ny = sources.shape[0], sources.shape[1], sources.shape[2]
    shifts = shift_ids.shape[0]
    sk = sketch.shape[0]
    rows = slab * ny
    planes = slab + 2 * HALO
    wide_rows, inner = planes * ny, (planes - 2) * ny
    pairs = rows // 2
    weights = 2 * (BASIS + SPLIT) * nb
    vec = (nb, LANES)
    held = PASSED * ny
    sketch, weight, wide, passed, kappa, mass = pl.pallas_call(
        functools.partial(prepare_kernel, n, groups, ny),
        out_shape=(
            pltpu.VMEM((pairs, sk, 2, LANES), BF16),
            pltpu.VMEM((pairs, weights, LANES), BF16),
            pltpu.VMEM((wide_rows, nb, 1, LANES), F32),
            pltpu.VMEM((2, held, nb, 1, LANES), F32),
            pltpu.VMEM((inner,) + vec, F32),
            pltpu.VMEM((inner,) + vec, F32),
        ),
        in_specs=[HBM_SPEC] * 4,
        out_specs=(VMEM_SPEC,) * 6,
        scratch_shapes=[
            pltpu.VMEM((2, inner, 1, LANES), F32),
            pltpu.VMEM((inner,) + vec, F32),
            pltpu.VMEM((inner,) + vec, F32),
            pltpu.VMEM((inner,) + vec, F32),
            pltpu.VMEM((inner - 2 * ny,) + vec, F32),
            pltpu.VMEM((inner - 2 * ny,) + vec, F32),
            pltpu.VMEM((inner - 2 * ny,) + vec, F32),
            DMA((1,)), DMA((2,)),
            DMA((2,)), DMA((HALO, 2)), DMA((2,)), DMA((2,)), DMA((1,)), DMA((2,)),
        ],
        compiler_params=pltpu.CompilerParams(
            collective_id=0, has_side_effects=True, vmem_limit_bytes=16 << 20
        ),
        name="prepare",
    )(
        in_hbm(sources.reshape(nb, rows, 1, LANES)), in_hbm(kappa.reshape(rows, 1, LANES)),
        in_hbm(mass.reshape(rows, 1, LANES)), in_hbm(sketch.reshape(sk, pairs, 2, LANES)),
    )
    parts = n // nb
    span = sk // LANES // parts
    fields, own, coeff = pl.pallas_call(
        functools.partial(project_kernel, n, groups, LINES, ny),
        out_shape=(
            pltpu.VMEM((groups, shifts, 3, rows) + vec, F32),
            pltpu.VMEM((groups, rows) + vec, F32),
            pltpu.VMEM((shifts, 6, groups) + vec, F32),
        ),
        in_specs=[VMEM_SPEC] * 6 + [SMEM_SPEC] * 2,
        out_specs=(VMEM_SPEC,) * 3,
        scratch_shapes=[
            pltpu.VMEM((groups - 1, wide_rows) + vec, F32),
            pltpu.VMEM((shifts, inner) + vec, F32),
            pltpu.VMEM((2 * sk, weights // 2), F32),
            pltpu.VMEM((inner,) + vec, F32),
            pltpu.VMEM((2, inner) + vec, F32),
            pltpu.VMEM((2, inner - 2 * ny) + vec, F32),
            pltpu.VMEM((sk // LANES, BASIS, nb, 1, LANES), F32),
            pltpu.VMEM((n, span, 16, 1, LANES), F32),
            pltpu.VMEM((groups * n, 1, LANES), F32),
            DMA((1,)), DMA((5,)), DMA((2,)), DMA((3, 2)),
            DMA((1,)), DMA((1,)), DMA((1,)), DMA((1,)), pltpu.SemaphoreType.REGULAR,
        ],
        compiler_params=pltpu.CompilerParams(
            collective_id=1, has_side_effects=True, vmem_limit_bytes=16 << 20
        ),
        name="project",
    )(
        in_vmem(sketch.reshape(pairs, 2 * sk, LANES)), in_vmem(weight),
        in_vmem(wide.reshape((wide_rows,) + vec)), in_vmem(passed.reshape((2, held) + vec)),
        in_vmem(kappa), in_vmem(mass), shift_table, shift_ids,
    )

    out = pltpu.HBM((shifts, groups * nb, rows, 1, LANES), F32)
    buf = pltpu.VMEM((groups, shifts, rows, nb, 1, LANES), F32)
    solution, residual = pl.pallas_call(
        combine_kernel,
        out_shape=(out, out),
        in_specs=[VMEM_SPEC] * 3,
        out_specs=(HBM_SPEC,) * 2,
        scratch_shapes=[buf, buf, DMA((2,))],
        compiler_params=pltpu.CompilerParams(vmem_limit_bytes=16 << 20),
        name="combine",
    )(in_vmem(fields), in_vmem(own), in_vmem(coeff))
    shape = (shifts, groups * nb, slab, ny, LANES)
    return solution.reshape(shape), residual.reshape(shape)


def solution(mesh):
    placed = (
        P("shift", "dom", None, None),
        P("dom", None, None),
        P("dom", None, None),
        P(),
        P("shift"),
        P(None, "dom", None, None),
    )
    return jax.shard_map(
        on_device,
        mesh=mesh,
        in_specs=placed,
        out_specs=(P("shift", None, "dom", None, None), P("shift", None, "dom", None, None)),
        check_vma=False,
    )
```

```python
import functools

import jax
import jax.numpy as jnp
from jax import lax
from jax.experimental import pallas as pl
from jax.experimental.pallas import tpu as pltpu
from jax.sharding import PartitionSpec as P

HALO = 3
LANES = 128
MID = 2.25
F32 = jnp.float32
BF16 = jnp.bfloat16
BASIS = 10
PASSED = 3
LINES = 4
SPLIT = 6
IMAGES = ((0,), (1, 6), (2, 3, 7), (4, 5, 8, 9))
VMEM_SPEC = pl.BlockSpec(memory_space=pltpu.VMEM)
HBM_SPEC = pl.BlockSpec(memory_space=pltpu.HBM)
SMEM_SPEC = pl.BlockSpec(memory_space=pltpu.SMEM)
DMA = pltpu.SemaphoreType.DMA


def in_hbm(array):
    return pltpu.with_memory_space_constraint(array, pltpu.HBM)


def in_vmem(array):
    return pltpu.with_memory_space_constraint(array, pltpu.VMEM)


def remote(src, dst, send, recv, **where):
    return pltpu.make_async_remote_copy(
        src_ref=src, dst_ref=dst, send_sem=send, recv_sem=recv,
        device_id=where, device_id_type=pl.DeviceIdType.MESH,
    )


def signal(sem, **where):
    pl.semaphore_signal(sem, inc=1, device_id=where, device_id_type=pl.DeviceIdType.MESH)


def wrapped(index, size):
    return jnp.where(index >= size, index - size, index)


def drain(ref, sem):
    pltpu.make_async_copy(ref, ref, sem).wait()


def plane_of(ref, p, ny):
    return ref[pl.ds(p * ny, ny)]


def neighbour_sum(ref, p, ny):
    inner = plane_of(ref, p, ny)
    total = plane_of(ref, p - 1, ny) + plane_of(ref, p + 1, ny)
    none = jnp.zeros((1,) + inner.shape[1:], F32)
    total = total + jnp.concatenate([none, inner[:-1]], axis=0)
    total = total + jnp.concatenate([inner[1:], none], axis=0)
    lane = lax.broadcasted_iota(jnp.int32, inner.shape, 2)
    total = total + jnp.where(lane > 0, pltpu.roll(inner, 1, 2), 0.0)
    return total + jnp.where(lane < LANES - 1, pltpu.roll(inner, LANES - 1, 2), 0.0)


def edge_flag(p, planes, width, low, high):
    if p < width:
        return low
    return high if p >= planes - width else None


def masked(value, flag):
    return value if flag is None else value * flag


def edge_flags(me, n):
    return (me > 0).astype(F32), (me < n - 1).astype(F32)


def prepare_kernel(
    n, groups, ny, src_hbm, kappa_hbm, mass_hbm, sketch_hbm,
    sketch_out, weights_out, wide, passed_out, kappa_out, mass1,
    coef, diag, g0, g1, h0, h1, h2,
    load_sem, in_sem, wide_send, wide_recv, coef_send, coef_recv, z_send, z_recv,
):
    me = lax.axis_index("dom")
    group = lax.axis_index("shift")
    nb, rows = src_hbm.shape[0], src_hbm.shape[1]
    slab = rows // ny
    right, left = wrapped(me + 1, n), wrapped(me + n - 1, n)
    up, down = wrapped(group + 1, groups), wrapped(group + groups - 1, groups)
    has_right, has_left = me < n - 1, me > 0
    depth = HALO * ny
    thin = (HALO - 1) * ny
    planes = slab + 2 * HALO

    barrier = pltpu.get_barrier_semaphore()
    inputs = [
        pltpu.make_async_copy(src_hbm.at[b], wide.at[pl.ds(depth, rows), b], in_sem.at[0])
        for b in range(nb)
    ]
    inputs.append(pltpu.make_async_copy(kappa_hbm, coef.at[0, pl.ds(thin, rows)], in_sem.at[1]))
    inputs.append(pltpu.make_async_copy(mass_hbm, coef.at[1, pl.ds(thin, rows)], in_sem.at[1]))
    for copy in inputs:
        copy.start()

    @pl.when(has_right)
    def _():
        signal(barrier, dom=right)

    @pl.when(has_left)
    def _():
        signal(barrier, dom=left)

    signal(barrier, shift=up)
    signal(barrier, shift=down)

    def load(k):
        return pltpu.make_async_copy(sketch_hbm.at[:, k], sketch_out.at[k], load_sem.at[0])

    loads = sketch_hbm.shape[1]
    for k in range(loads):
        load(k).start()
    drain(wide.at[pl.ds(depth, rows)], in_sem.at[0])
    drain(coef.at[:, pl.ds(thin, rows)], in_sem.at[1])

    def wide_halo(k, side):
        first, target, there = (
            (depth + rows - (k + 1) * ny, depth - (k + 1) * ny, right),
            (depth + k * ny, depth + rows + k * ny, left),
        )[side]
        return remote(
            wide.at[pl.ds(first, ny)], wide.at[pl.ds(target, ny)],
            wide_send.at[side], wide_recv.at[k, side], dom=there,
        )

    def coef_halo(side):
        first, target, there = ((rows, 0, right), (thin, thin + rows, left))[side]
        return remote(
            coef.at[:, pl.ds(first, thin)], coef.at[:, pl.ds(target, thin)],
            coef_send.at[side], coef_recv.at[side], dom=there,
        )

    def pass_on(way):
        count = passed_out.shape[1]
        there = (up, down)[way]
        return remote(
            wide.at[pl.ds(depth + way * (rows - count), count)], passed_out.at[way],
            z_send.at[0], z_recv.at[way], shift=there,
        )

    pl.semaphore_wait(barrier, has_right.astype(jnp.int32) + has_left.astype(jnp.int32) + 2)

    def send_halo(side):
        wide_halo(0, side).start()
        coef_halo(side).start()
        for k in range(1, HALO):
            wide_halo(k, side).start()

    pl.when(has_right)(lambda: send_halo(0))
    pl.when(has_left)(lambda: send_halo(1))
    for way in range(2):
        pass_on(way).start()

    field = wide.reshape(wide.shape[0], nb, LANES)

    @pl.when(jnp.logical_not(has_left))
    def _():
        field[pl.ds(0, depth)] = jnp.zeros((depth, nb, LANES), F32)
        coef[:, pl.ds(0, thin)] = jnp.zeros((2, thin, 1, LANES), F32)

    @pl.when(jnp.logical_not(has_right))
    def _():
        field[pl.ds(depth + rows, depth)] = jnp.zeros((depth, nb, LANES), F32)
        coef[:, pl.ds(thin + rows, thin)] = jnp.zeros((2, thin, 1, LANES), F32)

    full = (ny, nb, LANES)
    low, high = edge_flags(me, n)

    def factors(p):
        at = pl.ds(p * ny, ny)
        k = jnp.broadcast_to(coef[0, at], full)
        m = jnp.broadcast_to(coef[1, at] - 1.0, full)
        diag[at] = MID * m - k
        mass1[at] = m
        kappa_out[at] = k

    def level1(p):
        flag = edge_flag(p, planes - 2, 2, low, high)
        w = plane_of(field, p + 1, ny)
        out = pl.ds(p * ny, ny)
        g0[out] = masked(diag[out] * w - neighbour_sum(field, p + 1, ny), flag)
        g1[out] = mass1[out] * w

    def level2(p):
        flag = edge_flag(p, planes - 4, 1, low, high)
        at, out = pl.ds((p + 1) * ny, ny), pl.ds(p * ny, ny)
        d, m = diag[at], mass1[at]
        u0, u1 = g0[at], g1[at]
        h0[out] = masked(d * u0 - neighbour_sum(g0, p + 1, ny), flag)
        h1[out] = masked(d * u1 - neighbour_sum(g1, p + 1, ny) + m * u0, flag)
        h2[out] = m * u1

    def level3(p):
        at, inner = pl.ds((p + 2) * ny, ny), pl.ds((p + 1) * ny, ny)
        d, m = diag[at], mass1[at]
        v0, v1, v2 = h0[inner], h1[inner], h2[inner]
        e0 = d * v0 - neighbour_sum(h0, p + 1, ny)
        e1 = d * v1 - neighbour_sum(h1, p + 1, ny) + m * v0
        e2 = d * v2 - neighbour_sum(h2, p + 1, ny) + m * v1
        e3 = m * v2
        first = jnp.concatenate(
            [plane_of(field, p + HALO, ny), g0[at], v0, v1, e0, e1], axis=1
        )
        second = jnp.concatenate([g1[at], v2, e2, e3], axis=1)
        high_part = first.astype(BF16)
        low_part = (first - high_part.astype(F32)).astype(BF16)
        columns = jnp.concatenate([high_part, second.astype(BF16), low_part], axis=1)
        pairs = ny // 2
        weights_out[pl.ds(p * pairs, pairs)] = columns.reshape(pairs, 2 * columns.shape[1], LANES)

    done = [set(), set(), set(), set()]

    def advance(reach):
        ready = set(range(HALO - reach, planes - HALO + reach))
        if reach != 1:
            coefs = range(2, planes - 4) if reach == 0 else (0, 1, planes - 4, planes - 3)
            for p in (coefs if reach in (0, 2) else ()):
                factors(p)
        usable = range(2, planes - 4) if reach < 2 else range(planes - 2)
        for p in range(planes - 2):
            if p not in done[1] and {p, p + 1, p + 2} <= ready and p in usable:
                level1(p)
                done[1].add(p)
        for p in range(planes - 4):
            if p not in done[2] and {p, p + 1, p + 2} <= done[1]:
                level2(p)
                done[2].add(p)
        for p in range(slab):
            if p not in done[3] and {p, p + 1, p + 2} <= done[2]:
                level3(p)
                done[3].add(p)

    def clear_units(*accs):
        for acc in accs:
            pltpu.matmul_pop(acc)

    advance(0)
    pl.run_scoped(
        clear_units,
        pltpu.ACC(0)((sketch_hbm.shape[0], 2 * LANES), F32),
        pltpu.ACC(1)((sketch_hbm.shape[0], 2 * LANES), F32),
    )
    pl.when(has_left)(lambda: wide_halo(0, 0).wait_recv())
    pl.when(has_right)(lambda: wide_halo(0, 1).wait_recv())
    advance(1)

    def take(side):
        coef_halo(side).wait_recv()
        wide_halo(1, side).wait_recv()

    pl.when(has_left)(lambda: take(0))
    pl.when(has_right)(lambda: take(1))
    advance(2)
    pl.when(has_left)(lambda: wide_halo(2, 0).wait_recv())
    pl.when(has_right)(lambda: wide_halo(2, 1).wait_recv())
    advance(3)
    for way in range(2):
        pass_on(way).wait_recv()
    drain(sketch_out, load_sem.at[0])

    def sent(side):
        drain(wide.at[pl.ds(0, depth)], wide_send.at[side])
        drain(coef.at[:, pl.ds(0, thin)], coef_send.at[side])

    pl.when(has_right)(lambda: sent(0))
    pl.when(has_left)(lambda: sent(1))
    drain(wide.at[pl.ds(0, 2 * passed_out.shape[1])], z_send.at[0])


def solve_small(h_vals, entry):
    l00 = jnp.sqrt(entry[0][0])
    l10 = entry[1][0] / l00
    l20 = entry[2][0] / l00
    l11 = jnp.sqrt(entry[1][1] - l10 * l10)
    l21 = (entry[2][1] - l20 * l10) / l11
    l22 = jnp.sqrt(entry[2][2] - l20 * l20 - l21 * l21)
    f0 = h_vals[0] / l00
    f1 = (h_vals[1] - l10 * f0) / l11
    f2 = (h_vals[2] - l20 * f0 - l21 * f1) / l22
    c2 = f2 / l22
    c1 = (f1 - l21 * c2) / l11
    c0 = (f0 - l10 * c1 - l20 * c2) / l00
    return (c0, c1, c2)


def pair_lane(i, k):
    distance = (k - i) % BASIS
    if distance <= BASIS // 2:
        return BASIS * distance + i
    return BASIS * (BASIS - distance) + k


def coefficients(gram, sigma):
    tau, center = sigma - MID, sigma + 6.0

    def product(left, right):
        by_degree = {}
        for p, i in enumerate(IMAGES[left]):
            for q, k in enumerate(IMAGES[right]):
                at = pair_lane(i, k)
                column = gram[:, at : at + 1]
                by_degree[p + q] = by_degree[p + q] + column if p + q in by_degree else column
        top = max(by_degree)
        total = jnp.broadcast_to(by_degree[top], gram.shape)
        for degree in range(top - 1, -1, -1):
            total = total * tau + by_degree[degree]
        return total

    ww = [[product(i, k) if i <= k else None for k in range(4)] for i in range(4)]

    def between(i, k):
        total = ww[i][k]
        if i > 0:
            total = total + center * ww[i - 1][k]
        if k > 0:
            low = ww[min(i, k - 1)][max(i, k - 1)]
            if i > 0:
                low = low + center * ww[i - 1][k - 1]
            total = total + center * low
        return total

    scale = (1.0, 1.0, 1.0 / 6.0, 1.0 / 36.0)
    h_vals = [between(0, i) * scale[i] for i in (1, 2, 3)]
    entry = [[None] * 3 for _ in range(3)]
    for i in range(3):
        for k in range(i + 1):
            entry[i][k] = between(k + 1, i + 1) * (scale[i + 1] * scale[k + 1])
    ridge = 0.001 * (entry[0][0] + entry[1][1] + entry[2][2]) / 3.0 + 1.0
    for i in range(3):
        entry[i][i] = entry[i][i] + ridge
    c0, c1, c2 = solve_small(h_vals, entry)
    c1, c2 = c1 * (1.0 / 6.0), c2 * (1.0 / 36.0)
    return (c0, c1, c2, 1.0 - c0 * center, c0 + c1 * center, c1 + c2 * center)


def project_kernel(
    n, groups, lines, ny, sketch_ref, weights_ref, own_ref, passed_ref, kappa_ref, mass1_ref, table_ref, ids_ref,
    fields_out, own_out, coeff_out,
    wide, step_ref, picked, near, first, second, out_buf, in_buf, rows_buf,
    z_send, z_recv, halo_send, halo_recv, rs_send, rs_recv, g_send, g_recv, row_sem,
):
    me = lax.axis_index("dom")
    group = lax.axis_index("shift")
    planes = own_ref.shape[0] // ny
    nb = own_ref.shape[1]
    slab = planes - 2 * HALO
    rows, depth = slab * ny, HALO * ny
    right, left = wrapped(me + 1, n), wrapped(me + n - 1, n)
    around = [group] + [wrapped(group + t, groups) for t in range(1, groups)]
    up, down = around[1], around[groups - 1]
    has_right, has_left = me < n - 1, me > 0
    shifts = ids_ref.shape[0]
    low, high = edge_flags(me, n)

    barrier = pltpu.get_barrier_semaphore()
    row = n // lines
    base = me // row * row
    for t in range(1, row):
        signal(barrier, dom=base + wrapped(me - base + t, row))
    for t in range(1, lines):
        signal(barrier, dom=wrapped(me + t * row, n))
    for t in range(1, groups):
        signal(barrier, shift=around[t])

    slots = (down, up, around[groups // 2])
    came = passed_ref.shape[1]
    before = (range(came // ny), range(slab - came // ny, slab))
    half = slab // 2

    def planes_at(start, count):
        return pl.ds(depth + start * ny, count * ny)

    def across(way):
        at = planes_at((slab - 1, 0)[way] - (1 - way) * (slab - 1 - came // ny), slab - came // ny)
        return remote(
            own_ref.at[at], wide.at[way, at], z_send.at[0], z_recv.at[way], shift=(up, down)[way]
        )

    def beyond(way):
        at = pl.ds((way * half - before[way][0]) * ny, half * ny)
        return remote(
            passed_ref.at[way, at], wide.at[2, planes_at(way * half, half)],
            z_send.at[0], z_recv.at[2], shift=(up, down)[way],
        )

    def beside(way):
        at = pl.ds((depth + rows, 0)[way], depth)
        return remote(
            own_ref.at[at], wide.at[way, at], z_send.at[0], z_recv.at[3 + way],
            shift=(up, down)[way],
        )

    def relay(way):
        at = pl.ds((depth + rows, 0)[way], depth)
        return remote(
            wide.at[way, at], wide.at[2, at], z_send.at[0], z_recv.at[5 + way], shift=(up, down)[way]
        )

    def halo(index, side, src, first_plane, count):
        target = ((first_plane - (slab - HALO)) * ny, depth + rows + first_plane * ny)[side]
        return remote(
            src, wide.at[index, pl.ds(target, count * ny)],
            halo_send.at[side], halo_recv.at[index, side], dom=(right, left)[side],
        )

    def planes_for(side):
        return range(slab - HALO, slab) if side == 0 else range(HALO)

    def early_halo(index, side):
        mine = [p for p in planes_for(side) if p in before[index]]
        if index != side:
            return
        at = pl.ds((mine[0] - before[index][0]) * ny, len(mine) * ny)
        halo(index, side, passed_ref.at[index, at], mine[0], len(mine)).start()

    def late_halo(index, side):
        mine = [p for p in planes_for(side) if p not in before[index]]
        if mine and index == side:
            at = planes_at(mine[0], len(mine))
            halo(index, side, wide.at[index, at], mine[0], len(mine)).start()

    def to_both(start):
        pl.when(has_right)(lambda: start(0))
        pl.when(has_left)(lambda: start(1))

    def take_halo(index):
        def take(side):
            drain(wide.at[index, pl.ds(0, depth)], halo_recv.at[index, side])

        if index == 0:
            pl.when(has_left)(lambda: take(0))
        if index == 1:
            pl.when(has_right)(lambda: take(1))
        if index == 2:
            for way in range(2):
                drain(wide.at[2, pl.ds(0, depth)], z_recv.at[5 + way])

    steps = sketch_ref.shape[0] // 2
    pieces = 2
    tall = sketch_ref.shape[1] // (2 * pieces)
    split, columns = SPLIT * nb, BASIS * nb
    chunks = 2 * pieces * tall // (2 * LANES)
    parts = n // nb
    span = chunks // parts
    flat_out = out_buf.reshape(chunks * columns, LANES)

    def part_of(dest):
        return lax.rem(dest, 2) * (parts // 2) + lax.rem(dest // 2, parts // 2)

    def piece(dest):
        return out_buf.at[pl.ds(part_of(dest) * span, span), :, dest // parts]

    def scatter(dest):
        return remote(
            piece(dest), in_buf.at[me, :, pl.ds(0, BASIS)], rs_send.at[0], rs_recv.at[0], dom=dest
        )

    def stage(u):
        tile = jnp.concatenate([weights_ref[2 * u], weights_ref[2 * u + 1]], axis=1)
        for unit in range(2):
            pltpu.matmul_push_rhs(tile, 0, unit, transpose=True)

    def multiply(accs):
        def accumulate(u, part):
            for unit in range(2):
                at = pl.ds((2 * part + unit) * tall, tall)
                tile = jnp.concatenate([sketch_ref[2 * u, at], sketch_ref[2 * u + 1, at]], axis=1)
                pltpu.matmul_acc_lhs(accs[unit], tile, load_staged_rhs=0)

        def run(part, start, stop):
            def step(u, carry):
                accumulate(u, part)
                stage(u + 1)
                return carry

            lax.fori_loop(start, stop, step, 0)

        def collect(part):
            accumulate(steps - 1, part)
            if part + 1 < pieces:
                stage(0)
            odd = lax.rem(lax.broadcasted_iota(jnp.int32, (tall, LANES), 0), 2) == 1
            for unit in range(2):
                value = pltpu.matmul_pop(accs[unit])
                picked[pl.ds((2 * part + unit) * tall, tall)] = jnp.where(
                    odd, value[:, LANES:], value[:, :LANES]
                )
            first = part * 2 * tall
            turned = (
                picked[pl.ds(first, tall, stride=2)] + picked[pl.ds(first + 1, tall, stride=2)]
            ).T
            sketched = jnp.concatenate(
                [turned[:split] + turned[columns:], turned[split:columns]], axis=0
            )
            share = chunks // pieces
            for r in range(share):
                flat_out[pl.ds((part * share + r) * columns, columns)] = sketched[
                    :, r * LANES : (r + 1) * LANES
                ]

        def send(part):
            mine = n // pieces
            for t in range(mine):
                dest = pieces * lax.rem(me // pieces + t, mine) + part
                pl.when(dest != me)(lambda: scatter(dest).start())

        stage(0)
        run(0, 0, steps - 1)
        pl.semaphore_wait(barrier, row - 1 + lines - 1 + groups - 1)
        for t in range(1, lines):
            signal(row_sem, dom=wrapped(me + t * row, n))
        for way in range(2):
            across(way).start()
        for way in range(2):
            beside(way).start()
        for way in range(2):
            beyond(way).start()
        collect(0)
        run(1, 0, steps // 2)
        pl.semaphore_wait(row_sem, lines - 1)
        send(0)
        for index in range(2):
            to_both(lambda side: early_halo(index, side))
        run(1, steps // 2, steps - 1)
        collect(1)
        send(1)

    pl.run_scoped(
        lambda *accs: multiply(accs),
        pltpu.ACC(0)((tall, 2 * LANES), F32), pltpu.ACC(1)((tall, 2 * LANES), F32),
    )
    in_buf[me, :, pl.ds(0, BASIS)] = piece(me)[...]

    def clear(at, indices):
        for index in indices:
            wide[index, at] = jnp.zeros((depth, nb, LANES), F32)

    pl.when(jnp.logical_not(has_left))(lambda: clear(pl.ds(0, depth), (0,)))
    pl.when(jnp.logical_not(has_right))(lambda: clear(pl.ds(depth + rows, depth), (1,)))
    for index in range(2):
        wide[index, planes_at(before[index][0], came // ny)] = passed_ref[index]
    for j in range(shifts):
        step_ref[j] = table_ref[ids_ref[j]] * mass1_ref[...] - kappa_ref[...]

    def split_sums(field, at, acc):
        parts_of = [field[pl.ds(p * ny, ny)].reshape(ny * nb, LANES) for p in at]
        high_parts = [part.astype(BF16) for part in parts_of]
        low_parts = [
            (part - high_part.astype(F32)).astype(BF16)
            for part, high_part in zip(parts_of, high_parts)
        ]
        pltpu.matmul_acc_lhs(acc, jnp.concatenate(high_parts, axis=1))
        pltpu.matmul_acc_lhs(acc, jnp.concatenate(low_parts, axis=1))

    def plane_sum(field, p):
        inner = plane_of(field, p, ny)
        total = plane_of(field, p - 1, ny) + plane_of(field, p + 1, ny)
        none = jnp.zeros((1,) + inner.shape[1:], F32)
        total = total + jnp.concatenate([none, inner[:-1]], axis=0)
        return total + jnp.concatenate([inner[1:], none], axis=0)

    def neighbour_sums(field, start, stop, accs):
        pairs = [(p, p + 1) for p in range(start, stop, 2)]
        for pair, acc in zip(pairs, accs):
            split_sums(field, pair, acc)
        across_planes = [plane_sum(field, p) for p in range(start, stop)]
        for pair, acc in zip(pairs, accs):
            value = pltpu.matmul_pop(acc)
            for i, p in enumerate(pair):
                along = value[:, i * LANES : (i + 1) * LANES].reshape(ny, nb, LANES)
                yield p, across_planes[p - start] + along

    def images(field, slot, accs):
        for p, total in neighbour_sums(field, 1, planes - 1, accs[0]):
            near[pl.ds((p - 1) * ny, ny)] = total

        def shift_pair(u, carry):
            for i in range(2):
                j = 2 * u + i
                for p in range(planes - 2):
                    at = pl.ds(p * ny, ny)
                    flag = edge_flag(p, planes - 2, 2, low, high)
                    first[i, at] = masked(
                        step_ref[j, at] * plane_of(field, p + 1, ny) - near[at], flag
                    )
            for i in range(2):
                j = 2 * u + i
                for p, total in neighbour_sums(first.at[i], 1, planes - 3, accs[i]):
                    at = pl.ds(p * ny, ny)
                    flag = edge_flag(p - 1, planes - 4, 1, low, high)
                    second[i, pl.ds((p - 1) * ny, ny)] = masked(
                        step_ref[j, at] * first[i, at] - total, flag
                    )
            for i in range(2):
                j = 2 * u + i
                for p, total in neighbour_sums(second.at[i], 1, planes - 5, accs[i]):
                    at, inner, out = (pl.ds((p + k) * ny, ny) for k in (1, 0, -1))
                    fields_out[slot, j, 0, out] = first[i, at]
                    fields_out[slot, j, 1, out] = second[i, inner]
                    fields_out[slot, j, 2, out] = step_ref[j, at] * second[i, inner] - total
            return carry

        lax.fori_loop(0, shifts // 2, shift_pair, 0)
        for p in range(slab):
            own_out[slot, pl.ds(p * ny, ny)] = plane_of(field, p + HALO, ny)

    def after(*accs):
        accs = (accs[:4], accs[4:])
        here = lax.broadcasted_iota(jnp.int32, (2 * LANES, 2 * LANES), 0)
        there = lax.broadcasted_iota(jnp.int32, (2 * LANES, 2 * LANES), 1)
        beside = (jnp.abs(here - there) == 1) & (here // LANES == there // LANES)
        neighbours = jnp.where(beside, 1.0, 0.0).astype(BF16)
        for unit in range(2):
            pltpu.matmul_push_rhs(neighbours, 0, unit)
            pltpu.matmul_acc_lhs(
                accs[0][unit], jnp.zeros((ny * nb, 2 * LANES), BF16), load_staged_rhs=0
            )
        for way in range(2):
            across(way).wait_recv()
            to_both(lambda side: late_halo(way, side))
        images(own_ref, group, accs)
        for way in range(2):
            drain(wide.at[way, pl.ds(0, depth)], z_recv.at[3 + way])
            relay(way).start()
        peers = pl.ds(0, n - 1)
        drain(in_buf.at[peers, :, pl.ds(0, BASIS)], rs_recv.at[0])
        flat_in = in_buf.reshape(n * span * in_buf.shape[2], LANES)
        tile = span * in_buf.shape[2]
        total = flat_in[pl.ds(0, tile)]
        for t in range(1, n):
            total = total + flat_in[pl.ds(t * tile, tile)]
        lane = lax.broadcasted_iota(jnp.int32, (BASIS, LANES), 1)
        place = lax.broadcasted_iota(jnp.int32, (BASIS, LANES), 0)
        views = [total[r * in_buf.shape[2] :][:BASIS] for r in range(span)]
        twice = [jnp.concatenate([view, view], axis=0) for view in views]
        packed = jnp.zeros((BASIS, LANES), F32)
        for d in range(BASIS // 2 + 1):
            terms = sum(view * wrap[d : d + BASIS] for view, wrap in zip(views, twice))
            packed = jnp.where(lane == place + BASIS * d, jnp.sum(terms, axis=1, keepdims=True), packed)
        slot = group * n + part_of(me) * nb + me // parts
        rows_buf[slot] = jnp.sum(packed, axis=0, keepdims=True)

        def share(t, z):
            return remote(
                rows_buf.at[slot], rows_buf.at[slot], g_send.at[0], g_recv.at[0],
                dom=wrapped(me + t, n), shift=around[z],
            )

        for z in (2, 1, 3, 0):
            for t in range(n):
                if z or t:
                    share(t, z).start()
        take_halo(0)
        images(wide.at[0], slots[0], accs)
        take_halo(1)
        images(wide.at[1], slots[1], accs)
        drain(wide.at[2, pl.ds(depth, rows)], z_recv.at[2])
        take_halo(2)
        images(wide.at[2], slots[2], accs)
        everyone = pl.ds(0, groups * n - 1)
        drain(rows_buf.at[everyone], g_recv.at[0])

        lane_row = lax.broadcasted_iota(jnp.int32, (1, LANES), 1)
        sigma = jnp.full((1, LANES), MID, F32)
        for j in range(shifts):
            sigma = jnp.where(lane_row == j, table_ref[ids_ref[j]], sigma)
        flat_rows = rows_buf.reshape(groups * n, LANES)
        gram = []
        for g in range(groups):
            block = flat_rows[pl.ds(g * n, n)]
            gram.append(sum(block[q * nb : (q + 1) * nb] for q in range(parts)))
        solved = coefficients(jnp.concatenate(gram, axis=0), sigma)
        for i, value in enumerate(solved):
            for j in range(shifts):
                spreaded = jnp.broadcast_to(value[:, j : j + 1], value.shape)
                coeff_out[j, i] = spreaded.reshape(groups, nb, LANES)

        to_both(lambda side: drain(wide.at[0, pl.ds(0, depth)], halo_send.at[side]))
        drain(wide.at[pl.ds(0, 2), pl.ds(0, rows - came + half * ny + 2 * depth)], z_send.at[0])
        drain(in_buf.at[peers, :, pl.ds(0, BASIS)], rs_send.at[0])
        drain(rows_buf.at[everyone], g_send.at[0])

    unit_sums = [pltpu.ACC(i % 2)((ny * nb, 2 * LANES), F32) for i in range(8)]
    pl.run_scoped(after, *unit_sums)


def combine_kernel(fields_ref, own_ref, coeff_ref, sol_hbm, res_hbm, sol_buf, res_buf, sem):
    groups, shifts = fields_ref.shape[0], fields_ref.shape[1]
    rows, nb = fields_ref.shape[3], fields_ref.shape[4]

    def copies(g, j):
        out = []
        for which, (buf, hbm) in enumerate(((sol_buf, sol_hbm), (res_buf, res_hbm))):
            for b in range(nb):
                out.append(
                    pltpu.make_async_copy(
                        buf.at[g, j, :, b], hbm.at[j, g * nb + b], sem.at[which]
                    )
                )
        return out

    def one(u, carry):
        g, j = u // shifts, lax.rem(u, shifts)
        c = [coeff_ref[j, i, g][None] for i in range(6)]
        w0 = own_ref[g]
        w1, w2, w3 = (fields_ref[g, j, i] for i in range(3))
        sol_buf.at[g, j].reshape(rows, nb, LANES)[...] = c[0] * w0 + c[1] * w1 + c[2] * w2
        res_buf.at[g, j].reshape(rows, nb, LANES)[...] = (
            c[3] * w0 - c[4] * w1 - c[5] * w2 - c[2] * w3
        )
        for copy in copies(g, j):
            copy.start()
        return carry

    lax.fori_loop(0, groups * shifts, one, 0)

    drain(sol_hbm, sem.at[0])
    drain(res_hbm, sem.at[1])


def on_device(sources, kappa, mass, shift_table, shift_ids, sketch):
    n, groups = lax.axis_size("dom"), lax.axis_size("shift")
    nb, slab, ny = sources.shape[0], sources.shape[1], sources.shape[2]
    shifts = shift_ids.shape[0]
    sk = sketch.shape[0]
    rows = slab * ny
    planes = slab + 2 * HALO
    wide_rows, inner = planes * ny, (planes - 2) * ny
    pairs = rows // 2
    weights = 2 * (BASIS + SPLIT) * nb
    vec = (nb, LANES)
    held = PASSED * ny
    sketch, weight, wide, passed, kappa, mass = pl.pallas_call(
        functools.partial(prepare_kernel, n, groups, ny),
        out_shape=(
            pltpu.VMEM((pairs, sk, 2, LANES), BF16),
            pltpu.VMEM((pairs, weights, LANES), BF16),
            pltpu.VMEM((wide_rows, nb, 1, LANES), F32),
            pltpu.VMEM((2, held, nb, 1, LANES), F32),
            pltpu.VMEM((inner,) + vec, F32),
            pltpu.VMEM((inner,) + vec, F32),
        ),
        in_specs=[HBM_SPEC] * 4,
        out_specs=(VMEM_SPEC,) * 6,
        scratch_shapes=[
            pltpu.VMEM((2, inner, 1, LANES), F32),
            pltpu.VMEM((inner,) + vec, F32),
            pltpu.VMEM((inner,) + vec, F32),
            pltpu.VMEM((inner,) + vec, F32),
            pltpu.VMEM((inner - 2 * ny,) + vec, F32),
            pltpu.VMEM((inner - 2 * ny,) + vec, F32),
            pltpu.VMEM((inner - 2 * ny,) + vec, F32),
            DMA((1,)), DMA((2,)),
            DMA((2,)), DMA((HALO, 2)), DMA((2,)), DMA((2,)), DMA((1,)), DMA((2,)),
        ],
        compiler_params=pltpu.CompilerParams(
            collective_id=0, has_side_effects=True, vmem_limit_bytes=16 << 20
        ),
        name="prepare",
    )(
        in_hbm(sources.reshape(nb, rows, 1, LANES)), in_hbm(kappa.reshape(rows, 1, LANES)),
        in_hbm(mass.reshape(rows, 1, LANES)), in_hbm(sketch.reshape(sk, pairs, 2, LANES)),
    )
    parts = n // nb
    span = sk // LANES // parts
    fields, own, coeff = pl.pallas_call(
        functools.partial(project_kernel, n, groups, LINES, ny),
        out_shape=(
            pltpu.VMEM((groups, shifts, 3, rows) + vec, F32),
            pltpu.VMEM((groups, rows) + vec, F32),
            pltpu.VMEM((shifts, 6, groups) + vec, F32),
        ),
        in_specs=[VMEM_SPEC] * 6 + [SMEM_SPEC] * 2,
        out_specs=(VMEM_SPEC,) * 3,
        scratch_shapes=[
            pltpu.VMEM((groups - 1, wide_rows) + vec, F32),
            pltpu.VMEM((shifts, inner) + vec, F32),
            pltpu.VMEM((2 * sk, weights // 2), F32),
            pltpu.VMEM((inner,) + vec, F32),
            pltpu.VMEM((2, inner) + vec, F32),
            pltpu.VMEM((2, inner - 2 * ny) + vec, F32),
            pltpu.VMEM((sk // LANES, BASIS, nb, 1, LANES), F32),
            pltpu.VMEM((n, span, 16, 1, LANES), F32),
            pltpu.VMEM((groups * n, 1, LANES), F32),
            DMA((1,)), DMA((7,)), DMA((2,)), DMA((2, 2)),
            DMA((1,)), DMA((1,)), DMA((1,)), DMA((1,)), pltpu.SemaphoreType.REGULAR,
        ],
        compiler_params=pltpu.CompilerParams(
            collective_id=1, has_side_effects=True, vmem_limit_bytes=16 << 20
        ),
        name="project",
    )(
        in_vmem(sketch.reshape(pairs, 2 * sk, LANES)), in_vmem(weight),
        in_vmem(wide.reshape((wide_rows,) + vec)), in_vmem(passed.reshape((2, held) + vec)),
        in_vmem(kappa), in_vmem(mass), shift_table, shift_ids,
    )

    out = pltpu.HBM((shifts, groups * nb, rows, 1, LANES), F32)
    buf = pltpu.VMEM((groups, shifts, rows, nb, 1, LANES), F32)
    solution, residual = pl.pallas_call(
        combine_kernel,
        out_shape=(out, out),
        in_specs=[VMEM_SPEC] * 3,
        out_specs=(HBM_SPEC,) * 2,
        scratch_shapes=[buf, buf, DMA((2,))],
        compiler_params=pltpu.CompilerParams(vmem_limit_bytes=16 << 20),
        name="combine",
    )(in_vmem(fields), in_vmem(own), in_vmem(coeff))
    shape = (shifts, groups * nb, slab, ny, LANES)
    return solution.reshape(shape), residual.reshape(shape)


def solution(mesh):
    placed = (
        P("shift", "dom", None, None),
        P("dom", None, None),
        P("dom", None, None),
        P(),
        P("shift"),
        P(None, "dom", None, None),
    )
    return jax.shard_map(
        on_device,
        mesh=mesh,
        in_specs=placed,
        out_specs=(P("shift", None, "dom", None, None), P("shift", None, "dom", None, None)),
        check_vma=False,
    )
```

```python
import functools

import jax
import jax.numpy as jnp
from jax import lax
from jax.experimental import pallas as pl
from jax.experimental.pallas import tpu as pltpu
from jax.sharding import PartitionSpec as P

HALO = 3
LANES = 128
MID = 2.25
F32 = jnp.float32
BF16 = jnp.bfloat16
BASIS = 10
PASSED = 3
LINES = 4
SPLIT = 6
IMAGES = ((0,), (1, 6), (2, 3, 7), (4, 5, 8, 9))
VMEM_SPEC = pl.BlockSpec(memory_space=pltpu.VMEM)
HBM_SPEC = pl.BlockSpec(memory_space=pltpu.HBM)
SMEM_SPEC = pl.BlockSpec(memory_space=pltpu.SMEM)
DMA = pltpu.SemaphoreType.DMA


def in_hbm(array):
    return pltpu.with_memory_space_constraint(array, pltpu.HBM)


def in_vmem(array):
    return pltpu.with_memory_space_constraint(array, pltpu.VMEM)


def remote(src, dst, send, recv, **where):
    return pltpu.make_async_remote_copy(
        src_ref=src, dst_ref=dst, send_sem=send, recv_sem=recv,
        device_id=where, device_id_type=pl.DeviceIdType.MESH,
    )


def signal(sem, **where):
    pl.semaphore_signal(sem, inc=1, device_id=where, device_id_type=pl.DeviceIdType.MESH)


def wrapped(index, size):
    return jnp.where(index >= size, index - size, index)


def drain(ref, sem):
    pltpu.make_async_copy(ref, ref, sem).wait()


def plane_of(ref, p, ny):
    return ref[pl.ds(p * ny, ny)]


def neighbour_sum(ref, p, ny):
    inner = plane_of(ref, p, ny)
    total = plane_of(ref, p - 1, ny) + plane_of(ref, p + 1, ny)
    none = jnp.zeros((1,) + inner.shape[1:], F32)
    total = total + jnp.concatenate([none, inner[:-1]], axis=0)
    total = total + jnp.concatenate([inner[1:], none], axis=0)
    lane = lax.broadcasted_iota(jnp.int32, inner.shape, 2)
    total = total + jnp.where(lane > 0, pltpu.roll(inner, 1, 2), 0.0)
    return total + jnp.where(lane < LANES - 1, pltpu.roll(inner, LANES - 1, 2), 0.0)


def edge_flag(p, planes, width, low, high):
    if p < width:
        return low
    return high if p >= planes - width else None


def masked(value, flag):
    return value if flag is None else value * flag


def edge_flags(me, n):
    return (me > 0).astype(F32), (me < n - 1).astype(F32)


def prepare_kernel(
    n, groups, ny, src_hbm, kappa_hbm, mass_hbm, sketch_hbm,
    sketch_out, weights_out, wide, passed_out, kappa_out, mass1,
    coef, diag, g0, g1, h0, h1, h2,
    load_sem, in_sem, wide_send, wide_recv, coef_send, coef_recv, z_send, z_recv,
):
    me = lax.axis_index("dom")
    group = lax.axis_index("shift")
    nb, rows = src_hbm.shape[0], src_hbm.shape[1]
    slab = rows // ny
    right, left = wrapped(me + 1, n), wrapped(me + n - 1, n)
    up, down = wrapped(group + 1, groups), wrapped(group + groups - 1, groups)
    has_right, has_left = me < n - 1, me > 0
    depth = HALO * ny
    thin = (HALO - 1) * ny
    planes = slab + 2 * HALO

    barrier = pltpu.get_barrier_semaphore()
    inputs = [
        pltpu.make_async_copy(src_hbm.at[b], wide.at[pl.ds(depth, rows), b], in_sem.at[0])
        for b in range(nb)
    ]
    inputs.append(pltpu.make_async_copy(kappa_hbm, coef.at[0, pl.ds(thin, rows)], in_sem.at[1]))
    inputs.append(pltpu.make_async_copy(mass_hbm, coef.at[1, pl.ds(thin, rows)], in_sem.at[1]))
    for copy in inputs:
        copy.start()

    @pl.when(has_right)
    def _():
        signal(barrier, dom=right)

    @pl.when(has_left)
    def _():
        signal(barrier, dom=left)

    signal(barrier, shift=up)
    signal(barrier, shift=down)

    def load(k):
        return pltpu.make_async_copy(sketch_hbm.at[:, k], sketch_out.at[k], load_sem.at[0])

    loads = sketch_hbm.shape[1]
    for k in range(loads):
        load(k).start()
    drain(wide.at[pl.ds(depth, rows)], in_sem.at[0])
    drain(coef.at[:, pl.ds(thin, rows)], in_sem.at[1])

    def wide_halo(k, side):
        first, target, there = (
            (depth + rows - (k + 1) * ny, depth - (k + 1) * ny, right),
            (depth + k * ny, depth + rows + k * ny, left),
        )[side]
        return remote(
            wide.at[pl.ds(first, ny)], wide.at[pl.ds(target, ny)],
            wide_send.at[side], wide_recv.at[k, side], dom=there,
        )

    def coef_halo(side):
        first, target, there = ((rows, 0, right), (thin, thin + rows, left))[side]
        return remote(
            coef.at[:, pl.ds(first, thin)], coef.at[:, pl.ds(target, thin)],
            coef_send.at[side], coef_recv.at[side], dom=there,
        )

    def pass_on(way):
        count = passed_out.shape[1]
        there = (up, down)[way]
        return remote(
            wide.at[pl.ds(depth + way * (rows - count), count)], passed_out.at[way],
            z_send.at[0], z_recv.at[way], shift=there,
        )

    pl.semaphore_wait(barrier, has_right.astype(jnp.int32) + has_left.astype(jnp.int32) + 2)

    def send_halo(side):
        wide_halo(0, side).start()
        coef_halo(side).start()
        for k in range(1, HALO):
            wide_halo(k, side).start()

    pl.when(has_right)(lambda: send_halo(0))
    pl.when(has_left)(lambda: send_halo(1))
    for way in range(2):
        pass_on(way).start()

    field = wide.reshape(wide.shape[0], nb, LANES)

    @pl.when(jnp.logical_not(has_left))
    def _():
        field[pl.ds(0, depth)] = jnp.zeros((depth, nb, LANES), F32)
        coef[:, pl.ds(0, thin)] = jnp.zeros((2, thin, 1, LANES), F32)

    @pl.when(jnp.logical_not(has_right))
    def _():
        field[pl.ds(depth + rows, depth)] = jnp.zeros((depth, nb, LANES), F32)
        coef[:, pl.ds(thin + rows, thin)] = jnp.zeros((2, thin, 1, LANES), F32)

    full = (ny, nb, LANES)
    low, high = edge_flags(me, n)

    def factors(p):
        at = pl.ds(p * ny, ny)
        k = jnp.broadcast_to(coef[0, at], full)
        m = jnp.broadcast_to(coef[1, at] - 1.0, full)
        diag[at] = MID * m - k
        mass1[at] = m
        kappa_out[at] = k

    def level1(p):
        flag = edge_flag(p, planes - 2, 2, low, high)
        w = plane_of(field, p + 1, ny)
        out = pl.ds(p * ny, ny)
        g0[out] = masked(diag[out] * w - neighbour_sum(field, p + 1, ny), flag)
        g1[out] = mass1[out] * w

    def level2(p):
        flag = edge_flag(p, planes - 4, 1, low, high)
        at, out = pl.ds((p + 1) * ny, ny), pl.ds(p * ny, ny)
        d, m = diag[at], mass1[at]
        u0, u1 = g0[at], g1[at]
        h0[out] = masked(d * u0 - neighbour_sum(g0, p + 1, ny), flag)
        h1[out] = masked(d * u1 - neighbour_sum(g1, p + 1, ny) + m * u0, flag)
        h2[out] = m * u1

    def level3(p):
        at, inner = pl.ds((p + 2) * ny, ny), pl.ds((p + 1) * ny, ny)
        d, m = diag[at], mass1[at]
        v0, v1, v2 = h0[inner], h1[inner], h2[inner]
        e0 = d * v0 - neighbour_sum(h0, p + 1, ny)
        e1 = d * v1 - neighbour_sum(h1, p + 1, ny) + m * v0
        e2 = d * v2 - neighbour_sum(h2, p + 1, ny) + m * v1
        e3 = m * v2
        first = jnp.concatenate(
            [plane_of(field, p + HALO, ny), g0[at], v0, v1, e0, e1], axis=1
        )
        second = jnp.concatenate([g1[at], v2, e2, e3], axis=1)
        high_part = first.astype(BF16)
        low_part = (first - high_part.astype(F32)).astype(BF16)
        columns = jnp.concatenate([high_part, second.astype(BF16), low_part], axis=1)
        pairs = ny // 2
        weights_out[pl.ds(p * pairs, pairs)] = columns.reshape(pairs, 2 * columns.shape[1], LANES)

    done = [set(), set(), set(), set()]

    def advance(reach):
        ready = set(range(HALO - reach, planes - HALO + reach))
        if reach != 1:
            coefs = range(2, planes - 4) if reach == 0 else (0, 1, planes - 4, planes - 3)
            for p in (coefs if reach in (0, 2) else ()):
                factors(p)
        usable = range(2, planes - 4) if reach < 2 else range(planes - 2)
        for p in range(planes - 2):
            if p not in done[1] and {p, p + 1, p + 2} <= ready and p in usable:
                level1(p)
                done[1].add(p)
        for p in range(planes - 4):
            if p not in done[2] and {p, p + 1, p + 2} <= done[1]:
                level2(p)
                done[2].add(p)
        for p in range(slab):
            if p not in done[3] and {p, p + 1, p + 2} <= done[2]:
                level3(p)
                done[3].add(p)

    def clear_units(*accs):
        for acc in accs:
            pltpu.matmul_pop(acc)

    advance(0)
    pl.run_scoped(
        clear_units,
        pltpu.ACC(0)((sketch_hbm.shape[0], 2 * LANES), F32),
        pltpu.ACC(1)((sketch_hbm.shape[0], 2 * LANES), F32),
    )
    pl.when(has_left)(lambda: wide_halo(0, 0).wait_recv())
    pl.when(has_right)(lambda: wide_halo(0, 1).wait_recv())
    advance(1)

    def take(side):
        coef_halo(side).wait_recv()
        wide_halo(1, side).wait_recv()

    pl.when(has_left)(lambda: take(0))
    pl.when(has_right)(lambda: take(1))
    advance(2)
    pl.when(has_left)(lambda: wide_halo(2, 0).wait_recv())
    pl.when(has_right)(lambda: wide_halo(2, 1).wait_recv())
    advance(3)
    for way in range(2):
        pass_on(way).wait_recv()
    drain(sketch_out, load_sem.at[0])

    def sent(side):
        drain(wide.at[pl.ds(0, depth)], wide_send.at[side])
        drain(coef.at[:, pl.ds(0, thin)], coef_send.at[side])

    pl.when(has_right)(lambda: sent(0))
    pl.when(has_left)(lambda: sent(1))
    drain(wide.at[pl.ds(0, 2 * passed_out.shape[1])], z_send.at[0])


def solve_small(h_vals, entry):
    l00 = jnp.sqrt(entry[0][0])
    l10 = entry[1][0] / l00
    l20 = entry[2][0] / l00
    l11 = jnp.sqrt(entry[1][1] - l10 * l10)
    l21 = (entry[2][1] - l20 * l10) / l11
    l22 = jnp.sqrt(entry[2][2] - l20 * l20 - l21 * l21)
    f0 = h_vals[0] / l00
    f1 = (h_vals[1] - l10 * f0) / l11
    f2 = (h_vals[2] - l20 * f0 - l21 * f1) / l22
    c2 = f2 / l22
    c1 = (f1 - l21 * c2) / l11
    c0 = (f0 - l10 * c1 - l20 * c2) / l00
    return (c0, c1, c2)


def pair_lane(i, k):
    distance = (k - i) % BASIS
    if distance <= BASIS // 2:
        return BASIS * distance + i
    return BASIS * (BASIS - distance) + k


def coefficients(gram, sigma):
    tau, center = sigma - MID, sigma + 6.0

    def product(left, right):
        by_degree = {}
        for p, i in enumerate(IMAGES[left]):
            for q, k in enumerate(IMAGES[right]):
                at = pair_lane(i, k)
                column = gram[:, at : at + 1]
                by_degree[p + q] = by_degree[p + q] + column if p + q in by_degree else column
        top = max(by_degree)
        total = jnp.broadcast_to(by_degree[top], gram.shape)
        for degree in range(top - 1, -1, -1):
            total = total * tau + by_degree[degree]
        return total

    ww = [[product(i, k) if i <= k else None for k in range(4)] for i in range(4)]

    def between(i, k):
        total = ww[i][k]
        if i > 0:
            total = total + center * ww[i - 1][k]
        if k > 0:
            low = ww[min(i, k - 1)][max(i, k - 1)]
            if i > 0:
                low = low + center * ww[i - 1][k - 1]
            total = total + center * low
        return total

    scale = (1.0, 1.0, 1.0 / 6.0, 1.0 / 36.0)
    h_vals = [between(0, i) * scale[i] for i in (1, 2, 3)]
    entry = [[None] * 3 for _ in range(3)]
    for i in range(3):
        for k in range(i + 1):
            entry[i][k] = between(k + 1, i + 1) * (scale[i + 1] * scale[k + 1])
    ridge = 0.001 * (entry[0][0] + entry[1][1] + entry[2][2]) / 3.0 + 1.0
    for i in range(3):
        entry[i][i] = entry[i][i] + ridge
    c0, c1, c2 = solve_small(h_vals, entry)
    c1, c2 = c1 * (1.0 / 6.0), c2 * (1.0 / 36.0)
    return (c0, c1, c2, 1.0 - c0 * center, c0 + c1 * center, c1 + c2 * center)


def project_kernel(
    n, groups, lines, ny, sketch_ref, weights_ref, own_ref, passed_ref, kappa_ref, mass1_ref, table_ref, ids_ref,
    fields_out, own_out, coeff_out,
    wide, step_ref, picked, near, first, second, out_buf, in_buf, rows_buf,
    z_send, z_recv, halo_send, halo_recv, rs_send, rs_recv, g_send, g_recv, row_sem,
):
    me = lax.axis_index("dom")
    group = lax.axis_index("shift")
    planes = own_ref.shape[0] // ny
    nb = own_ref.shape[1]
    slab = planes - 2 * HALO
    rows, depth = slab * ny, HALO * ny
    right, left = wrapped(me + 1, n), wrapped(me + n - 1, n)
    around = [group] + [wrapped(group + t, groups) for t in range(1, groups)]
    up, down = around[1], around[groups - 1]
    has_right, has_left = me < n - 1, me > 0
    shifts = ids_ref.shape[0]
    low, high = edge_flags(me, n)

    barrier = pltpu.get_barrier_semaphore()
    row = n // lines
    base = me // row * row
    for t in range(1, row):
        signal(barrier, dom=base + wrapped(me - base + t, row))
    for t in range(1, lines):
        signal(barrier, dom=wrapped(me + t * row, n))
    for t in range(1, groups):
        signal(barrier, shift=around[t])

    slots = (down, up, around[groups // 2])
    came = passed_ref.shape[1]
    before = (range(came // ny), range(slab - came // ny, slab))
    half = slab // 2

    def planes_at(start, count):
        return pl.ds(depth + start * ny, count * ny)

    def across(way):
        at = planes_at((slab - 1, 0)[way] - (1 - way) * (slab - 1 - came // ny), slab - came // ny)
        return remote(
            own_ref.at[at], wide.at[way, at], z_send.at[0], z_recv.at[way], shift=(up, down)[way]
        )

    def beyond(way):
        at = pl.ds((way * half - before[way][0]) * ny, half * ny)
        return remote(
            passed_ref.at[way, at], wide.at[2, planes_at(way * half, half)],
            z_send.at[0], z_recv.at[2], shift=(up, down)[way],
        )

    def beside(way):
        at = pl.ds((depth + rows, 0)[way], depth)
        return remote(
            own_ref.at[at], wide.at[way, at], z_send.at[0], z_recv.at[3 + way],
            shift=(up, down)[way],
        )

    def relay(way):
        at = pl.ds((depth + rows, 0)[way], depth)
        return remote(
            wide.at[way, at], wide.at[2, at], z_send.at[0], z_recv.at[5 + way], shift=(up, down)[way]
        )

    def halo(index, side, src, first_plane, count):
        target = ((first_plane - (slab - HALO)) * ny, depth + rows + first_plane * ny)[side]
        return remote(
            src, wide.at[index, pl.ds(target, count * ny)],
            halo_send.at[side], halo_recv.at[index, side], dom=(right, left)[side],
        )

    def planes_for(side):
        return range(slab - HALO, slab) if side == 0 else range(HALO)

    def early_halo(index, side):
        mine = [p for p in planes_for(side) if p in before[index]]
        if index != side:
            return
        at = pl.ds((mine[0] - before[index][0]) * ny, len(mine) * ny)
        halo(index, side, passed_ref.at[index, at], mine[0], len(mine)).start()

    def late_halo(index, side):
        mine = [p for p in planes_for(side) if p not in before[index]]
        if mine and index == side:
            at = planes_at(mine[0], len(mine))
            halo(index, side, wide.at[index, at], mine[0], len(mine)).start()

    def to_both(start):
        pl.when(has_right)(lambda: start(0))
        pl.when(has_left)(lambda: start(1))

    def take_halo(index):
        def take(side):
            drain(wide.at[index, pl.ds(0, depth)], halo_recv.at[index, side])

        if index == 0:
            pl.when(has_left)(lambda: take(0))
        if index == 1:
            pl.when(has_right)(lambda: take(1))
        if index == 2:
            for way in range(2):
                drain(wide.at[2, pl.ds(0, depth)], z_recv.at[5 + way])

    steps = sketch_ref.shape[0] // 2
    pieces = 2
    tall = sketch_ref.shape[1] // (2 * pieces)
    split, columns = SPLIT * nb, BASIS * nb
    chunks = 2 * pieces * tall // (2 * LANES)
    parts = n // nb
    span = chunks // parts
    flat_out = out_buf.reshape(chunks * columns, LANES)

    def part_of(dest):
        return lax.rem(dest, 2) * (parts // 2) + lax.rem(dest // 2, parts // 2)

    def piece(dest):
        return out_buf.at[pl.ds(part_of(dest) * span, span), :, dest // parts]

    def scatter(dest):
        return remote(
            piece(dest), in_buf.at[me, :, pl.ds(0, BASIS)], rs_send.at[0], rs_recv.at[0], dom=dest
        )

    def stage(u):
        tile = jnp.concatenate([weights_ref[2 * u], weights_ref[2 * u + 1]], axis=1)
        for unit in range(2):
            pltpu.matmul_push_rhs(tile, 0, unit, transpose=True)

    def multiply(accs):
        def accumulate(u, part):
            for unit in range(2):
                at = pl.ds((2 * part + unit) * tall, tall)
                tile = jnp.concatenate([sketch_ref[2 * u, at], sketch_ref[2 * u + 1, at]], axis=1)
                pltpu.matmul_acc_lhs(accs[unit], tile, load_staged_rhs=0)

        def run(part, start, stop):
            def step(u, carry):
                accumulate(u, part)
                stage(u + 1)
                return carry

            lax.fori_loop(start, stop, step, 0)

        def collect(part):
            accumulate(steps - 1, part)
            if part + 1 < pieces:
                stage(0)
            odd = lax.rem(lax.broadcasted_iota(jnp.int32, (tall, LANES), 0), 2) == 1
            for unit in range(2):
                value = pltpu.matmul_pop(accs[unit])
                picked[pl.ds((2 * part + unit) * tall, tall)] = jnp.where(
                    odd, value[:, LANES:], value[:, :LANES]
                )
            first = part * 2 * tall
            turned = (
                picked[pl.ds(first, tall, stride=2)] + picked[pl.ds(first + 1, tall, stride=2)]
            ).T
            sketched = jnp.concatenate(
                [turned[:split] + turned[columns:], turned[split:columns]], axis=0
            )
            share = chunks // pieces
            for r in range(share):
                flat_out[pl.ds((part * share + r) * columns, columns)] = sketched[
                    :, r * LANES : (r + 1) * LANES
                ]

        def send(part):
            mine = n // pieces
            for t in range(mine):
                dest = pieces * lax.rem(me // pieces + t, mine) + part
                pl.when(dest != me)(lambda: scatter(dest).start())

        stage(0)
        run(0, 0, steps - 1)
        pl.semaphore_wait(barrier, row - 1 + lines - 1 + groups - 1)
        for t in range(1, lines):
            signal(row_sem, dom=wrapped(me + t * row, n))
        for way in range(2):
            across(way).start()
        for way in range(2):
            beside(way).start()
        for way in range(2):
            beyond(way).start()
        collect(0)
        run(1, 0, steps // 2)
        pl.semaphore_wait(row_sem, lines - 1)
        send(0)
        for index in range(2):
            to_both(lambda side: early_halo(index, side))
        run(1, steps // 2, steps - 1)
        collect(1)
        send(1)

    pl.run_scoped(
        lambda *accs: multiply(accs),
        pltpu.ACC(0)((tall, 2 * LANES), F32), pltpu.ACC(1)((tall, 2 * LANES), F32),
    )
    in_buf[me, :, pl.ds(0, BASIS)] = piece(me)[...]

    def clear(at, indices):
        for index in indices:
            wide[index, at] = jnp.zeros((depth, nb, LANES), F32)

    pl.when(jnp.logical_not(has_left))(lambda: clear(pl.ds(0, depth), (0,)))
    pl.when(jnp.logical_not(has_right))(lambda: clear(pl.ds(depth + rows, depth), (1,)))
    for index in range(2):
        wide[index, planes_at(before[index][0], came // ny)] = passed_ref[index]
    for j in range(shifts):
        step_ref[j] = table_ref[ids_ref[j]] * mass1_ref[...] - kappa_ref[...]

    def split_sums(field, at, acc):
        parts_of = [field[pl.ds(p * ny, ny)].reshape(ny * nb, LANES) for p in at]
        high_parts = [part.astype(BF16) for part in parts_of]
        low_parts = [
            (part - high_part.astype(F32)).astype(BF16)
            for part, high_part in zip(parts_of, high_parts)
        ]
        pltpu.matmul_acc_lhs(acc, jnp.concatenate(high_parts, axis=1))
        pltpu.matmul_acc_lhs(acc, jnp.concatenate(low_parts, axis=1))

    def plane_sum(field, p):
        inner = plane_of(field, p, ny)
        total = plane_of(field, p - 1, ny) + plane_of(field, p + 1, ny)
        none = jnp.zeros((1,) + inner.shape[1:], F32)
        total = total + jnp.concatenate([none, inner[:-1]], axis=0)
        return total + jnp.concatenate([inner[1:], none], axis=0)

    def neighbour_sums(field, start, stop, accs):
        pairs = [(p, p + 1) for p in range(start, stop, 2)]
        for pair, acc in zip(pairs, accs):
            split_sums(field, pair, acc)
        across_planes = [plane_sum(field, p) for p in range(start, stop)]
        for pair, acc in zip(pairs, accs):
            value = pltpu.matmul_pop(acc)
            for i, p in enumerate(pair):
                along = value[:, i * LANES : (i + 1) * LANES].reshape(ny, nb, LANES)
                yield p, across_planes[p - start] + along

    def images(field, slot, accs, start=0, stop=shifts // 2):
        if start == 0:
            for p, total in neighbour_sums(field, 1, planes - 1, accs[0]):
                near[pl.ds((p - 1) * ny, ny)] = total

        def shift_pair(u, carry):
            for i in range(2):
                j = 2 * u + i
                for p in range(planes - 2):
                    at = pl.ds(p * ny, ny)
                    flag = edge_flag(p, planes - 2, 2, low, high)
                    first[i, at] = masked(
                        step_ref[j, at] * plane_of(field, p + 1, ny) - near[at], flag
                    )
            for i in range(2):
                j = 2 * u + i
                for p, total in neighbour_sums(first.at[i], 1, planes - 3, accs[i]):
                    at = pl.ds(p * ny, ny)
                    flag = edge_flag(p - 1, planes - 4, 1, low, high)
                    second[i, pl.ds((p - 1) * ny, ny)] = masked(
                        step_ref[j, at] * first[i, at] - total, flag
                    )
            for i in range(2):
                j = 2 * u + i
                for p, total in neighbour_sums(second.at[i], 1, planes - 5, accs[i]):
                    at, inner, out = (pl.ds((p + k) * ny, ny) for k in (1, 0, -1))
                    fields_out[slot, j, 0, out] = first[i, at]
                    fields_out[slot, j, 1, out] = second[i, inner]
                    fields_out[slot, j, 2, out] = step_ref[j, at] * second[i, inner] - total
            return carry

        lax.fori_loop(start, stop, shift_pair, 0)
        if stop < shifts // 2:
            return
        for p in range(slab):
            own_out[slot, pl.ds(p * ny, ny)] = plane_of(field, p + HALO, ny)

    def after(*accs):
        accs = (accs[:4], accs[4:])
        here = lax.broadcasted_iota(jnp.int32, (2 * LANES, 2 * LANES), 0)
        there = lax.broadcasted_iota(jnp.int32, (2 * LANES, 2 * LANES), 1)
        beside = (jnp.abs(here - there) == 1) & (here // LANES == there // LANES)
        neighbours = jnp.where(beside, 1.0, 0.0).astype(BF16)
        for unit in range(2):
            pltpu.matmul_push_rhs(neighbours, 0, unit)
            pltpu.matmul_acc_lhs(
                accs[0][unit], jnp.zeros((ny * nb, 2 * LANES), BF16), load_staged_rhs=0
            )
        for way in range(2):
            across(way).wait_recv()
            to_both(lambda side: late_halo(way, side))
        images(own_ref, group, accs)
        for way in range(2):
            drain(wide.at[way, pl.ds(0, depth)], z_recv.at[3 + way])
            relay(way).start()
        take_halo(0)
        images(wide.at[0], slots[0], accs, stop=shifts // 4)
        peers = pl.ds(0, n - 1)
        drain(in_buf.at[peers, :, pl.ds(0, BASIS)], rs_recv.at[0])
        flat_in = in_buf.reshape(n * span * in_buf.shape[2], LANES)
        tile = span * in_buf.shape[2]
        total = flat_in[pl.ds(0, tile)]
        for t in range(1, n):
            total = total + flat_in[pl.ds(t * tile, tile)]
        lane = lax.broadcasted_iota(jnp.int32, (BASIS, LANES), 1)
        place = lax.broadcasted_iota(jnp.int32, (BASIS, LANES), 0)
        views = [total[r * in_buf.shape[2] :][:BASIS] for r in range(span)]
        twice = [jnp.concatenate([view, view], axis=0) for view in views]
        packed = jnp.zeros((BASIS, LANES), F32)
        for d in range(BASIS // 2 + 1):
            terms = sum(view * wrap[d : d + BASIS] for view, wrap in zip(views, twice))
            packed = jnp.where(lane == place + BASIS * d, jnp.sum(terms, axis=1, keepdims=True), packed)
        slot = group * n + part_of(me) * nb + me // parts
        rows_buf[slot] = jnp.sum(packed, axis=0, keepdims=True)

        def share(t, z):
            return remote(
                rows_buf.at[slot], rows_buf.at[slot], g_send.at[0], g_recv.at[0],
                dom=wrapped(me + t, n), shift=around[z],
            )

        for z in (2, 1, 3, 0):
            for t in range(n):
                if z or t:
                    share(t, z).start()
        images(wide.at[0], slots[0], accs, start=shifts // 4)
        take_halo(1)
        images(wide.at[1], slots[1], accs)
        drain(wide.at[2, pl.ds(depth, rows)], z_recv.at[2])
        take_halo(2)
        images(wide.at[2], slots[2], accs)
        everyone = pl.ds(0, groups * n - 1)
        drain(rows_buf.at[everyone], g_recv.at[0])

        lane_row = lax.broadcasted_iota(jnp.int32, (1, LANES), 1)
        sigma = jnp.full((1, LANES), MID, F32)
        for j in range(shifts):
            sigma = jnp.where(lane_row == j, table_ref[ids_ref[j]], sigma)
        flat_rows = rows_buf.reshape(groups * n, LANES)
        gram = []
        for g in range(groups):
            block = flat_rows[pl.ds(g * n, n)]
            gram.append(sum(block[q * nb : (q + 1) * nb] for q in range(parts)))
        solved = coefficients(jnp.concatenate(gram, axis=0), sigma)
        for i, value in enumerate(solved):
            for j in range(shifts):
                spreaded = jnp.broadcast_to(value[:, j : j + 1], value.shape)
                coeff_out[j, i] = spreaded.reshape(groups, nb, LANES)

        to_both(lambda side: drain(wide.at[0, pl.ds(0, depth)], halo_send.at[side]))
        drain(wide.at[pl.ds(0, 2), pl.ds(0, rows - came + half * ny + 2 * depth)], z_send.at[0])
        drain(in_buf.at[peers, :, pl.ds(0, BASIS)], rs_send.at[0])
        drain(rows_buf.at[everyone], g_send.at[0])

    unit_sums = [pltpu.ACC(i % 2)((ny * nb, 2 * LANES), F32) for i in range(8)]
    pl.run_scoped(after, *unit_sums)


def combine_kernel(fields_ref, own_ref, coeff_ref, sol_hbm, res_hbm, sol_buf, res_buf, sem):
    groups, shifts = fields_ref.shape[0], fields_ref.shape[1]
    rows, nb = fields_ref.shape[3], fields_ref.shape[4]

    def copies(g, j):
        out = []
        for which, (buf, hbm) in enumerate(((sol_buf, sol_hbm), (res_buf, res_hbm))):
            for b in range(nb):
                out.append(
                    pltpu.make_async_copy(
                        buf.at[g, j, :, b], hbm.at[j, g * nb + b], sem.at[which]
                    )
                )
        return out

    def one(u, carry):
        g, j = u // shifts, lax.rem(u, shifts)
        c = [coeff_ref[j, i, g][None] for i in range(6)]
        w0 = own_ref[g]
        w1, w2, w3 = (fields_ref[g, j, i] for i in range(3))
        sol_buf.at[g, j].reshape(rows, nb, LANES)[...] = c[0] * w0 + c[1] * w1 + c[2] * w2
        res_buf.at[g, j].reshape(rows, nb, LANES)[...] = (
            c[3] * w0 - c[4] * w1 - c[5] * w2 - c[2] * w3
        )
        for copy in copies(g, j):
            copy.start()
        return carry

    lax.fori_loop(0, groups * shifts, one, 0)

    drain(sol_hbm, sem.at[0])
    drain(res_hbm, sem.at[1])


def on_device(sources, kappa, mass, shift_table, shift_ids, sketch):
    n, groups = lax.axis_size("dom"), lax.axis_size("shift")
    nb, slab, ny = sources.shape[0], sources.shape[1], sources.shape[2]
    shifts = shift_ids.shape[0]
    sk = sketch.shape[0]
    rows = slab * ny
    planes = slab + 2 * HALO
    wide_rows, inner = planes * ny, (planes - 2) * ny
    pairs = rows // 2
    weights = 2 * (BASIS + SPLIT) * nb
    vec = (nb, LANES)
    held = PASSED * ny
    sketch, weight, wide, passed, kappa, mass = pl.pallas_call(
        functools.partial(prepare_kernel, n, groups, ny),
        out_shape=(
            pltpu.VMEM((pairs, sk, 2, LANES), BF16),
            pltpu.VMEM((pairs, weights, LANES), BF16),
            pltpu.VMEM((wide_rows, nb, 1, LANES), F32),
            pltpu.VMEM((2, held, nb, 1, LANES), F32),
            pltpu.VMEM((inner,) + vec, F32),
            pltpu.VMEM((inner,) + vec, F32),
        ),
        in_specs=[HBM_SPEC] * 4,
        out_specs=(VMEM_SPEC,) * 6,
        scratch_shapes=[
            pltpu.VMEM((2, inner, 1, LANES), F32),
            pltpu.VMEM((inner,) + vec, F32),
            pltpu.VMEM((inner,) + vec, F32),
            pltpu.VMEM((inner,) + vec, F32),
            pltpu.VMEM((inner - 2 * ny,) + vec, F32),
            pltpu.VMEM((inner - 2 * ny,) + vec, F32),
            pltpu.VMEM((inner - 2 * ny,) + vec, F32),
            DMA((1,)), DMA((2,)),
            DMA((2,)), DMA((HALO, 2)), DMA((2,)), DMA((2,)), DMA((1,)), DMA((2,)),
        ],
        compiler_params=pltpu.CompilerParams(
            collective_id=0, has_side_effects=True, vmem_limit_bytes=16 << 20
        ),
        name="prepare",
    )(
        in_hbm(sources.reshape(nb, rows, 1, LANES)), in_hbm(kappa.reshape(rows, 1, LANES)),
        in_hbm(mass.reshape(rows, 1, LANES)), in_hbm(sketch.reshape(sk, pairs, 2, LANES)),
    )
    parts = n // nb
    span = sk // LANES // parts
    fields, own, coeff = pl.pallas_call(
        functools.partial(project_kernel, n, groups, LINES, ny),
        out_shape=(
            pltpu.VMEM((groups, shifts, 3, rows) + vec, F32),
            pltpu.VMEM((groups, rows) + vec, F32),
            pltpu.VMEM((shifts, 6, groups) + vec, F32),
        ),
        in_specs=[VMEM_SPEC] * 6 + [SMEM_SPEC] * 2,
        out_specs=(VMEM_SPEC,) * 3,
        scratch_shapes=[
            pltpu.VMEM((groups - 1, wide_rows) + vec, F32),
            pltpu.VMEM((shifts, inner) + vec, F32),
            pltpu.VMEM((2 * sk, weights // 2), F32),
            pltpu.VMEM((inner,) + vec, F32),
            pltpu.VMEM((2, inner) + vec, F32),
            pltpu.VMEM((2, inner - 2 * ny) + vec, F32),
            pltpu.VMEM((sk // LANES, BASIS, nb, 1, LANES), F32),
            pltpu.VMEM((n, span, 16, 1, LANES), F32),
            pltpu.VMEM((groups * n, 1, LANES), F32),
            DMA((1,)), DMA((7,)), DMA((2,)), DMA((2, 2)),
            DMA((1,)), DMA((1,)), DMA((1,)), DMA((1,)), pltpu.SemaphoreType.REGULAR,
        ],
        compiler_params=pltpu.CompilerParams(
            collective_id=1, has_side_effects=True, vmem_limit_bytes=16 << 20
        ),
        name="project",
    )(
        in_vmem(sketch.reshape(pairs, 2 * sk, LANES)), in_vmem(weight),
        in_vmem(wide.reshape((wide_rows,) + vec)), in_vmem(passed.reshape((2, held) + vec)),
        in_vmem(kappa), in_vmem(mass), shift_table, shift_ids,
    )

    out = pltpu.HBM((shifts, groups * nb, rows, 1, LANES), F32)
    buf = pltpu.VMEM((groups, shifts, rows, nb, 1, LANES), F32)
    solution, residual = pl.pallas_call(
        combine_kernel,
        out_shape=(out, out),
        in_specs=[VMEM_SPEC] * 3,
        out_specs=(HBM_SPEC,) * 2,
        scratch_shapes=[buf, buf, DMA((2,))],
        compiler_params=pltpu.CompilerParams(vmem_limit_bytes=16 << 20),
        name="combine",
    )(in_vmem(fields), in_vmem(own), in_vmem(coeff))
    shape = (shifts, groups * nb, slab, ny, LANES)
    return solution.reshape(shape), residual.reshape(shape)


def solution(mesh):
    placed = (
        P("shift", "dom", None, None),
        P("dom", None, None),
        P("dom", None, None),
        P(),
        P("shift"),
        P(None, "dom", None, None),
    )
    return jax.shard_map(
        on_device,
        mesh=mesh,
        in_specs=placed,
        out_specs=(P("shift", None, "dom", None, None), P("shift", None, "dom", None, None)),
        check_vma=False,
    )
```
